128 devices in a mesh: rad: 8 (over z, core), ma: 16 (over y, x).
Axes of the slice: x: 4, y: 4, z: 4, core: 2. Of those that a mesh axis runs over, the one named last changes fastest.
Arguments:
- spectra: bfloat16 [128, 3, 2, 1024, 1024], P(('rad', 'ma')), may hold values from -0.19921875 to 0.19921875
- legendre: bfloat16 [1024, 1024, 512], P('ma', 'rad'), may hold values from -0.1875 to 0.1875
- selected: int32 [16], replicated, may hold values from 0 to 127, as said below
- m_order: int32 [1024], replicated, may hold values from 0 to 1023, each once
Outputs:
- shell_grid: float32 [16, 3, 2, 512, 3072], P(None, None, None, ('rad', 'ma'))
The draws below stay inside these ranges and needn't reach their ends.
Inputs may be any that keep to these rules, and one draw needn't show every extreme that they name: `selected`: 16 distinct radii, in no particular order. `m_order`: every wavenumber 0 to 1023 stands in exactly one slot.
All inputs are finite; a program needn't handle non-finite values.
Results may differ from the reference program's by a relative error of at most 0.012.
Values may be sent and summed in bfloat16 or wider, within the bound.
A program may use at most 192 MiB of HBM per device.

```python
import jax
import jax.numpy as jnp
from jax import lax

L = 1024
M = 1024
NPHI = 3072
FIELDS = 3
SEL = 16
R = 128
NTHH = 512
N_RAD = 8


def draw_selected(key, part):
    return jax.random.permutation(key, R)[:SEL].astype(jnp.int32)


def level_of(stream_key, extent, split, least, high):
    factor_of = 1.0
    for position, parts in split:
        draws = jax.random.uniform(jax.random.fold_in(jax.random.fold_in(stream_key, 6), position), (parts,), jnp.float32, least / len(split), high / len(split))
        factor_of = factor_of * jnp.repeat(jnp.exp(draws), extent[position] // parts).reshape((-1,) + (1,) * (len(extent) - 1 - position))
    return factor_of


def centred(rng, dims, deviation, reach, pieces=(), kind=jnp.bfloat16):
    factor_of = level_of(rng, dims, pieces, -0.22, 0.18) if pieces else 1.0
    drawn = jax.random.normal(rng, dims, jnp.float32) * deviation * factor_of
    return jnp.minimum(jnp.maximum(drawn, -reach), reach).astype(kind)


def setup_inputs(seed: int = 0) -> dict:
    keys = jax.random.split(jax.random.key(seed), 5)
    return {
        "spectra": centred(keys[0], (R, FIELDS, 2, M, L), 0.03, 0.19921875, ((0, 128),)),
        "legendre": centred(keys[1], (M, L, NTHH), L ** -0.5, 0.1875, ((0, 16), (1, 8))),
        "selected": draw_selected(jax.random.fold_in(keys[4], 71), 0),
        "m_order": jax.random.permutation(keys[3], M).astype(jnp.int32),
    }


def reference(spectra, legendre, selected, m_order):
    picked = spectra[selected]
    picked = picked[:, :, :, m_order, :]
    degree = jnp.arange(L, dtype=jnp.int32)
    tri_mask = degree[None, :] >= m_order[:, None]
    picked = jnp.where(tri_mask[None, None, None], picked, jnp.zeros((), jnp.bfloat16))
    width = SEL * FIELDS * 2
    coeffs = picked.reshape(width, M, L).transpose(1, 0, 2)
    m_sign = (1 - 2 * (m_order % 2)).astype(jnp.float32)
    part_len = L // N_RAD
    total = jnp.zeros((2, M, width, NTHH), jnp.float32)
    for part_index in range(N_RAD):
        first = part_index * part_len
        block = coeffs[:, :, first:first + part_len].astype(jnp.float32)
        ptab = legendre[:, first:first + part_len, :].astype(jnp.float32)
        even_sum = jnp.einsum('sil,slt->sit', block[:, :, 0::2], ptab[:, 0::2, :])
        odd_sum = jnp.einsum('sil,slt->sit', block[:, :, 1::2], ptab[:, 1::2, :])
        north_sum = (even_sum + odd_sum).astype(jnp.bfloat16)
        south_sum = (m_sign[:, None, None] * (even_sum - odd_sum)).astype(jnp.bfloat16)
        north_sum, south_sum = lax.optimization_barrier((north_sum, south_sum))
        total = total + jnp.stack([north_sum.astype(jnp.float32), south_sum.astype(jnp.float32)])
    latitude_sum = total.astype(jnp.bfloat16)
    arranged = latitude_sum.reshape(2, M, SEL, FIELDS, 2, NTHH).transpose(2, 3, 0, 5, 4, 1)
    arranged = arranged.reshape(SEL * FIELDS * 2 * NTHH, 2 * M)
    phase = (m_order[:, None] * jnp.arange(NPHI, dtype=jnp.int32)[None, :]) % NPHI
    angle = phase.astype(jnp.float32) * (2.0 * jnp.pi / NPHI)
    weight = jnp.where(m_order == 0, 1.0, 2.0).astype(jnp.float32)
    dft_table = jnp.concatenate([weight[:, None] * jnp.cos(angle), -weight[:, None] * jnp.sin(angle)], axis=0).astype(jnp.bfloat16)
    grid = jnp.dot(arranged.astype(jnp.float32), dft_table.astype(jnp.float32), preferred_element_type=jnp.float32)
    return grid.reshape(SEL, FIELDS, 2, NTHH, NPHI)
```

```python
import jax
import jax.numpy as jnp
from jax import lax
from jax.experimental import pallas as pl
from jax.experimental.pallas import tpu as pltpu
from jax.sharding import PartitionSpec as P

MESH = pl.DeviceIdType.MESH
M = 1024
NPHI = 3072
FIELDS = 3
SEL = 16
WIDTH = 2 * FIELDS * SEL
CHUNKS = 8
CS = 8


def synth_kernel(coef_ref, flip_ref, leg_ref, lat_ref, part, rcore, r1, r2,
                 core_s, core_r, z1_s, z1_r, z2_s, z2_r):
    rad = lax.axis_index("rad")
    core = lax.rem(rad, 2)
    z = rad // 2
    partner = z * 2 + 1 - core
    zu = lax.rem(z + 1, 4)
    zd = lax.rem(z + 3, 4)
    zo = lax.rem(z + 2, 4)
    up = zu * 2 + core
    down = zd * 2 + core

    barrier = pltpu.get_barrier_semaphore()
    for d in (partner, up, down):
        pl.semaphore_signal(barrier, inc=1, device_id={"rad": d}, device_id_type=MESH)
    pl.semaphore_wait(barrier, 3)

    def core_copy(k):
        return pltpu.make_async_remote_copy(
            src_ref=part.at[1 - core, k], dst_ref=rcore.at[k],
            send_sem=core_s.at[k], recv_sem=core_r.at[k],
            device_id={"rad": partner}, device_id_type=MESH)

    def z1_copy(k, side):
        return pltpu.make_async_remote_copy(
            src_ref=rcore.at[k, zo, side], dst_ref=r1.at[k, side],
            send_sem=z1_s.at[k, side], recv_sem=z1_r.at[k, side],
            device_id={"rad": up if side == 0 else down}, device_id_type=MESH)

    def z2_copy(k, side):
        return pltpu.make_async_remote_copy(
            src_ref=rcore.at[k, zu if side == 0 else zd], dst_ref=r2.at[k, side],
            send_sem=z2_s.at[k, side], recv_sem=z2_r.at[k, side],
            device_id={"rad": up if side == 0 else down}, device_id_type=MESH)

    low = lax.broadcasted_iota(jnp.int32, (WIDTH, 128), 1) < 64

    def legendre_chunk(k):
        def slot(j, carry):
            s = k * CS + j
            north = coef_ref[s]
            south = (north.astype(jnp.float32) * flip_ref[s]).astype(jnp.bfloat16)
            both = jnp.concatenate([north, south], axis=0)
            res = jnp.dot(both, leg_ref[s], preferred_element_type=jnp.float32)
            for q in range(4):
                nt = res[:WIDTH, 128 * q:128 * (q + 1)]
                st = res[WIDTH:, 128 * q:128 * (q + 1)]
                even = jnp.where(low, nt, pltpu.roll(st, 64, 1)).astype(jnp.bfloat16)
                odd = jnp.where(low, pltpu.roll(nt, 64, 1), st).astype(jnp.bfloat16)
                for side in range(2):
                    part[0, k, q, side, j] = even[48 * side:48 * (side + 1)]
                    part[1, k, q, side, j] = odd[48 * side:48 * (side + 1)]
            return carry
        lax.fori_loop(0, CS, slot, 0)

    def step(k, carry):
        @pl.when(k < CHUNKS)
        def _():
            legendre_chunk(k)
            core_copy(k).start()

        @pl.when((k >= 1) & (k < CHUNKS + 1))
        def _():
            c = k - 1
            core_copy(c).wait_recv()

            def add(n, carry):
                q = n // 2
                h = lax.rem(n, 2)
                a = part[core, c, q, h].astype(jnp.float32)
                b = rcore[c, q, h].astype(jnp.float32)
                rcore[c, q, h] = (a + b).astype(jnp.bfloat16)
                return carry
            lax.fori_loop(0, 8, add, 0)
            z1_copy(c, 0).start()
            z1_copy(c, 1).start()

        @pl.when((k >= 2) & (k < CHUNKS + 2))
        def _():
            c = k - 2
            for side in range(2):
                z1_copy(c, side).wait_recv()
                q = zu if side == 0 else zd
                a = rcore[c, q, side].astype(jnp.float32)
                b = r1[c, side].astype(jnp.float32)
                rcore[c, q, side] = (a + b).astype(jnp.bfloat16)
                z2_copy(c, side).start()

        @pl.when(k >= 3)
        def _():
            c = k - 3
            z2_copy(c, 0).wait_recv()
            z2_copy(c, 1).wait_recv()
            for side in range(2):
                total = rcore[c, z, side].astype(jnp.float32)
                total = total + r2[c, 0, side].astype(jnp.float32)
                total = total + r2[c, 1, side].astype(jnp.float32)
                lat_ref[c, side] = total.astype(jnp.bfloat16)
        return carry

    lax.fori_loop(0, CHUNKS + 3, step, 0)

    def drain(k, carry):
        core_copy(k).wait_send()
        for side in range(2):
            z1_copy(k, side).wait_send()
            z2_copy(k, side).wait_send()
        return carry
    lax.fori_loop(0, CHUNKS, drain, 0)


def synth(coef, flip, leg):
    bf = jnp.bfloat16
    vm = pl.BlockSpec(memory_space=pltpu.VMEM)
    return pl.pallas_call(
        synth_kernel,
        name="synth",
        out_shape=jax.ShapeDtypeStruct((CHUNKS, 2, CS, 48, 128), bf),
        in_specs=[vm, vm, vm],
        out_specs=vm,
        scratch_shapes=[
            pltpu.VMEM((2, CHUNKS, 4, 2, CS, 48, 128), bf),
            pltpu.VMEM((CHUNKS, 4, 2, CS, 48, 128), bf),
            pltpu.VMEM((CHUNKS, 2, CS, 48, 128), bf),
            pltpu.VMEM((CHUNKS, 2, 2, CS, 48, 128), bf),
            pltpu.SemaphoreType.DMA((CHUNKS,)),
            pltpu.SemaphoreType.DMA((CHUNKS,)),
            pltpu.SemaphoreType.DMA((CHUNKS, 2)),
            pltpu.SemaphoreType.DMA((CHUNKS, 2)),
            pltpu.SemaphoreType.DMA((CHUNKS, 2)),
            pltpu.SemaphoreType.DMA((CHUNKS, 2)),
        ],
        compiler_params=pltpu.CompilerParams(
            collective_id=1, has_side_effects=True, vmem_limit_bytes=56 * 1024 * 1024),
    )(coef, flip, leg)


PT = 256


def dft_kernel(lat_ref, c0_ref, s0_ref, rc_ref, rs_ref, out_ref, cs, sn, table):
    @pl.when(pl.program_id(0) == 0)
    def _():
        cs[...] = c0_ref[...]
        sn[...] = s0_ref[...]

    for half in range(PT // 128):
        def rows(b, carry, half=half):
            r = pl.ds(pl.multiple_of(b * 64, 64), 64)
            c = cs[r]
            s = sn[r]
            table[pl.ds(pl.multiple_of(b * 128, 128), 64), 128 * half:128 * (half + 1)] = c.astype(jnp.bfloat16)
            table[pl.ds(pl.multiple_of(b * 128 + 64, 64), 64), 128 * half:128 * (half + 1)] = (-s).astype(jnp.bfloat16)
            rc = rc_ref[r]
            rs = rs_ref[r]
            cs[r] = c * rc - s * rs
            sn[r] = s * rc + c * rs
            return carry
        lax.fori_loop(0, 16, rows, 0)
    lhs = jnp.concatenate([lat_ref[a] for a in range(16)], axis=1)
    acc = jnp.dot(lhs, table[...], preferred_element_type=jnp.float32)
    out_ref[...] = acc.reshape(out_ref.shape)


def dft(lat, c0, s0, rc, rs):
    full = lambda *dims: pl.BlockSpec(dims, lambda p: (0,) * len(dims))
    return pl.pallas_call(
        dft_kernel,
        name="dft",
        grid=(NPHI // PT,),
        out_shape=jax.ShapeDtypeStruct((SEL, FIELDS, 2, 4, NPHI), jnp.float32),
        in_specs=[full(16, 384, 128)] + [full(M, 128)] * 4,
        out_specs=pl.BlockSpec((SEL, FIELDS, 2, 4, PT), lambda p: (0, 0, 0, 0, p)),
        scratch_shapes=[
            pltpu.VMEM((M, 128), jnp.float32),
            pltpu.VMEM((M, 128), jnp.float32),
            pltpu.VMEM((2 * M, PT), jnp.bfloat16),
        ],
        compiler_params=pltpu.CompilerParams(
            dimension_semantics=("arbitrary",), vmem_limit_bytes=48 * 1024 * 1024),
    )(lat, c0, s0, rc, rs)


def local(spectra, legendre, selected, m_order):
    rad_count = lax.axis_size("rad")
    ma_count = lax.axis_size("ma")
    rad_index = lax.axis_index("rad")
    ma_index = lax.axis_index("ma")
    slot_count = legendre.shape[0]
    part_len = legendre.shape[1]
    channels = 2 * FIELDS

    step = 2.0 * jnp.pi / NPHI
    weight = jnp.where(m_order == 0, 1.0, 2.0).astype(jnp.float32)[:, None]
    phase = m_order[:, None] * jnp.arange(128, dtype=jnp.int32)[None, :] % NPHI
    angle = phase.astype(jnp.float32) * step
    turn = ((m_order * 128) % NPHI).astype(jnp.float32)[:, None] * step
    turn = jnp.broadcast_to(turn, (M, 128))
    c0, s0 = weight * jnp.cos(angle), weight * jnp.sin(angle)
    rc, rs = jnp.cos(turn), jnp.sin(turn)

    local_spec = spectra.reshape(channels, M, rad_count, part_len)
    local_spec = jnp.take(local_spec, m_order, axis=1)
    local_spec = local_spec.reshape(channels, ma_count, slot_count, rad_count, part_len)
    outgoing = local_spec.transpose(3, 1, 0, 2, 4)
    outgoing = outgoing.reshape(rad_count * ma_count, channels, slot_count, part_len)
    received = lax.all_to_all(outgoing, ("rad", "ma"), split_axis=0, concat_axis=0, tiled=True)
    onehot = (selected[:, None] == jnp.arange(rad_count * ma_count, dtype=jnp.int32)[None, :]).astype(jnp.bfloat16)
    coeffs = jnp.einsum("ij,jcsl->scil", onehot, received, preferred_element_type=jnp.float32)
    slot_m = lax.dynamic_slice_in_dim(m_order, ma_index * slot_count, slot_count)
    degree = rad_index * part_len + jnp.arange(part_len, dtype=jnp.int32)
    keep = degree[None, :] >= slot_m[:, None]
    coeffs = jnp.where(keep[:, None, None, :], coeffs, 0.0).astype(jnp.bfloat16)
    coeffs = coeffs.reshape(slot_count, WIDTH, part_len)
    flip = (1 - 2 * ((slot_m[:, None] + degree[None, :]) % 2)).astype(jnp.float32)[:, None, :]

    lat = synth(coeffs, flip, legendre)
    lat = lat.transpose(0, 2, 1, 3, 4).reshape(slot_count, FIELDS, 2, SEL, 2, ma_count, 4)
    lat = lat.transpose(5, 3, 1, 4, 6, 2, 0).reshape(ma_count, SEL * FIELDS * 2 * 4, 2 * slot_count)
    pieces = lax.all_to_all(lat, "ma", split_axis=0, concat_axis=0, tiled=True)
    return dft(pieces, c0, s0, rc, rs)


def solution(mesh):
    rad_ma = ("rad", "ma")
    in_specs = (P(rad_ma, None, None, None, None), P("ma", "rad", None), P(), P())
    out_specs = P(None, None, None, rad_ma, None)
    return jax.shard_map(local, mesh=mesh, in_specs=in_specs, out_specs=out_specs, check_vma=False)
```

```python
import jax
import jax.numpy as jnp
from jax import lax
from jax.experimental import pallas as pl
from jax.experimental.pallas import tpu as pltpu
from jax.sharding import PartitionSpec as P

MESH = pl.DeviceIdType.MESH
M = 1024
NPHI = 3072
FIELDS = 3
SEL = 16
WIDTH = 2 * FIELDS * SEL
BLOCKS = 4
CS = 16
CHUNKS = FIELDS * BLOCKS


def synth_kernel(coef_ref, flip_ref, leg_ref, lat_ref, part, rcore, r1, r2, latf, bsend,
                 core_s, core_r, z1_s, z1_r, z2_s, z2_r, b_s, b_r):
    rad = lax.axis_index("rad")
    ma = lax.axis_index("ma")
    core = lax.rem(rad, 2)
    z = rad // 2
    partner = z * 2 + 1 - core
    zu = lax.rem(z + 1, 4)
    zd = lax.rem(z + 3, 4)
    zo = lax.rem(z + 2, 4)
    up = zu * 2 + core
    down = zd * 2 + core

    barrier = pltpu.get_barrier_semaphore()
    for d in (partner, up, down):
        pl.semaphore_signal(barrier, inc=1, device_id={"rad": d}, device_id_type=MESH)
    for n in range(1, 16):
        pl.semaphore_signal(barrier, inc=1, device_id={"ma": lax.rem(ma + n, 16)}, device_id_type=MESH)
    pl.semaphore_wait(barrier, 18)

    def core_copy(k):
        return pltpu.make_async_remote_copy(
            src_ref=part.at[1 - core, k], dst_ref=rcore.at[k],
            send_sem=core_s.at[k], recv_sem=core_r.at[k],
            device_id={"rad": partner}, device_id_type=MESH)

    def z1_copy(k, side):
        return pltpu.make_async_remote_copy(
            src_ref=rcore.at[k, zo, side], dst_ref=r1.at[k, side],
            send_sem=z1_s.at[k, side], recv_sem=z1_r.at[k, side],
            device_id={"rad": up if side == 0 else down}, device_id_type=MESH)

    def z2_copy(k, side):
        return pltpu.make_async_remote_copy(
            src_ref=rcore.at[k, zu if side == 0 else zd], dst_ref=r2.at[k, side],
            send_sem=z2_s.at[k, side], recv_sem=z2_r.at[k, side],
            device_id={"rad": up if side == 0 else down}, device_id_type=MESH)

    def plane_copy(f, n):
        to = lax.rem(ma + n, 16)
        return pltpu.make_async_remote_copy(
            src_ref=bsend.at[f, to], dst_ref=lat_ref.at[f, ma],
            send_sem=b_s.at[f, n], recv_sem=b_r.at[f, n],
            device_id={"ma": to}, device_id_type=MESH)

    def plane_arrival(f, n):
        src = lax.rem(ma + 16 - n, 16)
        return pltpu.make_async_remote_copy(
            src_ref=bsend.at[f, src], dst_ref=lat_ref.at[f, src],
            send_sem=b_s.at[f, n], recv_sem=b_r.at[f, n],
            device_id={"ma": src}, device_id_type=MESH)

    low = lax.broadcasted_iota(jnp.int32, (32, 128), 1) < 64
    top = lax.broadcasted_iota(jnp.int32, (8, 128), 0) < 4

    def legendre_chunk(k):
        f = k // BLOCKS
        first = lax.rem(k, BLOCKS) * CS

        def slot(j, carry):
            s = first + j
            north = coef_ref[f, s]
            south = (north.astype(jnp.float32) * flip_ref[s]).astype(jnp.bfloat16)
            both = jnp.concatenate([north, south], axis=0)
            res = jnp.dot(both, leg_ref[s], preferred_element_type=jnp.float32)
            for q in range(4):
                nt = res[:32, 128 * q:128 * (q + 1)]
                st = res[32:, 128 * q:128 * (q + 1)]
                even = jnp.where(low, nt, pltpu.roll(st, 64, 1)).astype(jnp.bfloat16)
                odd = jnp.where(low, pltpu.roll(nt, 64, 1), st).astype(jnp.bfloat16)
                for side in range(2):
                    part[0, k, q, side, j] = even[16 * side:16 * (side + 1)]
                    part[1, k, q, side, j] = odd[16 * side:16 * (side + 1)]
            return carry
        lax.fori_loop(0, CS, slot, 0)

    def turn(f):
        def pair(n, carry):
            halves = []
            for i in (2 * n, 2 * n + 1):
                block = jnp.concatenate(
                    [latf[c, pl.ds(i, 64, stride=16), :] for c in range(2)], axis=0)
                halves.append(block.T)
            for b in range(8):
                first, second = [], []
                for x in halves:
                    nt, st = x[8 * b:8 * b + 8], x[64 + 8 * b:64 + 8 * b + 8]
                    first.append(jnp.where(top, nt, pltpu.roll(st, 4, 0)))
                    second.append(jnp.where(top, pltpu.roll(nt, 4, 0), st))
                bsend[f, 2 * b, n] = jnp.concatenate(first, axis=0).astype(jnp.bfloat16)
                bsend[f, 2 * b + 1, n] = jnp.concatenate(second, axis=0).astype(jnp.bfloat16)
            return carry
        lax.fori_loop(0, 8, pair, 0)
        lat_ref[f, ma] = bsend[f, ma]

    def step(k, carry):
        @pl.when(k < CHUNKS)
        def _():
            legendre_chunk(k)
            core_copy(k).start()

        @pl.when((k >= 1) & (k < CHUNKS + 1))
        def _():
            c = k - 1
            core_copy(c).wait_recv()

            def add(n, carry):
                q = n // 2
                h = lax.rem(n, 2)
                a = part[core, c, q, h].astype(jnp.float32)
                b = rcore[c, q, h].astype(jnp.float32)
                rcore[c, q, h] = (a + b).astype(jnp.bfloat16)
                return carry
            lax.fori_loop(0, 8, add, 0)
            z1_copy(c, 0).start()
            z1_copy(c, 1).start()

        @pl.when((k >= 2) & (k < CHUNKS + 2))
        def _():
            c = k - 2
            for side in range(2):
                z1_copy(c, side).wait_recv()
                q = zu if side == 0 else zd
                a = rcore[c, q, side].astype(jnp.float32)
                b = r1[c, side].astype(jnp.float32)
                rcore[c, q, side] = (a + b).astype(jnp.bfloat16)
                z2_copy(c, side).start()

        @pl.when(k >= 3)
        def _():
            c = k - 3
            f = c // BLOCKS
            block = lax.rem(c, BLOCKS)
            z2_copy(c, 0).wait_recv()
            z2_copy(c, 1).wait_recv()
            for side in range(2):
                total = rcore[c, z, side].astype(jnp.float32)
                total = total + r2[c, 0, side].astype(jnp.float32)
                total = total + r2[c, 1, side].astype(jnp.float32)
                rows = pl.ds(pl.multiple_of(block * 256, 256), 256)
                latf[side, rows, :] = total.reshape(256, 128)

            @pl.when(block == BLOCKS - 1)
            def _():
                turn(f)

                def send(n, carry):
                    plane_copy(f, n).start()
                    return carry
                lax.fori_loop(1, 16, send, 0)
        return carry

    lax.fori_loop(0, CHUNKS + 3, step, 0)

    def drain(k, carry):
        core_copy(k).wait_send()
        for side in range(2):
            z1_copy(k, side).wait_send()
            z2_copy(k, side).wait_send()
        return carry
    lax.fori_loop(0, CHUNKS, drain, 0)

    def settle(n, carry):
        for f in range(FIELDS):
            plane_copy(f, n).wait_send()
            plane_arrival(f, n).wait_recv()
        return carry
    lax.fori_loop(1, 16, settle, 0)


def synth(coef, flip, leg):
    bf = jnp.bfloat16
    vm = pl.BlockSpec(memory_space=pltpu.VMEM)
    dma = pltpu.SemaphoreType.DMA
    return pl.pallas_call(
        synth_kernel,
        name="synth",
        out_shape=jax.ShapeDtypeStruct((FIELDS, 16, 8, 16, 128), bf),
        in_specs=[vm, vm, vm],
        out_specs=vm,
        scratch_shapes=[
            pltpu.VMEM((2, CHUNKS, 4, 2, CS, 16, 128), bf),
            pltpu.VMEM((CHUNKS, 4, 2, CS, 16, 128), bf),
            pltpu.VMEM((CHUNKS, 2, CS, 16, 128), bf),
            pltpu.VMEM((CHUNKS, 2, 2, CS, 16, 128), bf),
            pltpu.VMEM((2, 1024, 128), jnp.float32),
            pltpu.VMEM((FIELDS, 16, 8, 16, 128), bf),
            dma((CHUNKS,)), dma((CHUNKS,)),
            dma((CHUNKS, 2)), dma((CHUNKS, 2)),
            dma((CHUNKS, 2)), dma((CHUNKS, 2)),
            dma((FIELDS, 16)), dma((FIELDS, 16)),
        ],
        compiler_params=pltpu.CompilerParams(
            collective_id=1, has_side_effects=True, vmem_limit_bytes=56 * 1024 * 1024),
    )(coef, flip, leg)


PT = 256


def dft_kernel(lat_ref, c0_ref, s0_ref, rc_ref, rs_ref, out_ref, cs, sn, table):
    @pl.when(pl.program_id(0) == 0)
    def _():
        cs[...] = c0_ref[...]
        sn[...] = s0_ref[...]

    for half in range(PT // 128):
        def rows(b, carry, half=half):
            r = pl.ds(pl.multiple_of(b * 64, 64), 64)
            c = cs[r]
            s = sn[r]
            table[pl.ds(pl.multiple_of(b * 128, 128), 64), 128 * half:128 * (half + 1)] = c.astype(jnp.bfloat16)
            table[pl.ds(pl.multiple_of(b * 128 + 64, 64), 64), 128 * half:128 * (half + 1)] = (-s).astype(jnp.bfloat16)
            rc = rc_ref[r]
            rs = rs_ref[r]
            cs[r] = c * rc - s * rs
            sn[r] = s * rc + c * rs
            return carry
        lax.fori_loop(0, 16, rows, 0)
    for f in range(FIELDS):
        lhs = jnp.concatenate([lat_ref[f, a].reshape(128, 128) for a in range(16)], axis=1)
        acc = jnp.dot(lhs, table[...], preferred_element_type=jnp.float32)
        out_ref[:, f] = acc.reshape(SEL, 2, 4, PT)


def dft(lat, c0, s0, rc, rs):
    full = lambda *dims: pl.BlockSpec(dims, lambda p: (0,) * len(dims))
    return pl.pallas_call(
        dft_kernel,
        name="dft",
        grid=(NPHI // PT,),
        out_shape=jax.ShapeDtypeStruct((SEL, FIELDS, 2, 4, NPHI), jnp.float32),
        in_specs=[full(FIELDS, 16, 8, 16, 128)] + [full(M, 128)] * 4,
        out_specs=pl.BlockSpec((SEL, FIELDS, 2, 4, PT), lambda p: (0, 0, 0, 0, p)),
        scratch_shapes=[
            pltpu.VMEM((M, 128), jnp.float32),
            pltpu.VMEM((M, 128), jnp.float32),
            pltpu.VMEM((2 * M, PT), jnp.bfloat16),
        ],
        compiler_params=pltpu.CompilerParams(
            dimension_semantics=("arbitrary",), vmem_limit_bytes=48 * 1024 * 1024),
    )(lat, c0, s0, rc, rs)


def local(spectra, legendre, selected, m_order):
    rad_count = lax.axis_size("rad")
    ma_count = lax.axis_size("ma")
    rad_index = lax.axis_index("rad")
    ma_index = lax.axis_index("ma")
    slot_count = legendre.shape[0]
    part_len = legendre.shape[1]
    channels = 2 * FIELDS

    step = 2.0 * jnp.pi / NPHI
    weight = jnp.where(m_order == 0, 1.0, 2.0).astype(jnp.float32)[:, None]
    phase = m_order[:, None] * jnp.arange(128, dtype=jnp.int32)[None, :] % NPHI
    angle = phase.astype(jnp.float32) * step
    turn = ((m_order * 128) % NPHI).astype(jnp.float32)[:, None] * step
    turn = jnp.broadcast_to(turn, (M, 128))
    c0, s0 = weight * jnp.cos(angle), weight * jnp.sin(angle)
    rc, rs = jnp.cos(turn), jnp.sin(turn)

    local_spec = spectra.reshape(channels, M, rad_count, part_len)
    local_spec = jnp.take(local_spec, m_order, axis=1)
    local_spec = local_spec.reshape(channels, ma_count, slot_count, rad_count, part_len)
    outgoing = local_spec.transpose(3, 1, 0, 2, 4)
    outgoing = outgoing.reshape(rad_count * ma_count, channels, slot_count, part_len)
    received = lax.all_to_all(outgoing, ("rad", "ma"), split_axis=0, concat_axis=0, tiled=True)
    onehot = (selected[:, None] == jnp.arange(rad_count * ma_count, dtype=jnp.int32)[None, :]).astype(jnp.bfloat16)
    coeffs = jnp.einsum("ij,jfcsl->fscil", onehot, received.reshape(-1, FIELDS, 2, slot_count, part_len), preferred_element_type=jnp.float32)
    slot_m = lax.dynamic_slice_in_dim(m_order, ma_index * slot_count, slot_count)
    degree = rad_index * part_len + jnp.arange(part_len, dtype=jnp.int32)
    keep = degree[None, :] >= slot_m[:, None]
    coeffs = jnp.where(keep[None, :, None, None, :], coeffs, 0.0).astype(jnp.bfloat16)
    coeffs = coeffs.reshape(FIELDS, slot_count, 2 * SEL, part_len)
    flip = (1 - 2 * ((slot_m[:, None] + degree[None, :]) % 2)).astype(jnp.float32)[:, None, :]

    lat = synth(coeffs, flip, legendre)
    return dft(lat, c0, s0, rc, rs)


def solution(mesh):
    rad_ma = ("rad", "ma")
    in_specs = (P(rad_ma, None, None, None, None), P("ma", "rad", None), P(), P())
    out_specs = P(None, None, None, rad_ma, None)
    return jax.shard_map(local, mesh=mesh, in_specs=in_specs, out_specs=out_specs, check_vma=False)
```

```python
import jax
import jax.numpy as jnp
from jax import lax
from jax.experimental import pallas as pl
from jax.experimental.pallas import tpu as pltpu
from jax.sharding import PartitionSpec as P

MESH = pl.DeviceIdType.MESH
M = 1024
NPHI = 3072
FIELDS = 3
SEL = 16
WIDTH = 2 * FIELDS * SEL
BLOCKS = 4
CS = 16
CHUNKS = FIELDS * BLOCKS


def relay_kernel(spec_ref, pick_ref, perm_ref, keep_ref, coef_ref, spec, asend, arecv, part, rcore, r1, r2,
                 load, a_s, a_r, core_s, core_r, z1_s, z1_r, z2_s, z2_r):
    rad = lax.axis_index("rad")
    ma = lax.axis_index("ma")
    core = lax.rem(rad, 2)
    z = rad // 2
    partner = z * 2 + 1 - core
    zu = lax.rem(z + 1, 4)
    zd = lax.rem(z + 3, 4)
    zo = lax.rem(z + 2, 4)
    up = zu * 2 + core
    down = zd * 2 + core

    def load_copy(ch):
        return pltpu.make_async_copy(spec_ref.at[ch], spec.at[ch], load.at[ch])

    for ch in range(2 * FIELDS):
        load_copy(ch).start()

    barrier = pltpu.get_barrier_semaphore()
    for d in (partner, up, down):
        pl.semaphore_signal(barrier, inc=1, device_id={"rad": d}, device_id_type=MESH)
    for n in range(1, 16):
        pl.semaphore_signal(barrier, inc=1, device_id={"ma": lax.rem(ma + n, 16)}, device_id_type=MESH)
    pl.semaphore_wait(barrier, 18)

    def a_copy(k, n):
        to = lax.rem(ma + n, 16)
        return pltpu.make_async_remote_copy(
            src_ref=asend.at[lax.rem(k, 3), to], dst_ref=arecv.at[k, ma],
            send_sem=a_s.at[k, n], recv_sem=a_r.at[k, n],
            device_id={"ma": to}, device_id_type=MESH)

    def a_arrival(k, n):
        src = lax.rem(ma + 16 - n, 16)
        return pltpu.make_async_remote_copy(
            src_ref=asend.at[lax.rem(k, 3), src], dst_ref=arecv.at[k, src],
            send_sem=a_s.at[k, n], recv_sem=a_r.at[k, n],
            device_id={"ma": src}, device_id_type=MESH)

    def core_copy(k):
        return pltpu.make_async_remote_copy(
            src_ref=part.at[1 - core, lax.rem(k, 3)], dst_ref=rcore.at[k],
            send_sem=core_s.at[k], recv_sem=core_r.at[k],
            device_id={"rad": partner}, device_id_type=MESH)

    def z1_copy(k, side):
        return pltpu.make_async_remote_copy(
            src_ref=rcore.at[k, zo, side], dst_ref=r1.at[k, side],
            send_sem=z1_s.at[k, side], recv_sem=z1_r.at[k, side],
            device_id={"rad": up if side == 0 else down}, device_id_type=MESH)

    def z2_copy(k, side):
        return pltpu.make_async_remote_copy(
            src_ref=rcore.at[k, zu if side == 0 else zd], dst_ref=r2.at[k, side],
            send_sem=z2_s.at[k, side], recv_sem=z2_r.at[k, side],
            device_id={"rad": up if side == 0 else down}, device_id_type=MESH)

    def each(first, last, body):
        def run(n, carry):
            body(n)
            return carry
        lax.fori_loop(first, last, run, 0)

    def gather(k):
        f = k // BLOCKS
        b = lax.rem(k, BLOCKS)
        ring = lax.rem(k, 3)

        @pl.when(b == 0)
        def _():
            load_copy(2 * f).wait()
            load_copy(2 * f + 1).wait()

        for c in range(2):
            for n in range(4):
                cols = slice(256 * n, 256 * (n + 1))
                rows = jnp.dot(pick_ref[b], spec[2 * f + c, :, cols], preferred_element_type=jnp.float32)
                asend[ring, :, c, :, cols] = rows.reshape(16, CS, 256).astype(jnp.bfloat16)

    def compact(k):
        ring = lax.rem(k, 3)
        for c in range(2):
            for n in range(4):
                cols = slice(256 * n, 256 * (n + 1))
                rows = arecv[k, :, c, :, cols].reshape(256, 256)
                got = jnp.dot(perm_ref[...], rows, preferred_element_type=jnp.float32)
                got = got.reshape(CS, 16, 256).astype(jnp.bfloat16)
                part[0, ring, n, c] = got[:, :, :128]
                part[1, ring, n, c] = got[:, :, 128:]

    def step(k, carry):
        @pl.when(k < CHUNKS)
        def _():
            @pl.when(k >= 3)
            def _():
                each(1, 16, lambda n: a_copy(k - 3, n).wait_send())
            gather(k)
            each(1, 16, lambda n: a_copy(k, n).start())
            arecv[k, ma] = asend[lax.rem(k, 3), ma]

        @pl.when((k >= 2) & (k < CHUNKS + 2))
        def _():
            c = k - 2
            each(1, 16, lambda n: a_arrival(c, n).wait_recv())

            @pl.when(c >= 3)
            def _():
                core_copy(c - 3).wait_send()
            compact(c)
            core_copy(c).start()

        @pl.when((k >= 3) & (k < CHUNKS + 3))
        def _():
            c = k - 3
            core_copy(c).wait_recv()

            def add(n):
                q = n // 2
                h = lax.rem(n, 2)
                a = part[core, lax.rem(c, 3), q, h].astype(jnp.float32)
                b = rcore[c, q, h].astype(jnp.float32)
                rcore[c, q, h] = (a + b).astype(jnp.bfloat16)
            each(0, 8, add)
            z1_copy(c, 0).start()
            z1_copy(c, 1).start()

        @pl.when((k >= 4) & (k < CHUNKS + 4))
        def _():
            c = k - 4
            for side in range(2):
                z1_copy(c, side).wait_recv()
                q = zu if side == 0 else zd
                a = rcore[c, q, side].astype(jnp.float32)
                b = r1[c, side].astype(jnp.float32)
                rcore[c, q, side] = (a + b).astype(jnp.bfloat16)
                z2_copy(c, side).start()

        @pl.when(k >= 5)
        def _():
            c = k - 5
            z2_copy(c, 0).wait_recv()
            z2_copy(c, 1).wait_recv()
            for side in range(2):
                total = rcore[c, z, side].astype(jnp.float32)
                total = total + r2[c, 0, side].astype(jnp.float32)
                total = total + r2[c, 1, side].astype(jnp.float32)
                slots = pl.ds(lax.rem(c, BLOCKS) * CS, CS)
                coef_ref[c, side] = (total * keep_ref[slots]).astype(jnp.bfloat16)
        return carry

    lax.fori_loop(0, CHUNKS + 5, step, 0)

    def drain(k):
        z1_copy(k, 0).wait_send()
        z1_copy(k, 1).wait_send()
        z2_copy(k, 0).wait_send()
        z2_copy(k, 1).wait_send()
    each(0, CHUNKS, drain)

    def tail(k):
        each(1, 16, lambda n: a_copy(k, n).wait_send())
        core_copy(k).wait_send()
    each(CHUNKS - 3, CHUNKS, tail)


def relay(spec, pick, perm, keep):
    bf = jnp.bfloat16
    vm = pl.BlockSpec(memory_space=pltpu.VMEM)
    dma = pltpu.SemaphoreType.DMA
    return pl.pallas_call(
        relay_kernel,
        name="relay",
        out_shape=jax.ShapeDtypeStruct((CHUNKS, 2, CS, SEL, 128), bf),
        in_specs=[pl.BlockSpec(memory_space=pl.ANY), vm, vm, vm],
        out_specs=vm,
        scratch_shapes=[
            pltpu.VMEM((2 * FIELDS, M, M), bf),
            pltpu.VMEM((3, 16, 2, CS, M), bf),
            pltpu.VMEM((CHUNKS, 16, 2, CS, M), bf),
            pltpu.VMEM((2, 3, 4, 2, CS, SEL, 128), bf),
            pltpu.VMEM((CHUNKS, 4, 2, CS, SEL, 128), bf),
            pltpu.VMEM((CHUNKS, 2, CS, SEL, 128), bf),
            pltpu.VMEM((CHUNKS, 2, 2, CS, SEL, 128), bf),
            dma((2 * FIELDS,)),
            dma((CHUNKS, 16)), dma((CHUNKS, 16)),
            dma((CHUNKS,)), dma((CHUNKS,)),
            dma((CHUNKS, 2)), dma((CHUNKS, 2)),
            dma((CHUNKS, 2)), dma((CHUNKS, 2)),
        ],
        compiler_params=pltpu.CompilerParams(
            collective_id=2, has_side_effects=True, vmem_limit_bytes=60 * 1024 * 1024),
    )(spec, pick, perm, keep)


def synth_kernel(coef_ref, flip_ref, leg_ref, lat_ref, part, rcore, r1, r2, latf, bsend,
                 core_s, core_r, z1_s, z1_r, z2_s, z2_r, b_s, b_r):
    rad = lax.axis_index("rad")
    ma = lax.axis_index("ma")
    core = lax.rem(rad, 2)
    z = rad // 2
    partner = z * 2 + 1 - core
    zu = lax.rem(z + 1, 4)
    zd = lax.rem(z + 3, 4)
    zo = lax.rem(z + 2, 4)
    up = zu * 2 + core
    down = zd * 2 + core

    barrier = pltpu.get_barrier_semaphore()
    for d in (partner, up, down):
        pl.semaphore_signal(barrier, inc=1, device_id={"rad": d}, device_id_type=MESH)
    for n in range(1, 16):
        pl.semaphore_signal(barrier, inc=1, device_id={"ma": lax.rem(ma + n, 16)}, device_id_type=MESH)
    pl.semaphore_wait(barrier, 18)

    def core_copy(k):
        return pltpu.make_async_remote_copy(
            src_ref=part.at[1 - core, k], dst_ref=rcore.at[k],
            send_sem=core_s.at[k], recv_sem=core_r.at[k],
            device_id={"rad": partner}, device_id_type=MESH)

    def z1_copy(k, side):
        return pltpu.make_async_remote_copy(
            src_ref=rcore.at[k, zo, side], dst_ref=r1.at[k, side],
            send_sem=z1_s.at[k, side], recv_sem=z1_r.at[k, side],
            device_id={"rad": up if side == 0 else down}, device_id_type=MESH)

    def z2_copy(k, side):
        return pltpu.make_async_remote_copy(
            src_ref=rcore.at[k, zu if side == 0 else zd], dst_ref=r2.at[k, side],
            send_sem=z2_s.at[k, side], recv_sem=z2_r.at[k, side],
            device_id={"rad": up if side == 0 else down}, device_id_type=MESH)

    def plane_copy(f, n):
        to = lax.rem(ma + n, 16)
        return pltpu.make_async_remote_copy(
            src_ref=bsend.at[f, to], dst_ref=lat_ref.at[f, ma],
            send_sem=b_s.at[f, n], recv_sem=b_r.at[f, n],
            device_id={"ma": to}, device_id_type=MESH)

    def plane_arrival(f, n):
        src = lax.rem(ma + 16 - n, 16)
        return pltpu.make_async_remote_copy(
            src_ref=bsend.at[f, src], dst_ref=lat_ref.at[f, src],
            send_sem=b_s.at[f, n], recv_sem=b_r.at[f, n],
            device_id={"ma": src}, device_id_type=MESH)

    low = lax.broadcasted_iota(jnp.int32, (32, 128), 1) < 64
    top = lax.broadcasted_iota(jnp.int32, (8, 128), 0) < 4

    def legendre_chunk(k):
        f = k // BLOCKS
        first = lax.rem(k, BLOCKS) * CS

        def slot(j, carry):
            s = first + j
            north = jnp.concatenate([coef_ref[k, 0, j], coef_ref[k, 1, j]], axis=0)
            south = (north.astype(jnp.float32) * flip_ref[s]).astype(jnp.bfloat16)
            both = jnp.concatenate([north, south], axis=0)
            res = jnp.dot(both, leg_ref[s], preferred_element_type=jnp.float32)
            for q in range(4):
                nt = res[:32, 128 * q:128 * (q + 1)]
                st = res[32:, 128 * q:128 * (q + 1)]
                even = jnp.where(low, nt, pltpu.roll(st, 64, 1)).astype(jnp.bfloat16)
                odd = jnp.where(low, pltpu.roll(nt, 64, 1), st).astype(jnp.bfloat16)
                for side in range(2):
                    part[0, k, q, side, j] = even[16 * side:16 * (side + 1)]
                    part[1, k, q, side, j] = odd[16 * side:16 * (side + 1)]
            return carry
        lax.fori_loop(0, CS, slot, 0)

    def turn(f):
        def pair(n, carry):
            halves = []
            for i in (2 * n, 2 * n + 1):
                block = jnp.concatenate(
                    [latf[c, pl.ds(i, 64, stride=16), :] for c in range(2)], axis=0)
                halves.append(block.T)
            for b in range(8):
                first, second = [], []
                for x in halves:
                    nt, st = x[8 * b:8 * b + 8], x[64 + 8 * b:64 + 8 * b + 8]
                    first.append(jnp.where(top, nt, pltpu.roll(st, 4, 0)))
                    second.append(jnp.where(top, pltpu.roll(nt, 4, 0), st))
                bsend[f, 2 * b, n] = jnp.concatenate(first, axis=0).astype(jnp.bfloat16)
                bsend[f, 2 * b + 1, n] = jnp.concatenate(second, axis=0).astype(jnp.bfloat16)
            return carry
        lax.fori_loop(0, 8, pair, 0)
        lat_ref[f, ma] = bsend[f, ma]

    def step(k, carry):
        @pl.when(k < CHUNKS)
        def _():
            legendre_chunk(k)
            core_copy(k).start()

        @pl.when((k >= 1) & (k < CHUNKS + 1))
        def _():
            c = k - 1
            core_copy(c).wait_recv()

            def add(n, carry):
                q = n // 2
                h = lax.rem(n, 2)
                a = part[core, c, q, h].astype(jnp.float32)
                b = rcore[c, q, h].astype(jnp.float32)
                rcore[c, q, h] = (a + b).astype(jnp.bfloat16)
                return carry
            lax.fori_loop(0, 8, add, 0)
            z1_copy(c, 0).start()
            z1_copy(c, 1).start()

        @pl.when((k >= 2) & (k < CHUNKS + 2))
        def _():
            c = k - 2
            for side in range(2):
                z1_copy(c, side).wait_recv()
                q = zu if side == 0 else zd
                a = rcore[c, q, side].astype(jnp.float32)
                b = r1[c, side].astype(jnp.float32)
                rcore[c, q, side] = (a + b).astype(jnp.bfloat16)
                z2_copy(c, side).start()

        @pl.when(k >= 3)
        def _():
            c = k - 3
            f = c // BLOCKS
            block = lax.rem(c, BLOCKS)
            z2_copy(c, 0).wait_recv()
            z2_copy(c, 1).wait_recv()
            for side in range(2):
                total = rcore[c, z, side].astype(jnp.float32)
                total = total + r2[c, 0, side].astype(jnp.float32)
                total = total + r2[c, 1, side].astype(jnp.float32)
                rows = pl.ds(pl.multiple_of(block * 256, 256), 256)
                latf[side, rows, :] = total.reshape(256, 128)

            @pl.when(block == BLOCKS - 1)
            def _():
                turn(f)

                def send(n, carry):
                    plane_copy(f, n).start()
                    return carry
                lax.fori_loop(1, 16, send, 0)
        return carry

    lax.fori_loop(0, CHUNKS + 3, step, 0)

    def drain(k, carry):
        core_copy(k).wait_send()
        for side in range(2):
            z1_copy(k, side).wait_send()
            z2_copy(k, side).wait_send()
        return carry
    lax.fori_loop(0, CHUNKS, drain, 0)

    def settle(n, carry):
        for f in range(FIELDS):
            plane_copy(f, n).wait_send()
            plane_arrival(f, n).wait_recv()
        return carry
    lax.fori_loop(1, 16, settle, 0)


def synth(coef, flip, leg):
    bf = jnp.bfloat16
    vm = pl.BlockSpec(memory_space=pltpu.VMEM)
    dma = pltpu.SemaphoreType.DMA
    return pl.pallas_call(
        synth_kernel,
        name="synth",
        out_shape=jax.ShapeDtypeStruct((FIELDS, 16, 8, 16, 128), bf),
        in_specs=[vm, vm, vm],
        out_specs=vm,
        scratch_shapes=[
            pltpu.VMEM((2, CHUNKS, 4, 2, CS, 16, 128), bf),
            pltpu.VMEM((CHUNKS, 4, 2, CS, 16, 128), bf),
            pltpu.VMEM((CHUNKS, 2, CS, 16, 128), bf),
            pltpu.VMEM((CHUNKS, 2, 2, CS, 16, 128), bf),
            pltpu.VMEM((2, 1024, 128), jnp.float32),
            pltpu.VMEM((FIELDS, 16, 8, 16, 128), bf),
            dma((CHUNKS,)), dma((CHUNKS,)),
            dma((CHUNKS, 2)), dma((CHUNKS, 2)),
            dma((CHUNKS, 2)), dma((CHUNKS, 2)),
            dma((FIELDS, 16)), dma((FIELDS, 16)),
        ],
        compiler_params=pltpu.CompilerParams(
            collective_id=1, has_side_effects=True, vmem_limit_bytes=56 * 1024 * 1024),
    )(coef, flip, leg)


PT = 256


def dft_kernel(lat_ref, c0_ref, s0_ref, rc_ref, rs_ref, out_ref, cs, sn, table):
    @pl.when(pl.program_id(0) == 0)
    def _():
        cs[...] = c0_ref[...]
        sn[...] = s0_ref[...]

    for half in range(PT // 128):
        def rows(b, carry, half=half):
            r = pl.ds(pl.multiple_of(b * 64, 64), 64)
            c = cs[r]
            s = sn[r]
            table[pl.ds(pl.multiple_of(b * 128, 128), 64), 128 * half:128 * (half + 1)] = c.astype(jnp.bfloat16)
            table[pl.ds(pl.multiple_of(b * 128 + 64, 64), 64), 128 * half:128 * (half + 1)] = (-s).astype(jnp.bfloat16)
            rc = rc_ref[r]
            rs = rs_ref[r]
            cs[r] = c * rc - s * rs
            sn[r] = s * rc + c * rs
            return carry
        lax.fori_loop(0, 16, rows, 0)
    for f in range(FIELDS):
        lhs = jnp.concatenate([lat_ref[f, a].reshape(128, 128) for a in range(16)], axis=1)
        acc = jnp.dot(lhs, table[...], preferred_element_type=jnp.float32)
        out_ref[:, f] = acc.reshape(SEL, 2, 4, PT)


def dft(lat, c0, s0, rc, rs):
    full = lambda *dims: pl.BlockSpec(dims, lambda p: (0,) * len(dims))
    return pl.pallas_call(
        dft_kernel,
        name="dft",
        grid=(NPHI // PT,),
        out_shape=jax.ShapeDtypeStruct((SEL, FIELDS, 2, 4, NPHI), jnp.float32),
        in_specs=[full(FIELDS, 16, 8, 16, 128)] + [full(M, 128)] * 4,
        out_specs=pl.BlockSpec((SEL, FIELDS, 2, 4, PT), lambda p: (0, 0, 0, 0, p)),
        scratch_shapes=[
            pltpu.VMEM((M, 128), jnp.float32),
            pltpu.VMEM((M, 128), jnp.float32),
            pltpu.VMEM((2 * M, PT), jnp.bfloat16),
        ],
        compiler_params=pltpu.CompilerParams(
            dimension_semantics=("arbitrary",), vmem_limit_bytes=48 * 1024 * 1024),
    )(lat, c0, s0, rc, rs)


def local(spectra, legendre, selected, m_order):
    rad_count = lax.axis_size("rad")
    ma_count = lax.axis_size("ma")
    rad_index = lax.axis_index("rad")
    ma_index = lax.axis_index("ma")
    slot_count = legendre.shape[0]
    part_len = legendre.shape[1]
    channels = 2 * FIELDS

    step = 2.0 * jnp.pi / NPHI
    weight = jnp.where(m_order == 0, 1.0, 2.0).astype(jnp.float32)[:, None]
    phase = m_order[:, None] * jnp.arange(128, dtype=jnp.int32)[None, :] % NPHI
    angle = phase.astype(jnp.float32) * step
    turn = ((m_order * 128) % NPHI).astype(jnp.float32)[:, None] * step
    turn = jnp.broadcast_to(turn, (M, 128))
    c0, s0 = weight * jnp.cos(angle), weight * jnp.sin(angle)
    rc, rs = jnp.cos(turn), jnp.sin(turn)

    slot_m = lax.dynamic_slice_in_dim(m_order, ma_index * slot_count, slot_count)
    degree = rad_index * part_len + jnp.arange(part_len, dtype=jnp.int32)
    keep = (degree[None, :] >= slot_m[:, None]).astype(jnp.float32)[:, None, :]
    flip = (1 - 2 * ((slot_m[:, None] + degree[None, :]) % 2)).astype(jnp.float32)[:, None, :]

    blocks = m_order.reshape(ma_count, BLOCKS, CS).transpose(1, 0, 2).reshape(BLOCKS, ma_count * CS)
    pick = (blocks[:, :, None] == jnp.arange(M, dtype=jnp.int32)).astype(jnp.bfloat16)
    lane = jnp.arange(16 * CS, dtype=jnp.int32)
    row = lane[:, None]
    owner = rad_index * ma_count + lane // CS
    perm = (jnp.tile(selected, CS)[:, None] == owner[None, :]) & (row // SEL == lane[None, :] % CS)
    coeffs = relay(spectra.reshape(channels, M, M), pick, perm.astype(jnp.bfloat16), keep)

    lat = synth(coeffs, flip, legendre)
    return dft(lat, c0, s0, rc, rs)


def solution(mesh):
    rad_ma = ("rad", "ma")
    in_specs = (P(rad_ma, None, None, None, None), P("ma", "rad", None), P(), P())
    out_specs = P(None, None, None, rad_ma, None)
    return jax.shard_map(local, mesh=mesh, in_specs=in_specs, out_specs=out_specs, check_vma=False)
```

```python
import jax
import jax.numpy as jnp
from jax import lax
from jax.experimental import pallas as pl
from jax.experimental.pallas import tpu as pltpu
from jax.sharding import PartitionSpec as P

MESH = pl.DeviceIdType.MESH
M = 1024
NPHI = 3072
FIELDS = 3
SEL = 16
BLOCKS = 4
CS = 16
CHUNKS = FIELDS * BLOCKS


def flow_kernel(spec_ref, leg_ref, pick_ref, perm_ref, keep_ref, flip_ref, lat_ref,
                spec, leg, asend, arecv, coef,
                part1, core1, up1, in1, part2, core2, up2, in2, latf, bsend,
                load, leg_load, a_s, a_r, b_s, b_r, *rad_sems):
    rad = lax.axis_index("rad")
    ma = lax.axis_index("ma")
    core = lax.rem(rad, 2)
    z = rad // 2
    partner = z * 2 + 1 - core
    zu = lax.rem(z + 1, 4)
    zd = lax.rem(z + 3, 4)
    zo = lax.rem(z + 2, 4)
    up = zu * 2 + core
    down = zd * 2 + core

    def each(first, last, body):
        def run(n, carry):
            body(n)
            return carry
        lax.fori_loop(first, last, run, 0)

    def load_copy(f, c):
        return pltpu.make_async_copy(spec_ref.at[2 * f + c], spec.at[c], load.at[c])

    def leg_copy(k):
        rows = pl.ds(lax.rem(k, BLOCKS) * CS, CS)
        return pltpu.make_async_copy(leg_ref.at[rows], leg.at[lax.rem(k, 2)], leg_load.at[lax.rem(k, 2)])

    load_copy(0, 0).start()
    load_copy(0, 1).start()
    leg_copy(0).start()

    barrier = pltpu.get_barrier_semaphore()
    for d in (partner, up, down):
        pl.semaphore_signal(barrier, inc=1, device_id={"rad": d}, device_id_type=MESH)
    for n in range(1, 16):
        pl.semaphore_signal(barrier, inc=1, device_id={"ma": lax.rem(ma + n, 16)}, device_id_type=MESH)
    pl.semaphore_wait(barrier, 18)

    def a_copy(k, n):
        to = lax.rem(ma + n, 16)
        return pltpu.make_async_remote_copy(
            src_ref=asend.at[lax.rem(k, 3), to], dst_ref=arecv.at[k, ma],
            send_sem=a_s.at[k, n], recv_sem=a_r.at[k, n],
            device_id={"ma": to}, device_id_type=MESH)

    def a_arrival(k, n):
        src = lax.rem(ma + 16 - n, 16)
        return pltpu.make_async_remote_copy(
            src_ref=asend.at[lax.rem(k, 3), src], dst_ref=arecv.at[k, src],
            send_sem=a_s.at[k, n], recv_sem=a_r.at[k, n],
            device_id={"ma": src}, device_id_type=MESH)

    def plane_copy(f, n):
        to = lax.rem(ma + n, 16)
        return pltpu.make_async_remote_copy(
            src_ref=bsend.at[f, to], dst_ref=lat_ref.at[f, ma],
            send_sem=b_s.at[f, n], recv_sem=b_r.at[f, n],
            device_id={"ma": to}, device_id_type=MESH)

    def plane_arrival(f, n):
        src = lax.rem(ma + 16 - n, 16)
        return pltpu.make_async_remote_copy(
            src_ref=bsend.at[f, src], dst_ref=lat_ref.at[f, src],
            send_sem=b_s.at[f, n], recv_sem=b_r.at[f, n],
            device_id={"ma": src}, device_id_type=MESH)

    class Reduce:
        def __init__(self, part, rcore, r1, r2, sems):
            self.part, self.rcore, self.r1, self.r2 = part, rcore, r1, r2
            self.core_s, self.core_r, self.z1_s, self.z1_r, self.z2_s, self.z2_r = sems

        def core_copy(self, k):
            return pltpu.make_async_remote_copy(
                src_ref=self.part.at[1 - core, lax.rem(k, 3)], dst_ref=self.rcore.at[k],
                send_sem=self.core_s.at[k], recv_sem=self.core_r.at[k],
                device_id={"rad": partner}, device_id_type=MESH)

        def z1_copy(self, k, side):
            return pltpu.make_async_remote_copy(
                src_ref=self.rcore.at[k, zo, side], dst_ref=self.r1.at[k, side],
                send_sem=self.z1_s.at[k, side], recv_sem=self.z1_r.at[k, side],
                device_id={"rad": up if side == 0 else down}, device_id_type=MESH)

        def z2_copy(self, k, side):
            return pltpu.make_async_remote_copy(
                src_ref=self.rcore.at[k, zu if side == 0 else zd], dst_ref=self.r2.at[k, side],
                send_sem=self.z2_s.at[k, side], recv_sem=self.z2_r.at[k, side],
                device_id={"rad": up if side == 0 else down}, device_id_type=MESH)

        def free(self, k):
            @pl.when(k >= 3)
            def _():
                self.core_copy(k - 3).wait_send()

        def add(self, k):
            self.core_copy(k).wait_recv()

            def body(n):
                q = n // 2
                h = lax.rem(n, 2)
                a = self.part[core, lax.rem(k, 3), q, h].astype(jnp.float32)
                b = self.rcore[k, q, h].astype(jnp.float32)
                self.rcore[k, q, h] = (a + b).astype(jnp.bfloat16)
            each(0, 8, body)
            self.z1_copy(k, 0).start()
            self.z1_copy(k, 1).start()

        def forward(self, k):
            for side in range(2):
                self.z1_copy(k, side).wait_recv()
                q = zu if side == 0 else zd
                a = self.rcore[k, q, side].astype(jnp.float32)
                b = self.r1[k, side].astype(jnp.float32)
                self.rcore[k, q, side] = (a + b).astype(jnp.bfloat16)
                self.z2_copy(k, side).start()

        def finish(self, k, store):
            self.z2_copy(k, 0).wait_recv()
            self.z2_copy(k, 1).wait_recv()
            for side in range(2):
                total = self.rcore[k, z, side].astype(jnp.float32)
                total = total + self.r2[k, 0, side].astype(jnp.float32)
                total = total + self.r2[k, 1, side].astype(jnp.float32)
                store(side, total)

        def drain(self):
            def body(k):
                for side in range(2):
                    self.z1_copy(k, side).wait_send()
                    self.z2_copy(k, side).wait_send()
            each(0, CHUNKS, body)
            each(CHUNKS - 3, CHUNKS, lambda k: self.core_copy(k).wait_send())

    relay = Reduce(part1, core1, up1, in1, rad_sems[:6])
    sums = Reduce(part2, core2, up2, in2, rad_sems[6:])

    def gather(k):
        f = k // BLOCKS
        b = lax.rem(k, BLOCKS)
        ring = lax.rem(k, 3)

        @pl.when(b == 0)
        def _():
            load_copy(f, 0).wait()
            load_copy(f, 1).wait()

        for c in range(2):
            for n in range(4):
                cols = slice(256 * n, 256 * (n + 1))
                rows = jnp.dot(pick_ref[b], spec[c, :, cols], preferred_element_type=jnp.float32)
                asend[ring, :, c, :, cols] = rows.reshape(16, CS, 256).astype(jnp.bfloat16)

        @pl.when((b == BLOCKS - 1) & (f < FIELDS - 1))
        def _():
            load_copy(f + 1, 0).start()
            load_copy(f + 1, 1).start()

    def compact(k):
        ring = lax.rem(k, 3)
        for c in range(2):
            for n in range(4):
                cols = slice(256 * n, 256 * (n + 1))
                rows = arecv[k, :, c, :, cols].reshape(256, 256)
                got = jnp.dot(perm_ref[...], rows, preferred_element_type=jnp.float32)
                got = got.reshape(CS, 16, 256).astype(jnp.bfloat16)
                part1[0, ring, n, c] = got[:, :, :128]
                part1[1, ring, n, c] = got[:, :, 128:]

    low = lax.broadcasted_iota(jnp.int32, (32, 128), 1) < 64
    top = lax.broadcasted_iota(jnp.int32, (8, 128), 0) < 4

    def legendre(k):
        first = lax.rem(k, BLOCKS) * CS
        ring = lax.rem(k, 3)
        leg_copy(k).wait()

        @pl.when(k < CHUNKS - 1)
        def _():
            leg_copy(k + 1).start()

        def store(side, total):
            coef[side] = (total * keep_ref[pl.ds(first, CS)]).astype(jnp.bfloat16)
        relay.finish(k, store)

        def slot(j):
            north = jnp.concatenate([coef[0, j], coef[1, j]], axis=0)
            south = (north.astype(jnp.float32) * flip_ref[first + j]).astype(jnp.bfloat16)
            both = jnp.concatenate([north, south], axis=0)
            res = jnp.dot(both, leg[lax.rem(k, 2), j], preferred_element_type=jnp.float32)
            for q in range(4):
                nt = res[:32, 128 * q:128 * (q + 1)]
                st = res[32:, 128 * q:128 * (q + 1)]
                even = jnp.where(low, nt, pltpu.roll(st, 64, 1)).astype(jnp.bfloat16)
                odd = jnp.where(low, pltpu.roll(nt, 64, 1), st).astype(jnp.bfloat16)
                for side in range(2):
                    part2[0, ring, q, side, j] = even[16 * side:16 * (side + 1)]
                    part2[1, ring, q, side, j] = odd[16 * side:16 * (side + 1)]
        each(0, CS, slot)

    def turn(f):
        def pair(n):
            halves = []
            for i in (2 * n, 2 * n + 1):
                block = jnp.concatenate(
                    [latf[c, pl.ds(i, 64, stride=16), :] for c in range(2)], axis=0)
                halves.append(block.T)
            for b in range(8):
                first, second = [], []
                for x in halves:
                    nt, st = x[8 * b:8 * b + 8], x[64 + 8 * b:64 + 8 * b + 8]
                    first.append(jnp.where(top, nt, pltpu.roll(st, 4, 0)))
                    second.append(jnp.where(top, pltpu.roll(nt, 4, 0), st))
                bsend[f, 2 * b, n] = jnp.concatenate(first, axis=0).astype(jnp.bfloat16)
                bsend[f, 2 * b + 1, n] = jnp.concatenate(second, axis=0).astype(jnp.bfloat16)
        each(0, 8, pair)
        lat_ref[f, ma] = bsend[f, ma]

    def between(k, first, last, body):
        @pl.when((k >= first) & (k < last))
        def _():
            body()

    def step(k, carry):
        def send():
            @pl.when(k >= 3)
            def _():
                each(1, 16, lambda n: a_copy(k - 3, n).wait_send())
            gather(k)
            each(1, 16, lambda n: a_copy(k, n).start())
            arecv[k, ma] = asend[lax.rem(k, 3), ma]
        between(k, 0, CHUNKS, send)
        between(k, 3, CHUNKS + 3, lambda: relay.forward(k - 3))
        between(k, 4, CHUNKS + 4, lambda: sums.forward(k - 4))

        def arrive():
            c = k - 2
            each(1, 16, lambda n: a_arrival(c, n).wait_recv())
            relay.free(c)
            compact(c)
            relay.core_copy(c).start()
        between(k, 2, CHUNKS + 2, arrive)

        def transform():
            c = k - 3
            sums.free(c)
            legendre(c)
            sums.core_copy(c).start()
        between(k, 3, CHUNKS + 3, transform)
        between(k, 2, CHUNKS + 2, lambda: relay.add(k - 2))

        def settle():
            c = k - 4
            f = c // BLOCKS
            block = lax.rem(c, BLOCKS)
            rows = pl.ds(pl.multiple_of(block * 256, 256), 256)

            def store(side, total):
                latf[side, rows, :] = total.reshape(256, 128)
            sums.finish(c, store)

            @pl.when(block == BLOCKS - 1)
            def _():
                turn(f)
                each(1, 16, lambda n: plane_copy(f, n).start())
        between(k, 4, CHUNKS + 4, settle)
        between(k, 3, CHUNKS + 3, lambda: sums.add(k - 3))
        return carry

    lax.fori_loop(0, CHUNKS + 4, step, 0)

    relay.drain()
    sums.drain()
    for k in range(CHUNKS - 3, CHUNKS):
        each(1, 16, lambda n: a_copy(k, n).wait_send())

    def last(n):
        for f in range(FIELDS):
            plane_copy(f, n).wait_send()
            plane_arrival(f, n).wait_recv()
    each(1, 16, last)


def flow(spec, leg, pick, perm, keep, flip):
    bf = jnp.bfloat16
    vm = pl.BlockSpec(memory_space=pltpu.VMEM)
    hbm = pl.BlockSpec(memory_space=pl.ANY)
    dma = pltpu.SemaphoreType.DMA
    reduce_scratch = [
        pltpu.VMEM((2, 3, 4, 2, CS, SEL, 128), bf),
        pltpu.VMEM((CHUNKS, 4, 2, CS, SEL, 128), bf),
        pltpu.VMEM((CHUNKS, 2, CS, SEL, 128), bf),
        pltpu.VMEM((CHUNKS, 2, 2, CS, SEL, 128), bf),
    ]
    return pl.pallas_call(
        flow_kernel,
        name="flow",
        out_shape=jax.ShapeDtypeStruct((FIELDS, 16, 8, 16, 128), bf),
        in_specs=[hbm, hbm, vm, vm, vm, vm],
        out_specs=vm,
        scratch_shapes=[
            pltpu.VMEM((2, M, M), bf),
            pltpu.VMEM((2, CS, 128, 512), bf),
            pltpu.VMEM((3, 16, 2, CS, M), bf),
            pltpu.VMEM((CHUNKS, 16, 2, CS, M), bf),
            pltpu.VMEM((2, CS, SEL, 128), bf),
            *reduce_scratch, *reduce_scratch,
            pltpu.VMEM((2, 1024, 128), jnp.float32),
            pltpu.VMEM((FIELDS, 16, 8, 16, 128), bf),
            dma((2,)), dma((2,)),
            dma((CHUNKS, 16)), dma((CHUNKS, 16)),
            dma((FIELDS, 16)), dma((FIELDS, 16)),
            *([dma((CHUNKS,))] * 2 + [dma((CHUNKS, 2))] * 4) * 2,
        ],
        compiler_params=pltpu.CompilerParams(
            collective_id=1, has_side_effects=True, vmem_limit_bytes=67043328),
    )(spec, leg, pick, perm, keep, flip)


PT = 256


def dft_kernel(lat_ref, c0_ref, s0_ref, rc_ref, rs_ref, out_ref, cs, sn, table):
    @pl.when(pl.program_id(0) == 0)
    def _():
        cs[...] = c0_ref[...]
        sn[...] = s0_ref[...]

    for half in range(PT // 128):
        def rows(b, carry, half=half):
            r = pl.ds(pl.multiple_of(b * 64, 64), 64)
            c = cs[r]
            s = sn[r]
            table[pl.ds(pl.multiple_of(b * 128, 128), 64), 128 * half:128 * (half + 1)] = c.astype(jnp.bfloat16)
            table[pl.ds(pl.multiple_of(b * 128 + 64, 64), 64), 128 * half:128 * (half + 1)] = (-s).astype(jnp.bfloat16)
            rc = rc_ref[r]
            rs = rs_ref[r]
            cs[r] = c * rc - s * rs
            sn[r] = s * rc + c * rs
            return carry
        lax.fori_loop(0, 16, rows, 0)
    for f in range(FIELDS):
        lhs = jnp.concatenate([lat_ref[f, a].reshape(128, 128) for a in range(16)], axis=1)
        acc = jnp.dot(lhs, table[...], preferred_element_type=jnp.float32)
        out_ref[:, f] = acc.reshape(SEL, 2, 4, PT)


def dft(lat, c0, s0, rc, rs):
    full = lambda *dims: pl.BlockSpec(dims, lambda p: (0,) * len(dims))
    return pl.pallas_call(
        dft_kernel,
        name="dft",
        grid=(NPHI // PT,),
        out_shape=jax.ShapeDtypeStruct((SEL, FIELDS, 2, 4, NPHI), jnp.float32),
        in_specs=[full(FIELDS, 16, 8, 16, 128)] + [full(M, 128)] * 4,
        out_specs=pl.BlockSpec((SEL, FIELDS, 2, 4, PT), lambda p: (0, 0, 0, 0, p)),
        scratch_shapes=[
            pltpu.VMEM((M, 128), jnp.float32),
            pltpu.VMEM((M, 128), jnp.float32),
            pltpu.VMEM((2 * M, PT), jnp.bfloat16),
        ],
        compiler_params=pltpu.CompilerParams(
            dimension_semantics=("arbitrary",), vmem_limit_bytes=48 * 1024 * 1024),
    )(lat, c0, s0, rc, rs)


def local(spectra, legendre, selected, m_order):
    rad_count = lax.axis_size("rad")
    ma_count = lax.axis_size("ma")
    rad_index = lax.axis_index("rad")
    ma_index = lax.axis_index("ma")
    slot_count = legendre.shape[0]
    part_len = legendre.shape[1]
    channels = 2 * FIELDS

    step = 2.0 * jnp.pi / NPHI
    weight = jnp.where(m_order == 0, 1.0, 2.0).astype(jnp.float32)[:, None]
    phase = m_order[:, None] * jnp.arange(128, dtype=jnp.int32)[None, :] % NPHI
    angle = phase.astype(jnp.float32) * step
    turn = ((m_order * 128) % NPHI).astype(jnp.float32)[:, None] * step
    turn = jnp.broadcast_to(turn, (M, 128))
    c0, s0 = weight * jnp.cos(angle), weight * jnp.sin(angle)
    rc, rs = jnp.cos(turn), jnp.sin(turn)

    slot_m = lax.dynamic_slice_in_dim(m_order, ma_index * slot_count, slot_count)
    degree = rad_index * part_len + jnp.arange(part_len, dtype=jnp.int32)
    keep = (degree[None, :] >= slot_m[:, None]).astype(jnp.float32)[:, None, :]
    flip = (1 - 2 * ((slot_m[:, None] + degree[None, :]) % 2)).astype(jnp.float32)[:, None, :]

    blocks = m_order.reshape(ma_count, BLOCKS, CS).transpose(1, 0, 2).reshape(BLOCKS, ma_count * CS)
    pick = (blocks[:, :, None] == jnp.arange(M, dtype=jnp.int32)).astype(jnp.bfloat16)
    lane = jnp.arange(16 * CS, dtype=jnp.int32)
    row = lane[:, None]
    owner = rad_index * ma_count + lane // CS
    perm = (jnp.tile(selected, CS)[:, None] == owner[None, :]) & (row // SEL == lane[None, :] % CS)
    lat = flow(spectra.reshape(channels, M, M), legendre, pick, perm.astype(jnp.bfloat16), keep, flip)
    return dft(lat, c0, s0, rc, rs)


def solution(mesh):
    rad_ma = ("rad", "ma")
    in_specs = (P(rad_ma, None, None, None, None), P("ma", "rad", None), P(), P())
    out_specs = P(None, None, None, rad_ma, None)
    return jax.shard_map(local, mesh=mesh, in_specs=in_specs, out_specs=out_specs, check_vma=False)
```

```python
import jax
import jax.numpy as jnp
from jax import lax
from jax.experimental import pallas as pl
from jax.experimental.pallas import tpu as pltpu
from jax.sharding import PartitionSpec as P

MESH = pl.DeviceIdType.MESH
M = 1024
NPHI = 3072
FIELDS = 3
SEL = 16
BLOCKS = 4
CS = 16
CHUNKS = FIELDS * BLOCKS


def flow_kernel(spec_ref, leg_ref, order_ref, chosen_ref, lat_ref, base_ref,
                spec, leg, pick_ref, perm_ref, base, asend, arecv, coef,
                part1, core1, up1, in1, part2, core2, up2, in2, latf, bsend,
                load, leg_load, base_sem, a_s, a_r, b_s, b_r, *rad_sems):
    rad = lax.axis_index("rad")
    ma = lax.axis_index("ma")
    core = lax.rem(rad, 2)
    z = rad // 2
    partner = z * 2 + 1 - core
    zu = lax.rem(z + 1, 4)
    zd = lax.rem(z + 3, 4)
    zo = lax.rem(z + 2, 4)
    up = zu * 2 + core
    down = zd * 2 + core

    def each(first, last, body):
        def run(n, carry):
            body(n)
            return carry
        lax.fori_loop(first, last, run, 0)

    def load_copy(f, c):
        return pltpu.make_async_copy(spec_ref.at[2 * f + c], spec.at[c], load.at[c])

    def leg_copy(k):
        rows = pl.ds(lax.rem(k, BLOCKS) * CS, CS)
        return pltpu.make_async_copy(leg_ref.at[rows], leg.at[lax.rem(k, 2)], leg_load.at[lax.rem(k, 2)])

    load_copy(0, 0).start()
    load_copy(0, 1).start()
    leg_copy(0).start()

    lane = lax.broadcasted_iota(jnp.int32, (16, 128), 1)
    degree = rad * 128 + lax.broadcasted_iota(jnp.int32, (1, 128), 1)
    for j in range(CS):
        for half in range(2):
            hit = (chosen_ref[...] == rad * 16 + 8 * half + lane // 16) & (lax.rem(lane, 16) == j)
            perm_ref[16 * j:16 * (j + 1), 128 * half:128 * (half + 1)] = jnp.where(hit, 1.0, 0.0).astype(jnp.bfloat16)

    def make_pick(b):
        def body(a):
            held = order_ref[pl.ds(a * 64 + b * CS, CS), :]
            for n in range(8):
                hit = jnp.where(held == lane + 128 * n, 1.0, 0.0).astype(jnp.bfloat16)
                pick_ref[b, pl.ds(pl.multiple_of(a * 16, 16), 16), 128 * n:128 * (n + 1)] = hit
        each(0, 16, body)

    def base_copy():
        return pltpu.make_async_copy(base, base_ref, base_sem)

    def make_base():
        def body(n):
            rows = pl.ds(pl.multiple_of(n * 32, 32), 32)
            held = order_ref[rows, :]
            m = held.astype(jnp.float32)
            point = lax.broadcasted_iota(jnp.int32, (32, 128), 1).astype(jnp.float32)
            weight = jnp.where(held == 0, 1.0, 2.0)
            for at, scale, where in ((m * point, weight, 0), (m * 128.0, 1.0, 2)):
                at = at - NPHI * jnp.floor(at * (1.0 / NPHI))
                angle = at * (2.0 * jnp.pi / NPHI)
                base[where, rows, :] = scale * jnp.cos(angle)
                base[where + 1, rows, :] = scale * jnp.sin(angle)
        each(0, 32, body)
        base_copy().start()

    barrier = pltpu.get_barrier_semaphore()
    for d in (partner, up, down):
        pl.semaphore_signal(barrier, inc=1, device_id={"rad": d}, device_id_type=MESH)
    for n in range(1, 16):
        pl.semaphore_signal(barrier, inc=1, device_id={"ma": lax.rem(ma + n, 16)}, device_id_type=MESH)
    pl.semaphore_wait(barrier, 18)

    def a_copy(k, n):
        to = lax.rem(ma + n, 16)
        return pltpu.make_async_remote_copy(
            src_ref=asend.at[lax.rem(k, 3), to], dst_ref=arecv.at[k, ma],
            send_sem=a_s.at[k, n], recv_sem=a_r.at[k, n],
            device_id={"ma": to}, device_id_type=MESH)

    def a_arrival(k, n):
        src = lax.rem(ma + 16 - n, 16)
        return pltpu.make_async_remote_copy(
            src_ref=asend.at[lax.rem(k, 3), src], dst_ref=arecv.at[k, src],
            send_sem=a_s.at[k, n], recv_sem=a_r.at[k, n],
            device_id={"ma": src}, device_id_type=MESH)

    def plane_copy(f, n):
        to = lax.rem(ma + n, 16)
        return pltpu.make_async_remote_copy(
            src_ref=bsend.at[f, to], dst_ref=lat_ref.at[f, ma],
            send_sem=b_s.at[f, n], recv_sem=b_r.at[f, n],
            device_id={"ma": to}, device_id_type=MESH)

    def plane_arrival(f, n):
        src = lax.rem(ma + 16 - n, 16)
        return pltpu.make_async_remote_copy(
            src_ref=bsend.at[f, src], dst_ref=lat_ref.at[f, src],
            send_sem=b_s.at[f, n], recv_sem=b_r.at[f, n],
            device_id={"ma": src}, device_id_type=MESH)

    class Reduce:
        def __init__(self, part, rcore, r1, r2, sems):
            self.part, self.rcore, self.r1, self.r2 = part, rcore, r1, r2
            self.core_s, self.core_r, self.z1_s, self.z1_r, self.z2_s, self.z2_r = sems

        def core_copy(self, k):
            return pltpu.make_async_remote_copy(
                src_ref=self.part.at[1 - core, lax.rem(k, 3)], dst_ref=self.rcore.at[k],
                send_sem=self.core_s.at[k], recv_sem=self.core_r.at[k],
                device_id={"rad": partner}, device_id_type=MESH)

        def z1_copy(self, k, side):
            return pltpu.make_async_remote_copy(
                src_ref=self.rcore.at[k, zo, side], dst_ref=self.r1.at[k, side],
                send_sem=self.z1_s.at[k, side], recv_sem=self.z1_r.at[k, side],
                device_id={"rad": up if side == 0 else down}, device_id_type=MESH)

        def z2_copy(self, k, side):
            return pltpu.make_async_remote_copy(
                src_ref=self.rcore.at[k, zu if side == 0 else zd], dst_ref=self.r2.at[k, side],
                send_sem=self.z2_s.at[k, side], recv_sem=self.z2_r.at[k, side],
                device_id={"rad": up if side == 0 else down}, device_id_type=MESH)

        def free(self, k):
            @pl.when(k >= 3)
            def _():
                self.core_copy(k - 3).wait_send()

        def add(self, k):
            self.core_copy(k).wait_recv()

            def body(n):
                q = n // 2
                h = lax.rem(n, 2)
                a = self.part[core, lax.rem(k, 3), q, h].astype(jnp.float32)
                b = self.rcore[k, q, h].astype(jnp.float32)
                self.rcore[k, q, h] = (a + b).astype(jnp.bfloat16)
            each(0, 8, body)
            self.z1_copy(k, 0).start()
            self.z1_copy(k, 1).start()

        def forward(self, k):
            for side in range(2):
                self.z1_copy(k, side).wait_recv()
                q = zu if side == 0 else zd
                a = self.rcore[k, q, side].astype(jnp.float32)
                b = self.r1[k, side].astype(jnp.float32)
                self.rcore[k, q, side] = (a + b).astype(jnp.bfloat16)
                self.z2_copy(k, side).start()

        def finish(self, k, store):
            self.z2_copy(k, 0).wait_recv()
            self.z2_copy(k, 1).wait_recv()
            for side in range(2):
                total = self.rcore[k, z, side].astype(jnp.float32)
                total = total + self.r2[k, 0, side].astype(jnp.float32)
                total = total + self.r2[k, 1, side].astype(jnp.float32)
                store(side, total)

        def drain(self):
            def body(k):
                for side in range(2):
                    self.z1_copy(k, side).wait_send()
                    self.z2_copy(k, side).wait_send()
            each(0, CHUNKS, body)
            each(CHUNKS - 3, CHUNKS, lambda k: self.core_copy(k).wait_send())

    relay = Reduce(part1, core1, up1, in1, rad_sems[:6])
    sums = Reduce(part2, core2, up2, in2, rad_sems[6:])

    def gather(k):
        f = k // BLOCKS
        b = lax.rem(k, BLOCKS)
        ring = lax.rem(k, 3)

        @pl.when(b == 0)
        def _():
            load_copy(f, 0).wait()
            load_copy(f, 1).wait()

        for c in range(2):
            for n in range(4):
                cols = slice(256 * n, 256 * (n + 1))
                rows = jnp.dot(pick_ref[b], spec[c, :, cols], preferred_element_type=jnp.float32)
                asend[ring, :, c, :, cols] = rows.reshape(16, CS, 256).astype(jnp.bfloat16)

        @pl.when((b == BLOCKS - 1) & (f < FIELDS - 1))
        def _():
            load_copy(f + 1, 0).start()
            load_copy(f + 1, 1).start()

    def compact(k):
        ring = lax.rem(k, 3)
        for c in range(2):
            for n in range(4):
                cols = slice(256 * n, 256 * (n + 1))
                rows = arecv[k, :, c, :, cols].reshape(256, 256)
                got = jnp.dot(perm_ref[...], rows, preferred_element_type=jnp.float32)
                got = got.reshape(CS, 16, 256).astype(jnp.bfloat16)
                part1[0, ring, n, c] = got[:, :, :128]
                part1[1, ring, n, c] = got[:, :, 128:]

    low = lax.broadcasted_iota(jnp.int32, (32, 128), 1) < 64
    top = lax.broadcasted_iota(jnp.int32, (8, 128), 0) < 4

    def legendre(k):
        first = lax.rem(k, BLOCKS) * CS
        ring = lax.rem(k, 3)
        leg_copy(k).wait()

        @pl.when(k < CHUNKS - 1)
        def _():
            leg_copy(k + 1).start()

        def store(side, total):
            keep = degree >= order_ref[pl.ds(ma * 64 + first, CS), :]
            coef[side] = jnp.where(keep[:, None, :], total, 0.0).astype(jnp.bfloat16)
        relay.finish(k, store)

        def slot(j):
            north = jnp.concatenate([coef[0, j], coef[1, j]], axis=0)
            odd = lax.rem(order_ref[pl.ds(ma * 64 + first + j, 1), :] + degree, 2)
            south = jnp.where(odd == 1, -north.astype(jnp.float32), north.astype(jnp.float32)).astype(jnp.bfloat16)
            both = jnp.concatenate([north, south], axis=0)
            res = jnp.dot(both, leg[lax.rem(k, 2), j], preferred_element_type=jnp.float32)
            for q in range(4):
                nt = res[:32, 128 * q:128 * (q + 1)]
                st = res[32:, 128 * q:128 * (q + 1)]
                even = jnp.where(low, nt, pltpu.roll(st, 64, 1)).astype(jnp.bfloat16)
                odd = jnp.where(low, pltpu.roll(nt, 64, 1), st).astype(jnp.bfloat16)
                for side in range(2):
                    part2[0, ring, q, side, j] = even[16 * side:16 * (side + 1)]
                    part2[1, ring, q, side, j] = odd[16 * side:16 * (side + 1)]
        each(0, CS, slot)

    def turn(f):
        def pair(n):
            halves = []
            for i in (2 * n, 2 * n + 1):
                block = jnp.concatenate(
                    [latf[c, pl.ds(i, 64, stride=16), :] for c in range(2)], axis=0)
                halves.append(block.T)
            for b in range(8):
                first, second = [], []
                for x in halves:
                    nt, st = x[8 * b:8 * b + 8], x[64 + 8 * b:64 + 8 * b + 8]
                    first.append(jnp.where(top, nt, pltpu.roll(st, 4, 0)))
                    second.append(jnp.where(top, pltpu.roll(nt, 4, 0), st))
                bsend[f, 2 * b, n] = jnp.concatenate(first, axis=0).astype(jnp.bfloat16)
                bsend[f, 2 * b + 1, n] = jnp.concatenate(second, axis=0).astype(jnp.bfloat16)
        each(0, 8, pair)
        lat_ref[f, ma] = bsend[f, ma]

    def between(k, first, last, body):
        @pl.when((k >= first) & (k < last))
        def _():
            body()

    def step(k, carry):
        def send():
            @pl.when(k >= 3)
            def _():
                each(1, 16, lambda n: a_copy(k - 3, n).wait_send())
            @pl.when(k < BLOCKS)
            def _():
                make_pick(k)
            gather(k)
            each(1, 16, lambda n: a_copy(k, n).start())
            arecv[k, ma] = asend[lax.rem(k, 3), ma]
        between(k, 0, CHUNKS, send)

        @pl.when(k == 6)
        def _():
            make_base()
        between(k, 3, CHUNKS + 3, lambda: relay.forward(k - 3))
        between(k, 4, CHUNKS + 4, lambda: sums.forward(k - 4))

        def arrive():
            c = k - 2
            each(1, 16, lambda n: a_arrival(c, n).wait_recv())
            relay.free(c)
            compact(c)
            relay.core_copy(c).start()
        between(k, 2, CHUNKS + 2, arrive)

        def transform():
            c = k - 3
            sums.free(c)
            legendre(c)
            sums.core_copy(c).start()
        between(k, 3, CHUNKS + 3, transform)
        between(k, 2, CHUNKS + 2, lambda: relay.add(k - 2))

        def settle():
            c = k - 4
            f = c // BLOCKS
            block = lax.rem(c, BLOCKS)
            rows = pl.ds(pl.multiple_of(block * 256, 256), 256)

            def store(side, total):
                latf[side, rows, :] = total.reshape(256, 128)
            sums.finish(c, store)

            @pl.when(block == BLOCKS - 1)
            def _():
                turn(f)
                each(1, 16, lambda n: plane_copy(f, n).start())
        between(k, 4, CHUNKS + 4, settle)
        between(k, 3, CHUNKS + 3, lambda: sums.add(k - 3))
        return carry

    lax.fori_loop(0, CHUNKS + 4, step, 0)

    base_copy().wait()
    relay.drain()
    sums.drain()
    for k in range(CHUNKS - 3, CHUNKS):
        each(1, 16, lambda n: a_copy(k, n).wait_send())

    def last(n):
        for f in range(FIELDS):
            plane_copy(f, n).wait_send()
            plane_arrival(f, n).wait_recv()
    each(1, 16, last)


def flow(spec, leg, order, chosen):
    bf = jnp.bfloat16
    vm = pl.BlockSpec(memory_space=pltpu.VMEM)
    hbm = pl.BlockSpec(memory_space=pl.ANY)
    dma = pltpu.SemaphoreType.DMA
    reduce_scratch = [
        pltpu.VMEM((2, 3, 4, 2, CS, SEL, 128), bf),
        pltpu.VMEM((CHUNKS, 4, 2, CS, SEL, 128), bf),
        pltpu.VMEM((CHUNKS, 2, CS, SEL, 128), bf),
        pltpu.VMEM((CHUNKS, 2, 2, CS, SEL, 128), bf),
    ]
    return pl.pallas_call(
        flow_kernel,
        name="flow",
        out_shape=[jax.ShapeDtypeStruct((FIELDS, 16, 8, 16, 128), bf),
                   jax.ShapeDtypeStruct((4, M, 128), jnp.float32)],
        in_specs=[hbm, hbm, vm, vm],
        out_specs=[vm, hbm],
        scratch_shapes=[
            pltpu.VMEM((2, M, M), bf),
            pltpu.VMEM((2, CS, 128, 512), bf),
            pltpu.VMEM((BLOCKS, 16 * CS, M), bf),
            pltpu.VMEM((16 * CS, 16 * CS), bf),
            pltpu.VMEM((4, M, 128), jnp.float32),
            pltpu.VMEM((3, 16, 2, CS, M), bf),
            pltpu.VMEM((CHUNKS, 16, 2, CS, M), bf),
            pltpu.VMEM((2, CS, SEL, 128), bf),
            *reduce_scratch, *reduce_scratch,
            pltpu.VMEM((2, 1024, 128), jnp.float32),
            pltpu.VMEM((FIELDS, 16, 8, 16, 128), bf),
            dma((2,)), dma((2,)), dma(()),
            dma((CHUNKS, 16)), dma((CHUNKS, 16)),
            dma((FIELDS, 16)), dma((FIELDS, 16)),
            *([dma((CHUNKS,))] * 2 + [dma((CHUNKS, 2))] * 4) * 2,
        ],
        compiler_params=pltpu.CompilerParams(
            collective_id=1, has_side_effects=True, vmem_limit_bytes=67043328),
    )(spec, leg, order, chosen)


PT = 256
STEPS = NPHI // 2 // PT


def dft_kernel(lat_ref, base_ref, out_ref, lhs, cs, sn, ctab, stab, held):
    low = lax.broadcasted_iota(jnp.int32, (128, 128), 1) < 64
    for f in range(FIELDS):
        rows = slice(128 * f, 128 * (f + 1))
        for b in range(8):
            x0 = lat_ref[f, 2 * b].reshape(128, 128).astype(jnp.float32)
            x1 = lat_ref[f, 2 * b + 1].reshape(128, 128).astype(jnp.float32)
            cols = slice(128 * b, 128 * (b + 1))
            lhs[0, rows, cols] = jnp.where(low, x0, pltpu.roll(x1, 64, 1)).astype(jnp.bfloat16)
            lhs[1, rows, cols] = jnp.where(low, pltpu.roll(x0, 64, 1), x1).astype(jnp.bfloat16)
    cs[...] = base_ref[0]
    sn[...] = base_ref[1]
    lane = lax.broadcasted_iota(jnp.int32, (128, 128), 1)
    back = lax.rem(128 - lane, 128)

    def put(f, tile, x):
        cols = pl.ds(pl.multiple_of(tile * 128, 128), 128)
        out_ref[:, f, :, :, cols] = x.reshape(SEL, 2, 4, 128)

    def step(u, carry):
        for half in range(2):
            cols = slice(128 * half, 128 * (half + 1))

            def rows(b, carry, cols=cols):
                r = pl.ds(pl.multiple_of(b * 64, 64), 64)
                c = cs[r]
                s = sn[r]
                ctab[r, cols] = c.astype(jnp.bfloat16)
                stab[r, cols] = (-s).astype(jnp.bfloat16)
                rc = base_ref[2, r]
                rs = base_ref[3, r]
                cs[r] = c * rc - s * rs
                sn[r] = s * rc + c * rs
                return carry
            lax.fori_loop(0, 16, rows, 0)
        for f in range(FIELDS):
            at = slice(128 * f, 128 * (f + 1))
            even = jnp.dot(lhs[0, at], ctab[...], preferred_element_type=jnp.float32)
            odd = jnp.dot(lhs[1, at], stab[...], preferred_element_type=jnp.float32)
            plus = even + odd
            less = even - odd
            first, second = less[:, :128], less[:, 128:]

            @pl.when(u > 0)
            def _():
                put(f, 24 - 2 * u, jnp.where(lane == 0, first, held[f]))

            @pl.when(u < STEPS)
            def _():
                put(f, 2 * u, plus[:, :128])
                put(f, 2 * u + 1, plus[:, 128:])
                turned = jnp.take_along_axis(first, back, axis=1)
                put(f, 23 - 2 * u, jnp.where(lane == 0, second, turned))
                held[f] = jnp.take_along_axis(second, back, axis=1)
        return carry

    lax.fori_loop(0, STEPS + 1, step, 0)


def dft(lat, base):
    vm = pl.BlockSpec(memory_space=pltpu.VMEM)
    f32 = jnp.float32
    return pl.pallas_call(
        dft_kernel,
        name="dft",
        out_shape=jax.ShapeDtypeStruct((SEL, FIELDS, 2, 4, NPHI), f32),
        in_specs=[vm, vm],
        out_specs=vm,
        scratch_shapes=[
            pltpu.VMEM((2, FIELDS * 128, M), jnp.bfloat16),
            pltpu.VMEM((M, 128), f32),
            pltpu.VMEM((M, 128), f32),
            pltpu.VMEM((M, PT), jnp.bfloat16),
            pltpu.VMEM((M, PT), jnp.bfloat16),
            pltpu.VMEM((FIELDS, 128, 128), f32),
        ],
        compiler_params=pltpu.CompilerParams(vmem_limit_bytes=48 * 1024 * 1024),
    )(lat, base)


def local(spectra, legendre, selected, m_order):
    order = jnp.broadcast_to(m_order[:, None], (M, 128))
    chosen = jnp.broadcast_to(selected[:, None], (SEL, 128))
    lat, base = flow(spectra.reshape(2 * FIELDS, M, M), legendre, order, chosen)
    return dft(lat, base)


def solution(mesh):
    rad_ma = ("rad", "ma")
    in_specs = (P(rad_ma, None, None, None, None), P("ma", "rad", None), P(), P())
    out_specs = P(None, None, None, rad_ma, None)
    return jax.shard_map(local, mesh=mesh, in_specs=in_specs, out_specs=out_specs, check_vma=False)
```

```python
import jax
import jax.numpy as jnp
from jax import lax
from jax.experimental import pallas as pl
from jax.experimental.pallas import tpu as pltpu
from jax.sharding import PartitionSpec as P

MESH = pl.DeviceIdType.MESH
M = 1024
NPHI = 3072
FIELDS = 3
SEL = 16
BLOCKS = 4
CS = 16
CHUNKS = FIELDS * BLOCKS
STEPS = NPHI // 2 // 256


def flow_kernel(spec_ref, leg_ref, order_ref, chosen_ref, out_ref,
                spec, leg, pick_ref, perm_ref, base, lat_ref, lhs, held, tiles, asend, arecv, coef,
                part1, core1, up1, in1, part2, core2, up2, in2, latf, bsend,
                load, leg_load, out_sem, a_s, a_r, b_s, b_r, *rad_sems):
    rad = lax.axis_index("rad")
    ma = lax.axis_index("ma")
    core = lax.rem(rad, 2)
    z = rad // 2
    partner = z * 2 + 1 - core
    zu = lax.rem(z + 1, 4)
    zd = lax.rem(z + 3, 4)
    zo = lax.rem(z + 2, 4)
    up = zu * 2 + core
    down = zd * 2 + core

    def each(first, last, body):
        def run(n, carry):
            body(n)
            return carry
        lax.fori_loop(first, last, run, 0)

    def load_copy(f, c):
        return pltpu.make_async_copy(spec_ref.at[2 * f + c], spec.at[c], load.at[c])

    def leg_copy(k):
        rows = pl.ds(lax.rem(k, BLOCKS) * CS, CS)
        return pltpu.make_async_copy(leg_ref.at[rows], leg.at[lax.rem(k, 2)], leg_load.at[lax.rem(k, 2)])

    load_copy(0, 0).start()
    load_copy(0, 1).start()
    leg_copy(0).start()

    lane = lax.broadcasted_iota(jnp.int32, (16, 128), 1)
    degree = rad * 128 + lax.broadcasted_iota(jnp.int32, (1, 128), 1)
    for j in range(CS):
        for half in range(2):
            hit = (chosen_ref[...] == rad * 16 + 8 * half + lane // 16) & (lax.rem(lane, 16) == j)
            perm_ref[16 * j:16 * (j + 1), 128 * half:128 * (half + 1)] = jnp.where(hit, 1.0, 0.0).astype(jnp.bfloat16)

    def make_pick(b):
        def body(a):
            held = order_ref[pl.ds(a * 64 + b * CS, CS), :]
            for n in range(8):
                hit = jnp.where(held == lane + 128 * n, 1.0, 0.0).astype(jnp.bfloat16)
                pick_ref[b, pl.ds(pl.multiple_of(a * 16, 16), 16), 128 * n:128 * (n + 1)] = hit
        each(0, 16, body)

    def make_base():
        def body(n):
            rows = pl.ds(pl.multiple_of(n * 32, 32), 32)
            held = order_ref[rows, :]
            m = held.astype(jnp.float32)
            point = lax.broadcasted_iota(jnp.int32, (32, 128), 1).astype(jnp.float32)
            weight = jnp.where(held == 0, 1.0, 2.0)
            for at, scale, where in ((m * point, weight, 0), (m * 128.0, 1.0, 2)):
                at = at - NPHI * jnp.floor(at * (1.0 / NPHI))
                angle = at * (2.0 * jnp.pi / NPHI)
                base[where, rows, :] = scale * jnp.cos(angle)
                base[where + 1, rows, :] = scale * jnp.sin(angle)
        each(0, 32, body)

    barrier = pltpu.get_barrier_semaphore()
    for d in (partner, up, down):
        pl.semaphore_signal(barrier, inc=1, device_id={"rad": d}, device_id_type=MESH)
    for n in range(1, 16):
        pl.semaphore_signal(barrier, inc=1, device_id={"ma": lax.rem(ma + n, 16)}, device_id_type=MESH)

    def a_copy(k, n):
        to = lax.rem(ma + n, 16)
        return pltpu.make_async_remote_copy(
            src_ref=asend.at[lax.rem(k, 3), to], dst_ref=arecv.at[k, ma],
            send_sem=a_s.at[k, n], recv_sem=a_r.at[k, n],
            device_id={"ma": to}, device_id_type=MESH)

    def a_arrival(k, n):
        src = lax.rem(ma + 16 - n, 16)
        return pltpu.make_async_remote_copy(
            src_ref=asend.at[lax.rem(k, 3), src], dst_ref=arecv.at[k, src],
            send_sem=a_s.at[k, n], recv_sem=a_r.at[k, n],
            device_id={"ma": src}, device_id_type=MESH)

    def plane_copy(f, n):
        to = lax.rem(ma + n, 16)
        return pltpu.make_async_remote_copy(
            src_ref=bsend.at[f, to], dst_ref=lat_ref.at[f, ma],
            send_sem=b_s.at[f, n], recv_sem=b_r.at[f, n],
            device_id={"ma": to}, device_id_type=MESH)

    def plane_arrival(f, n):
        src = lax.rem(ma + 16 - n, 16)
        return pltpu.make_async_remote_copy(
            src_ref=bsend.at[f, src], dst_ref=lat_ref.at[f, src],
            send_sem=b_s.at[f, n], recv_sem=b_r.at[f, n],
            device_id={"ma": src}, device_id_type=MESH)

    class Reduce:
        def __init__(self, part, rcore, r1, r2, sems):
            self.part, self.rcore, self.r1, self.r2 = part, rcore, r1, r2
            self.core_s, self.core_r, self.z1_s, self.z1_r, self.z2_s, self.z2_r = sems

        def core_copy(self, k):
            return pltpu.make_async_remote_copy(
                src_ref=self.part.at[1 - core, lax.rem(k, 3)], dst_ref=self.rcore.at[k],
                send_sem=self.core_s.at[k], recv_sem=self.core_r.at[k],
                device_id={"rad": partner}, device_id_type=MESH)

        def z1_copy(self, k, side):
            return pltpu.make_async_remote_copy(
                src_ref=self.rcore.at[k, zo, side], dst_ref=self.r1.at[k, side],
                send_sem=self.z1_s.at[k, side], recv_sem=self.z1_r.at[k, side],
                device_id={"rad": up if side == 0 else down}, device_id_type=MESH)

        def z2_copy(self, k, side):
            return pltpu.make_async_remote_copy(
                src_ref=self.rcore.at[k, zu if side == 0 else zd], dst_ref=self.r2.at[k, side],
                send_sem=self.z2_s.at[k, side], recv_sem=self.z2_r.at[k, side],
                device_id={"rad": up if side == 0 else down}, device_id_type=MESH)

        def free(self, k):
            @pl.when(k >= 3)
            def _():
                self.core_copy(k - 3).wait_send()

        def add(self, k):
            self.core_copy(k).wait_recv()

            def body(n):
                q = n // 2
                h = lax.rem(n, 2)
                a = self.part[core, lax.rem(k, 3), q, h].astype(jnp.float32)
                b = self.rcore[k, q, h].astype(jnp.float32)
                self.rcore[k, q, h] = (a + b).astype(jnp.bfloat16)
            each(0, 8, body)
            self.z1_copy(k, 0).start()
            self.z1_copy(k, 1).start()

        def forward(self, k):
            for side in range(2):
                self.z1_copy(k, side).wait_recv()
                q = zu if side == 0 else zd
                a = self.rcore[k, q, side].astype(jnp.float32)
                b = self.r1[k, side].astype(jnp.float32)
                self.rcore[k, q, side] = (a + b).astype(jnp.bfloat16)
                self.z2_copy(k, side).start()

        def finish(self, k, store):
            self.z2_copy(k, 0).wait_recv()
            self.z2_copy(k, 1).wait_recv()
            for side in range(2):
                total = self.rcore[k, z, side].astype(jnp.float32)
                total = total + self.r2[k, 0, side].astype(jnp.float32)
                total = total + self.r2[k, 1, side].astype(jnp.float32)
                store(side, total)

        def drain(self):
            def body(k):
                for side in range(2):
                    self.z1_copy(k, side).wait_send()
                    self.z2_copy(k, side).wait_send()
            each(0, CHUNKS, body)
            each(CHUNKS - 3, CHUNKS, lambda k: self.core_copy(k).wait_send())

    relay = Reduce(part1, core1, up1, in1, rad_sems[:6])
    sums = Reduce(part2, core2, up2, in2, rad_sems[6:])

    def gather(k):
        f = k // BLOCKS
        b = lax.rem(k, BLOCKS)
        ring = lax.rem(k, 3)

        @pl.when(b == 0)
        def _():
            load_copy(f, 0).wait()
            load_copy(f, 1).wait()

        for c in range(2):
            for n in range(4):
                cols = slice(256 * n, 256 * (n + 1))
                rows = jnp.dot(pick_ref[b], spec[c, :, cols], preferred_element_type=jnp.float32)
                asend[ring, :, c, :, cols] = rows.reshape(16, CS, 256).astype(jnp.bfloat16)

        @pl.when((b == BLOCKS - 1) & (f < FIELDS - 1))
        def _():
            load_copy(f + 1, 0).start()
            load_copy(f + 1, 1).start()

    def compact(k):
        ring = lax.rem(k, 3)
        for c in range(2):
            for n in range(4):
                cols = slice(256 * n, 256 * (n + 1))
                rows = arecv[k, :, c, :, cols].reshape(256, 256)
                got = jnp.dot(perm_ref[...], rows, preferred_element_type=jnp.float32)
                got = got.reshape(CS, 16, 256).astype(jnp.bfloat16)
                part1[0, ring, n, c] = got[:, :, :128]
                part1[1, ring, n, c] = got[:, :, 128:]

    low = lax.broadcasted_iota(jnp.int32, (32, 128), 1) < 64
    top = lax.broadcasted_iota(jnp.int32, (8, 128), 0) < 4

    def legendre(k):
        first = lax.rem(k, BLOCKS) * CS
        ring = lax.rem(k, 3)
        leg_copy(k).wait()

        @pl.when(k < CHUNKS - 1)
        def _():
            leg_copy(k + 1).start()

        def store(side, total):
            keep = degree >= order_ref[pl.ds(ma * 64 + first, CS), :]
            coef[side] = jnp.where(keep[:, None, :], total, 0.0).astype(jnp.bfloat16)
        relay.finish(k, store)

        def slot(j):
            north = jnp.concatenate([coef[0, j], coef[1, j]], axis=0)
            odd = lax.rem(order_ref[pl.ds(ma * 64 + first + j, 1), :] + degree, 2)
            south = jnp.where(odd == 1, -north.astype(jnp.float32), north.astype(jnp.float32)).astype(jnp.bfloat16)
            both = jnp.concatenate([north, south], axis=0)
            res = jnp.dot(both, leg[lax.rem(k, 2), j], preferred_element_type=jnp.float32)
            for q in range(4):
                nt = res[:32, 128 * q:128 * (q + 1)]
                st = res[32:, 128 * q:128 * (q + 1)]
                even = jnp.where(low, nt, pltpu.roll(st, 64, 1)).astype(jnp.bfloat16)
                odd = jnp.where(low, pltpu.roll(nt, 64, 1), st).astype(jnp.bfloat16)
                for side in range(2):
                    part2[0, ring, q, side, j] = even[16 * side:16 * (side + 1)]
                    part2[1, ring, q, side, j] = odd[16 * side:16 * (side + 1)]
        each(0, CS, slot)

    def turn(f):
        def pair(n):
            halves = []
            for i in (2 * n, 2 * n + 1):
                block = jnp.concatenate(
                    [latf[c, pl.ds(i, 64, stride=16), :] for c in range(2)], axis=0)
                halves.append(block.T)
            for b in range(8):
                first, second = [], []
                for x in halves:
                    nt, st = x[8 * b:8 * b + 8], x[64 + 8 * b:64 + 8 * b + 8]
                    first.append(jnp.where(top, nt, pltpu.roll(st, 4, 0)))
                    second.append(jnp.where(top, pltpu.roll(nt, 4, 0), st))
                bsend[f, 2 * b, n] = jnp.concatenate(first, axis=0).astype(jnp.bfloat16)
                bsend[f, 2 * b + 1, n] = jnp.concatenate(second, axis=0).astype(jnp.bfloat16)
        each(0, 8, pair)
        lat_ref[f, ma] = bsend[f, ma]

    def out_copy(f, u, kind):
        tile = (2 * u, 2 * u + 1, 23 - 2 * u, 24 - 2 * u)[kind]
        slot = 4 * lax.rem(u, 2) + kind
        cols = pl.ds(pl.multiple_of(tile * 128, 128), 128)
        return pltpu.make_async_copy(tiles.at[slot], out_ref.at[:, f, :, :, cols], out_sem.at[slot])

    def out_wait(f, u):
        @pl.when(u < STEPS)
        def _():
            for kind in range(3):
                out_copy(f, u, kind).wait()

        @pl.when(u > 0)
        def _():
            out_copy(f, u, 3).wait()

    def make_table(u):
        for half in range(2):
            for g in range(2):
                def rows(n, half=half, g=g):
                    r = pl.ds(pl.multiple_of(512 * g + 64 * n, 64), 64)
                    c = base[0, r, :]
                    s = base[1, r, :]
                    at = 256 * g + 128 * half
                    arecv[u, pl.ds(2 * n, 2), :, :, at:at + 128] = c.reshape(2, 2, CS, 128).astype(jnp.bfloat16)
                    arecv[u, pl.ds(2 * n, 2), :, :, 512 + at:640 + at] = (-s).reshape(2, 2, CS, 128).astype(jnp.bfloat16)
                    rc = base[2, r, :]
                    rs = base[3, r, :]
                    base[0, r, :] = c * rc - s * rs
                    base[1, r, :] = s * rc + c * rs
                each(0, 8, rows)

    left = lax.broadcasted_iota(jnp.int32, (128, 128), 1)
    back = lax.rem(128 - left, 128)

    def gather_rows(f):
        each(1, 16, lambda n: plane_arrival(f, n).wait_recv())
        for b in range(8):
            x0 = lat_ref[f, 2 * b].reshape(128, 128).astype(jnp.float32)
            x1 = lat_ref[f, 2 * b + 1].reshape(128, 128).astype(jnp.float32)
            cols = slice(128 * b, 128 * (b + 1))
            lhs[0, :, cols] = jnp.where(left < 64, x0, pltpu.roll(x1, 64, 1)).astype(jnp.bfloat16)
            lhs[1, :, cols] = jnp.where(left < 64, pltpu.roll(x0, 64, 1), x1).astype(jnp.bfloat16)

    def longitudes(f, u):
        @pl.when(u >= 2)
        def _():
            out_wait(f, u - 2)
        sums2 = []
        for c in range(2):
            acc = jnp.zeros((128, 256), jnp.float32)
            for g in range(2):
                at = 512 * c + 256 * g
                table = arecv[u, :, :, :, at:at + 256].reshape(512, 256)
                acc = acc + jnp.dot(lhs[c, :, 512 * g:512 * (g + 1)], table, preferred_element_type=jnp.float32)
            sums2.append(acc)
        plus = sums2[0] + sums2[1]
        less = sums2[0] - sums2[1]
        first, second = less[:, :128], less[:, 128:]
        slot = 4 * lax.rem(u, 2)

        def put(kind, x):
            tiles[slot + kind] = x.reshape(SEL, 2, 4, 128)
            out_copy(f, u, kind).start()

        @pl.when(u > 0)
        def _():
            put(3, jnp.where(left == 0, first, held[...]))

        @pl.when(u < STEPS)
        def _():
            put(0, plus[:, :128])
            put(1, plus[:, 128:])
            put(2, jnp.where(left == 0, second, jnp.take_along_axis(first, back, axis=1)))
            held[...] = jnp.take_along_axis(second, back, axis=1)

        @pl.when(u == STEPS)
        def _():
            out_wait(f, u - 1)
            out_wait(f, u)

    def between(k, first, last, body):
        @pl.when((k >= first) & (k < last))
        def _():
            body()

    def step(k, carry):
        def send():
            @pl.when(k >= 3)
            def _():
                each(1, 16, lambda n: a_copy(k - 3, n).wait_send())
            @pl.when((k > 0) & (k < BLOCKS))
            def _():
                make_pick(k)

            @pl.when(k > 0)
            def _():
                gather(k)
            each(1, 16, lambda n: a_copy(k, n).start())
            arecv[k, ma] = asend[lax.rem(k, 3), ma]
        between(k, 0, CHUNKS, send)

        @pl.when(k == 2)
        def _():
            make_base()
        between(k, 3, CHUNKS + 3, lambda: relay.forward(k - 3))
        between(k, 4, CHUNKS + 4, lambda: sums.forward(k - 4))
        first = jnp.where(k < 13, 2 * (k - 9), jnp.where(k == 14, 1, 4))
        count = jnp.where((k < 9) | (k == 13), 0, jnp.where(k < 13, 1, 2))

        @pl.when(k == 9)
        def _():
            gather_rows(0)
        each(first, first + count, lambda u: longitudes(jnp.where(k < 13, 0, 1), u))

        def arrive():
            c = k - 2
            each(1, 16, lambda n: a_arrival(c, n).wait_recv())
            relay.free(c)
            compact(c)
            relay.core_copy(c).start()
        between(k, 2, CHUNKS + 2, arrive)

        def transform():
            c = k - 3
            sums.free(c)
            legendre(c)
            sums.core_copy(c).start()
        between(k, 3, CHUNKS + 3, transform)
        between(k, 2, CHUNKS + 2, lambda: relay.add(k - 2))

        def settle():
            c = k - 4
            f = c // BLOCKS
            block = lax.rem(c, BLOCKS)
            rows = pl.ds(pl.multiple_of(block * 256, 256), 256)

            def store(side, total):
                latf[side, rows, :] = total.reshape(256, 128)
            sums.finish(c, store)

            @pl.when(block == BLOCKS - 1)
            def _():
                turn(f)
                each(1, 16, lambda n: plane_copy(f, n).start())
        between(k, 4, CHUNKS + 4, settle)
        between(k, 3, CHUNKS + 3, lambda: sums.add(k - 3))
        between(k, 3, 3 + STEPS + 1, lambda: make_table(k - 3))

        @pl.when(k == 13)
        def _():
            gather_rows(1)
        second = jnp.where(k < 13, 2 * (k - 9) + 1, jnp.where(k == 13, 0, 3))
        more = jnp.where((k < 9) | (k == 12) | (k == 15), 0, 1)
        each(second, second + more, lambda u: longitudes(jnp.where(k < 13, 0, 1), u))
        return carry

    make_pick(0)
    gather(0)
    pl.semaphore_wait(barrier, 18)
    lax.fori_loop(0, CHUNKS + 4, step, 0)

    longitudes(1, STEPS)
    gather_rows(2)
    each(0, STEPS + 1, lambda u: longitudes(2, u))
    relay.drain()
    sums.drain()
    for k in range(CHUNKS - 3, CHUNKS):
        each(1, 16, lambda n: a_copy(k, n).wait_send())

    def last(n):
        for f in range(FIELDS):
            plane_copy(f, n).wait_send()
    each(1, 16, last)


def flow(spec, leg, order, chosen):
    bf = jnp.bfloat16
    vm = pl.BlockSpec(memory_space=pltpu.VMEM)
    hbm = pl.BlockSpec(memory_space=pl.ANY)
    dma = pltpu.SemaphoreType.DMA
    reduce_scratch = [
        pltpu.VMEM((2, 3, 4, 2, CS, SEL, 128), bf),
        pltpu.VMEM((CHUNKS, 4, 2, CS, SEL, 128), bf),
        pltpu.VMEM((CHUNKS, 2, CS, SEL, 128), bf),
        pltpu.VMEM((CHUNKS, 2, 2, CS, SEL, 128), bf),
    ]
    return pl.pallas_call(
        flow_kernel,
        name="flow",
        out_shape=jax.ShapeDtypeStruct((SEL, FIELDS, 2, 4, NPHI), jnp.float32),
        in_specs=[hbm, hbm, vm, vm],
        out_specs=hbm,
        scratch_shapes=[
            pltpu.VMEM((2, M, M), bf),
            pltpu.VMEM((2, CS, 128, 512), bf),
            pltpu.VMEM((BLOCKS, 16 * CS, M), bf),
            pltpu.VMEM((16 * CS, 16 * CS), bf),
            pltpu.VMEM((4, M, 128), jnp.float32),
            pltpu.VMEM((FIELDS, 16, 8, 16, 128), bf),
            pltpu.VMEM((2, 128, M), bf),
            pltpu.VMEM((128, 128), jnp.float32),
            pltpu.VMEM((8, SEL, 2, 4, 128), jnp.float32),
            pltpu.VMEM((3, 16, 2, CS, M), bf),
            pltpu.VMEM((CHUNKS, 16, 2, CS, M), bf),
            pltpu.VMEM((2, CS, SEL, 128), bf),
            *reduce_scratch, *reduce_scratch,
            pltpu.VMEM((2, 1024, 128), jnp.float32),
            pltpu.VMEM((FIELDS, 16, 8, 16, 128), bf),
            dma((2,)), dma((2,)), dma((8,)),
            dma((CHUNKS, 16)), dma((CHUNKS, 16)),
            dma((FIELDS, 16)), dma((FIELDS, 16)),
            *([dma((CHUNKS,))] * 2 + [dma((CHUNKS, 2))] * 4) * 2,
        ],
        compiler_params=pltpu.CompilerParams(
            collective_id=1, has_side_effects=True, vmem_limit_bytes=67043328),
    )(spec, leg, order, chosen)


def local(spectra, legendre, selected, m_order):
    order = jnp.broadcast_to(m_order[:, None], (M, 128))
    chosen = jnp.broadcast_to(selected[:, None], (SEL, 128))
    return flow(spectra.reshape(2 * FIELDS, M, M), legendre, order, chosen)


def solution(mesh):
    rad_ma = ("rad", "ma")
    in_specs = (P(rad_ma, None, None, None, None), P("ma", "rad", None), P(), P())
    out_specs = P(None, None, None, rad_ma, None)
    return jax.shard_map(local, mesh=mesh, in_specs=in_specs, out_specs=out_specs, check_vma=False)
```

```python
import jax
import jax.numpy as jnp
from jax import lax
from jax.experimental import pallas as pl
from jax.experimental.pallas import tpu as pltpu
from jax.sharding import PartitionSpec as P

MESH = pl.DeviceIdType.MESH
M = 1024
NPHI = 3072
FIELDS = 3
SEL = 16
BLOCKS = 4
CS = 16
CHUNKS = FIELDS * BLOCKS
STEPS = NPHI // 2 // 256


def tile_copy(tiles, sems, target, u, kind):
    tile = (2 * u, 2 * u + 1, 23 - 2 * u, 24 - 2 * u)[kind]
    slot = 4 * lax.rem(u, 2) + kind
    cols = pl.ds(pl.multiple_of(tile * 128, 128), 128)
    return pltpu.make_async_copy(tiles.at[slot], target(cols), sems.at[slot])


def spread_rows(lat, lhs):
    low = lax.broadcasted_iota(jnp.int32, (128, 128), 1) < 64
    for b in range(8):
        x0 = lat(2 * b).reshape(128, 128).astype(jnp.float32)
        x1 = lat(2 * b + 1).reshape(128, 128).astype(jnp.float32)
        cols = slice(128 * b, 128 * (b + 1))
        lhs[0, :, cols] = jnp.where(low, x0, pltpu.roll(x1, 64, 1)).astype(jnp.bfloat16)
        lhs[1, :, cols] = jnp.where(low, pltpu.roll(x0, 64, 1), x1).astype(jnp.bfloat16)


def longitude_step(u, table, lhs, held, tiles, out_copy):
    lane = lax.broadcasted_iota(jnp.int32, (128, 128), 1)
    back = lax.rem(128 - lane, 128)

    def out_wait(v):
        @pl.when(v < STEPS)
        def _():
            for kind in range(3):
                out_copy(v, kind).wait()

        @pl.when(v > 0)
        def _():
            out_copy(v, 3).wait()

    @pl.when(u >= 2)
    def _():
        out_wait(u - 2)
    parts = []
    for c in range(2):
        acc = jnp.zeros((128, 256), jnp.float32)
        for g in range(2):
            at = 512 * c + 256 * g
            rows = table(slice(at, at + 256)).reshape(512, 256)
            acc = acc + jnp.dot(lhs[c, :, 512 * g:512 * (g + 1)], rows, preferred_element_type=jnp.float32)
        parts.append(acc)
    plus = parts[0] + parts[1]
    less = parts[0] - parts[1]
    first, second = less[:, :128], less[:, 128:]
    slot = 4 * lax.rem(u, 2)

    def put(kind, x):
        tiles[slot + kind] = x.reshape(SEL, 2, 4, 128)
        out_copy(u, kind).start()

    @pl.when(u > 0)
    def _():
        put(3, jnp.where(lane == 0, first, held[...]))

    @pl.when(u < STEPS)
    def _():
        put(0, plus[:, :128])
        put(1, plus[:, 128:])
        put(2, jnp.where(lane == 0, second, jnp.take_along_axis(first, back, axis=1)))
        held[...] = jnp.take_along_axis(second, back, axis=1)

    @pl.when(u == STEPS)
    def _():
        out_wait(u - 1)
        out_wait(u)


def flow_kernel(spec_ref, leg_ref, held_ref, selected_ref, out_ref, last_ref, table_ref,
                spec, leg, order_ref, pick_ref, perm_ref, base, lat_ref, lhs, held, tiles, asend, arecv, coef,
                part1, core1, up1, in1, part2, core2, up2, in2, latf, bsend,
                load, leg_load, out_sem, table_sem, last_sem, a_s, a_r, b_s, b_r, *rad_sems):
    rad = lax.axis_index("rad")
    ma = lax.axis_index("ma")
    core = lax.rem(rad, 2)
    z = rad // 2
    partner = z * 2 + 1 - core
    zu = lax.rem(z + 1, 4)
    zd = lax.rem(z + 3, 4)
    zo = lax.rem(z + 2, 4)
    up = zu * 2 + core
    down = zd * 2 + core

    def each(first, last, body):
        def run(n, carry):
            body(n)
            return carry
        lax.fori_loop(first, last, run, 0)

    def load_copy(f, c):
        return pltpu.make_async_copy(spec_ref.at[2 * f + c], spec.at[c], load.at[c])

    def leg_copy(k):
        rows = pl.ds(lax.rem(k, BLOCKS) * CS, CS)
        return pltpu.make_async_copy(leg_ref.at[rows], leg.at[lax.rem(k, 2)], leg_load.at[lax.rem(k, 2)])

    load_copy(0, 0).start()
    load_copy(0, 1).start()
    leg_copy(0).start()

    lane = lax.broadcasted_iota(jnp.int32, (16, 128), 1)
    degree = rad * 128 + lax.broadcasted_iota(jnp.int32, (1, 128), 1)
    for r in range(8):
        line = jnp.broadcast_to(held_ref[r:r + 1, :].astype(jnp.float32), (128, 128))
        order_ref[128 * r:128 * (r + 1), :] = line.T.astype(jnp.int32)
    row = lax.broadcasted_iota(jnp.int32, (16, 128), 0)
    chosen = jnp.zeros((16, 128), jnp.int32)
    for i in range(SEL):
        chosen = jnp.where(row == i, selected_ref[i], chosen)
    for j in range(CS):
        for half in range(2):
            hit = (chosen == rad * 16 + 8 * half + lane // 16) & (lax.rem(lane, 16) == j)
            perm_ref[16 * j:16 * (j + 1), 128 * half:128 * (half + 1)] = jnp.where(hit, 1.0, 0.0).astype(jnp.bfloat16)

    def make_pick(b):
        def body(a):
            held = order_ref[pl.ds(a * 64 + b * CS, CS), :]
            for n in range(8):
                hit = jnp.where(held == lane + 128 * n, 1.0, 0.0).astype(jnp.bfloat16)
                pick_ref[b, pl.ds(pl.multiple_of(a * 16, 16), 16), 128 * n:128 * (n + 1)] = hit
        each(0, 16, body)

    def make_base():
        def body(n):
            rows = pl.ds(pl.multiple_of(n * 32, 32), 32)
            held = order_ref[rows, :]
            m = held.astype(jnp.float32)
            point = lax.broadcasted_iota(jnp.int32, (32, 128), 1).astype(jnp.float32)
            weight = jnp.where(held == 0, 1.0, 2.0)
            for at, scale, where in ((m * point, weight, 0), (m * 128.0, 1.0, 2)):
                at = at - NPHI * jnp.floor(at * (1.0 / NPHI))
                angle = at * (2.0 * jnp.pi / NPHI)
                base[where, rows, :] = scale * jnp.cos(angle)
                base[where + 1, rows, :] = scale * jnp.sin(angle)
        each(0, 32, body)

    barrier = pltpu.get_barrier_semaphore()
    for d in (partner, up, down):
        pl.semaphore_signal(barrier, inc=1, device_id={"rad": d}, device_id_type=MESH)
    for n in range(1, 16):
        pl.semaphore_signal(barrier, inc=1, device_id={"ma": lax.rem(ma + n, 16)}, device_id_type=MESH)

    def a_copy(k, n):
        to = lax.rem(ma + n, 16)
        return pltpu.make_async_remote_copy(
            src_ref=asend.at[lax.rem(k, 3), to], dst_ref=arecv.at[k, ma],
            send_sem=a_s.at[k, n], recv_sem=a_r.at[k, n],
            device_id={"ma": to}, device_id_type=MESH)

    def a_arrival(k, n):
        src = lax.rem(ma + 16 - n, 16)
        return pltpu.make_async_remote_copy(
            src_ref=asend.at[lax.rem(k, 3), src], dst_ref=arecv.at[k, src],
            send_sem=a_s.at[k, n], recv_sem=a_r.at[k, n],
            device_id={"ma": src}, device_id_type=MESH)

    def plane_copy(f, n):
        to = lax.rem(ma + n, 16)
        return pltpu.make_async_remote_copy(
            src_ref=bsend.at[f, to], dst_ref=lat_ref.at[f, ma],
            send_sem=b_s.at[f, n], recv_sem=b_r.at[f, n],
            device_id={"ma": to}, device_id_type=MESH)

    def plane_arrival(f, n):
        src = lax.rem(ma + 16 - n, 16)
        return pltpu.make_async_remote_copy(
            src_ref=bsend.at[f, src], dst_ref=lat_ref.at[f, src],
            send_sem=b_s.at[f, n], recv_sem=b_r.at[f, n],
            device_id={"ma": src}, device_id_type=MESH)

    class Reduce:
        def __init__(self, part, rcore, r1, r2, sems):
            self.part, self.rcore, self.r1, self.r2 = part, rcore, r1, r2
            self.core_s, self.core_r, self.z1_s, self.z1_r, self.z2_s, self.z2_r = sems

        def core_copy(self, k):
            return pltpu.make_async_remote_copy(
                src_ref=self.part.at[1 - core, lax.rem(k, 3)], dst_ref=self.rcore.at[k],
                send_sem=self.core_s.at[k], recv_sem=self.core_r.at[k],
                device_id={"rad": partner}, device_id_type=MESH)

        def z1_copy(self, k, side):
            return pltpu.make_async_remote_copy(
                src_ref=self.rcore.at[k, zo, side], dst_ref=self.r1.at[k, side],
                send_sem=self.z1_s.at[k, side], recv_sem=self.z1_r.at[k, side],
                device_id={"rad": up if side == 0 else down}, device_id_type=MESH)

        def z2_copy(self, k, side):
            return pltpu.make_async_remote_copy(
                src_ref=self.rcore.at[k, zu if side == 0 else zd], dst_ref=self.r2.at[k, side],
                send_sem=self.z2_s.at[k, side], recv_sem=self.z2_r.at[k, side],
                device_id={"rad": up if side == 0 else down}, device_id_type=MESH)

        def free(self, k):
            @pl.when(k >= 3)
            def _():
                self.core_copy(k - 3).wait_send()

        def add(self, k):
            self.core_copy(k).wait_recv()

            def body(n):
                q = n // 2
                h = lax.rem(n, 2)
                a = self.part[core, lax.rem(k, 3), q, h].astype(jnp.float32)
                b = self.rcore[k, q, h].astype(jnp.float32)
                self.rcore[k, q, h] = (a + b).astype(jnp.bfloat16)
            each(0, 8, body)
            self.z1_copy(k, 0).start()
            self.z1_copy(k, 1).start()

        def forward(self, k):
            for side in range(2):
                self.z1_copy(k, side).wait_recv()
                q = zu if side == 0 else zd
                a = self.rcore[k, q, side].astype(jnp.float32)
                b = self.r1[k, side].astype(jnp.float32)
                self.rcore[k, q, side] = (a + b).astype(jnp.bfloat16)
                self.z2_copy(k, side).start()

        def finish(self, k, store):
            self.z2_copy(k, 0).wait_recv()
            self.z2_copy(k, 1).wait_recv()
            for side in range(2):
                total = self.rcore[k, z, side].astype(jnp.float32)
                total = total + self.r2[k, 0, side].astype(jnp.float32)
                total = total + self.r2[k, 1, side].astype(jnp.float32)
                store(side, total)

        def drain(self):
            def body(k):
                for side in range(2):
                    self.z1_copy(k, side).wait_send()
                    self.z2_copy(k, side).wait_send()
            each(0, CHUNKS, body)
            each(CHUNKS - 3, CHUNKS, lambda k: self.core_copy(k).wait_send())

    relay = Reduce(part1, core1, up1, in1, rad_sems[:6])
    sums = Reduce(part2, core2, up2, in2, rad_sems[6:])

    def gather(k):
        f = k // BLOCKS
        b = lax.rem(k, BLOCKS)
        ring = lax.rem(k, 3)

        @pl.when(b == 0)
        def _():
            load_copy(f, 0).wait()
            load_copy(f, 1).wait()

        for c in range(2):
            for n in range(4):
                cols = slice(256 * n, 256 * (n + 1))
                rows = jnp.dot(pick_ref[b], spec[c, :, cols], preferred_element_type=jnp.float32)
                asend[ring, :, c, :, cols] = rows.reshape(16, CS, 256).astype(jnp.bfloat16)

        @pl.when((b == BLOCKS - 1) & (f < FIELDS - 1))
        def _():
            load_copy(f + 1, 0).start()
            load_copy(f + 1, 1).start()

    def compact(k):
        ring = lax.rem(k, 3)
        for c in range(2):
            for n in range(4):
                cols = slice(256 * n, 256 * (n + 1))
                rows = arecv[k, :, c, :, cols].reshape(256, 256)
                got = jnp.dot(perm_ref[...], rows, preferred_element_type=jnp.float32)
                got = got.reshape(CS, 16, 256).astype(jnp.bfloat16)
                part1[0, ring, n, c] = got[:, :, :128]
                part1[1, ring, n, c] = got[:, :, 128:]

    low = lax.broadcasted_iota(jnp.int32, (32, 128), 1) < 64
    top = lax.broadcasted_iota(jnp.int32, (8, 128), 0) < 4

    def legendre(k):
        first = lax.rem(k, BLOCKS) * CS
        ring = lax.rem(k, 3)
        leg_copy(k).wait()

        @pl.when(k < CHUNKS - 1)
        def _():
            leg_copy(k + 1).start()

        def store(side, total):
            keep = degree >= order_ref[pl.ds(ma * 64 + first, CS), :]
            coef[side] = jnp.where(keep[:, None, :], total, 0.0).astype(jnp.bfloat16)
        relay.finish(k, store)

        def slot(j):
            north = jnp.concatenate([coef[0, j], coef[1, j]], axis=0)
            odd = lax.rem(order_ref[pl.ds(ma * 64 + first + j, 1), :] + degree, 2)
            south = jnp.where(odd == 1, -north.astype(jnp.float32), north.astype(jnp.float32)).astype(jnp.bfloat16)
            both = jnp.concatenate([north, south], axis=0)
            res = jnp.dot(both, leg[lax.rem(k, 2), j], preferred_element_type=jnp.float32)
            for q in range(4):
                nt = res[:32, 128 * q:128 * (q + 1)]
                st = res[32:, 128 * q:128 * (q + 1)]
                even = jnp.where(low, nt, pltpu.roll(st, 64, 1)).astype(jnp.bfloat16)
                odd = jnp.where(low, pltpu.roll(nt, 64, 1), st).astype(jnp.bfloat16)
                for side in range(2):
                    part2[0, ring, q, side, j] = even[16 * side:16 * (side + 1)]
                    part2[1, ring, q, side, j] = odd[16 * side:16 * (side + 1)]
        each(0, CS, slot)

    def turn(f):
        def pair(n):
            halves = []
            for i in (2 * n, 2 * n + 1):
                block = jnp.concatenate(
                    [latf[c, pl.ds(i, 64, stride=16), :] for c in range(2)], axis=0)
                halves.append(block.T)
            for b in range(8):
                first, second = [], []
                for x in halves:
                    nt, st = x[8 * b:8 * b + 8], x[64 + 8 * b:64 + 8 * b + 8]
                    first.append(jnp.where(top, nt, pltpu.roll(st, 4, 0)))
                    second.append(jnp.where(top, pltpu.roll(nt, 4, 0), st))
                bsend[f, 2 * b, n] = jnp.concatenate(first, axis=0).astype(jnp.bfloat16)
                bsend[f, 2 * b + 1, n] = jnp.concatenate(second, axis=0).astype(jnp.bfloat16)
        each(0, 8, pair)
        lat_ref[f, ma] = bsend[f, ma]

    def make_table(u):
        for half in range(2):
            for g in range(2):
                def rows(n, half=half, g=g):
                    r = pl.ds(pl.multiple_of(512 * g + 64 * n, 64), 64)
                    c = base[0, r, :]
                    s = base[1, r, :]
                    at = 256 * g + 128 * half
                    arecv[u, pl.ds(2 * n, 2), :, :, at:at + 128] = c.reshape(2, 2, CS, 128).astype(jnp.bfloat16)
                    arecv[u, pl.ds(2 * n, 2), :, :, 512 + at:640 + at] = (-s).reshape(2, 2, CS, 128).astype(jnp.bfloat16)
                    rc = base[2, r, :]
                    rs = base[3, r, :]
                    base[0, r, :] = c * rc - s * rs
                    base[1, r, :] = s * rc + c * rs
                each(0, 8, rows)

    def out_copy(f, u, kind):
        return tile_copy(tiles, out_sem, lambda cols: out_ref.at[:, f, :, :, cols], u, kind)

    def table_copy(u):
        return pltpu.make_async_copy(arecv.at[u], table_ref.at[u], table_sem.at[u])

    def gather_rows(f):
        each(1, 16, lambda n: plane_arrival(f, n).wait_recv())
        spread_rows(lambda a: lat_ref[f, a], lhs)

    def longitudes(f, u):
        longitude_step(u, lambda cols: arecv[u, :, :, :, cols], lhs, held, tiles,
                       lambda v, kind: out_copy(f, v, kind))

    def between(k, first, last, body):
        @pl.when((k >= first) & (k < last))
        def _():
            body()

    def step(k, carry):
        def send():
            @pl.when(k >= 3)
            def _():
                each(1, 16, lambda n: a_copy(k - 3, n).wait_send())
            @pl.when((k > 0) & (k < BLOCKS))
            def _():
                make_pick(k)

            @pl.when(k > 0)
            def _():
                gather(k)
            each(1, 16, lambda n: a_copy(k, n).start())
            arecv[k, ma] = asend[lax.rem(k, 3), ma]
        between(k, 0, CHUNKS, send)

        @pl.when(k == 2)
        def _():
            make_base()
        between(k, 3, CHUNKS + 3, lambda: relay.forward(k - 3))
        between(k, 4, CHUNKS + 4, lambda: sums.forward(k - 4))
        first = jnp.where(k < 13, 2 * (k - 9), jnp.where(k == 14, 1, 4))
        count = jnp.where((k < 9) | (k == 13), 0, jnp.where(k < 13, 1, 2))

        @pl.when(k == 9)
        def _():
            gather_rows(0)
        each(first, first + count, lambda u: longitudes(jnp.where(k < 13, 0, 1), u))

        def arrive():
            c = k - 2
            each(1, 16, lambda n: a_arrival(c, n).wait_recv())
            relay.free(c)
            compact(c)
            relay.core_copy(c).start()
        between(k, 2, CHUNKS + 2, arrive)

        def transform():
            c = k - 3
            sums.free(c)
            legendre(c)
            sums.core_copy(c).start()
        between(k, 3, CHUNKS + 3, transform)
        between(k, 2, CHUNKS + 2, lambda: relay.add(k - 2))

        def settle():
            c = k - 4
            f = c // BLOCKS
            block = lax.rem(c, BLOCKS)
            rows = pl.ds(pl.multiple_of(block * 256, 256), 256)

            def store(side, total):
                latf[side, rows, :] = total.reshape(256, 128)
            sums.finish(c, store)

            @pl.when(block == BLOCKS - 1)
            def _():
                turn(f)
                each(1, 16, lambda n: plane_copy(f, n).start())
        between(k, 4, CHUNKS + 4, settle)
        between(k, 3, CHUNKS + 3, lambda: sums.add(k - 3))

        def fill():
            make_table(k - 3)
            table_copy(k - 3).start()
        between(k, 3, 3 + STEPS + 1, fill)

        @pl.when(k == 13)
        def _():
            gather_rows(1)
        second = jnp.where(k < 13, 2 * (k - 9) + 1, jnp.where(k == 13, 0, 3))
        more = jnp.where((k < 9) | (k == 12) | (k == 15), 0, 1)
        each(second, second + more, lambda u: longitudes(jnp.where(k < 13, 0, 1), u))
        return carry

    make_pick(0)
    gather(0)
    pl.semaphore_wait(barrier, 18)
    lax.fori_loop(0, CHUNKS + 4, step, 0)

    longitudes(1, STEPS)
    each(1, 16, lambda n: plane_arrival(2, n).wait_recv())
    last_copy = pltpu.make_async_copy(lat_ref.at[2], last_ref, last_sem)
    last_copy.start()
    last_copy.wait()
    each(0, STEPS + 1, lambda u: table_copy(u).wait())
    relay.drain()
    sums.drain()
    for k in range(CHUNKS - 3, CHUNKS):
        each(1, 16, lambda n: a_copy(k, n).wait_send())

    def last(n):
        for f in range(FIELDS):
            plane_copy(f, n).wait_send()
    each(1, 16, last)


def flow(spec, leg, order, chosen):
    bf = jnp.bfloat16
    vm = pl.BlockSpec(memory_space=pltpu.VMEM)
    hbm = pl.BlockSpec(memory_space=pl.ANY)
    dma = pltpu.SemaphoreType.DMA
    reduce_scratch = [
        pltpu.VMEM((2, 3, 4, 2, CS, SEL, 128), bf),
        pltpu.VMEM((CHUNKS, 4, 2, CS, SEL, 128), bf),
        pltpu.VMEM((CHUNKS, 2, CS, SEL, 128), bf),
        pltpu.VMEM((CHUNKS, 2, 2, CS, SEL, 128), bf),
    ]
    return pl.pallas_call(
        flow_kernel,
        name="flow",
        out_shape=[jax.ShapeDtypeStruct((SEL, FIELDS - 1, 2, 4, NPHI), jnp.float32),
                   jax.ShapeDtypeStruct((16, 8, 16, 128), bf),
                   jax.ShapeDtypeStruct((STEPS + 1, 16, 2, CS, M), bf)],
        in_specs=[hbm, hbm, vm, pl.BlockSpec(memory_space=pltpu.SMEM)],
        out_specs=[hbm, hbm, hbm],
        scratch_shapes=[
            pltpu.VMEM((2, M, M), bf),
            pltpu.VMEM((2, CS, 128, 512), bf),
            pltpu.VMEM((M, 128), jnp.int32),
            pltpu.VMEM((BLOCKS, 16 * CS, M), bf),
            pltpu.VMEM((16 * CS, 16 * CS), bf),
            pltpu.VMEM((4, M, 128), jnp.float32),
            pltpu.VMEM((FIELDS, 16, 8, 16, 128), bf),
            pltpu.VMEM((2, 128, M), bf),
            pltpu.VMEM((128, 128), jnp.float32),
            pltpu.VMEM((8, SEL, 2, 4, 128), jnp.float32),
            pltpu.VMEM((3, 16, 2, CS, M), bf),
            pltpu.VMEM((CHUNKS, 16, 2, CS, M), bf),
            pltpu.VMEM((2, CS, SEL, 128), bf),
            *reduce_scratch, *reduce_scratch,
            pltpu.VMEM((2, 1024, 128), jnp.float32),
            pltpu.VMEM((FIELDS, 16, 8, 16, 128), bf),
            dma((2,)), dma((2,)), dma((8,)), dma((STEPS + 1,)), dma(()),
            dma((CHUNKS, 16)), dma((CHUNKS, 16)),
            dma((FIELDS, 16)), dma((FIELDS, 16)),
            *([dma((CHUNKS,))] * 2 + [dma((CHUNKS, 2))] * 4) * 2,
        ],
        compiler_params=pltpu.CompilerParams(
            collective_id=1, has_side_effects=True, vmem_limit_bytes=67043328),
    )(spec, leg, order, chosen)


def last_kernel(done_ref, lat_ref, table_ref, out_ref, moved, tables, lhs, held, tiles, in_sem, back_sem, table_sem, out_sem):
    def move_in(n):
        return pltpu.make_async_copy(done_ref.at[pl.ds(4 * n, 4)], moved.at[pl.ds(4 * n, 4)], in_sem.at[n])

    def move_out(n):
        return pltpu.make_async_copy(moved.at[pl.ds(4 * n, 4)], out_ref.at[pl.ds(4 * n, 4), :2], back_sem.at[n])

    def table_copy(u):
        return pltpu.make_async_copy(table_ref.at[u], tables.at[u], table_sem.at[u])

    table_copy(0).start()
    for u in range(1, STEPS + 1):
        if u <= 4:
            move_in(u - 1).start()
        table_copy(u).start()
    spread_rows(lambda a: lat_ref[a], lhs)

    def step(u, carry):
        table_copy(u).wait()

        @pl.when((u >= 1) & (u < 5))
        def _():
            move_in(u - 1).wait()
            move_out(u - 1).start()
        longitude_step(u, lambda cols: tables[u, :, :, :, cols], lhs, held, tiles,
                       lambda v, kind: tile_copy(tiles, out_sem, lambda c: out_ref.at[:, 2, :, :, c], v, kind))
        return carry
    lax.fori_loop(0, STEPS + 1, step, 0)
    for n in range(4):
        move_out(n).wait()


def last(done, lat, tables):
    bf = jnp.bfloat16
    hbm = pl.BlockSpec(memory_space=pl.ANY)
    dma = pltpu.SemaphoreType.DMA
    return pl.pallas_call(
        last_kernel,
        name="last",
        out_shape=jax.ShapeDtypeStruct((SEL, FIELDS, 2, 4, NPHI), jnp.float32),
        in_specs=[hbm, pl.BlockSpec(memory_space=pltpu.VMEM), hbm],
        out_specs=hbm,
        scratch_shapes=[
            pltpu.VMEM((SEL, FIELDS - 1, 2, 4, NPHI), jnp.float32),
            pltpu.VMEM((STEPS + 1, 16, 2, CS, M), bf),
            pltpu.VMEM((2, 128, M), bf),
            pltpu.VMEM((128, 128), jnp.float32),
            pltpu.VMEM((8, SEL, 2, 4, 128), jnp.float32),
            dma((4,)), dma((4,)), dma((STEPS + 1,)), dma((8,)),
        ],
        compiler_params=pltpu.CompilerParams(vmem_limit_bytes=60 * 1024 * 1024),
    )(done, lat, tables)


def local(spectra, legendre, selected, m_order):
    return last(*flow(spectra.reshape(2 * FIELDS, M, M), legendre, m_order.reshape(8, 128), selected))


def solution(mesh):
    rad_ma = ("rad", "ma")
    in_specs = (P(rad_ma, None, None, None, None), P("ma", "rad", None), P(), P())
    out_specs = P(None, None, None, rad_ma, None)
    return jax.shard_map(local, mesh=mesh, in_specs=in_specs, out_specs=out_specs, check_vma=False)
```

```python
import jax
import jax.numpy as jnp
from jax import lax
from jax.experimental import pallas as pl
from jax.experimental.pallas import tpu as pltpu
from jax.sharding import PartitionSpec as P

MESH = pl.DeviceIdType.MESH
M = 1024
NPHI = 3072
FIELDS = 3
SEL = 16
BLOCKS = 4
CS = 16
CHUNKS = FIELDS * BLOCKS
STEPS = NPHI // 2 // 256
HALVES = 2 * FIELDS


def tile_copy(tiles, sems, target, u, kind):
    tile = (2 * u, 2 * u + 1, 23 - 2 * u, 24 - 2 * u)[kind]
    slot = 4 * lax.rem(u, 2) + kind
    cols = pl.ds(pl.multiple_of(tile * 128, 128), 128)
    return pltpu.make_async_copy(tiles.at[slot], target(cols), sems.at[slot])


def spread_rows(lat, lhs):
    quarter = lax.broadcasted_iota(jnp.int32, (64, 128), 1) // 32
    for b in range(8):
        held = [lat(n % 2, 2 * b + n // 2).reshape(64, 128).astype(jnp.float32) for n in range(4)]
        for c in range(2):
            pair = []
            for odd in range(2):
                row = None
                for n in range(4):
                    shift = (32 * n - 64 * odd - 32 * c) % 128
                    piece = pltpu.roll(held[n], shift, 1) if shift else held[n]
                    row = piece if row is None else jnp.where(quarter == n, piece, row)
                pair.append(row)
            rows = [pair[n % 2][8 * (n // 2):8 * (n // 2) + 8] for n in range(16)]
            lhs[c, :, 128 * b:128 * (b + 1)] = jnp.concatenate(rows, axis=0).astype(jnp.bfloat16)


def longitude_step(u, table, lhs, held, tiles, out_copy):
    lane = lax.broadcasted_iota(jnp.int32, (128, 128), 1)
    back = lax.rem(128 - lane, 128)

    def out_wait(v):
        @pl.when(v < STEPS)
        def _():
            for kind in range(3):
                out_copy(v, kind).wait()

        @pl.when(v > 0)
        def _():
            out_copy(v, 3).wait()

    @pl.when(u >= 2)
    def _():
        out_wait(u - 2)
    parts = []
    for c in range(2):
        acc = jnp.zeros((128, 256), jnp.float32)
        for g in range(2):
            at = 512 * c + 256 * g
            rows = table(slice(at, at + 256)).reshape(512, 256)
            acc = acc + jnp.dot(lhs[c, :, 512 * g:512 * (g + 1)], rows, preferred_element_type=jnp.float32)
        parts.append(acc)
    plus = parts[0] + parts[1]
    less = parts[0] - parts[1]
    first, second = less[:, :128], less[:, 128:]
    slot = 4 * lax.rem(u, 2)

    def put(kind, x):
        tiles[slot + kind] = x.reshape(SEL, 2, 4, 128)
        out_copy(u, kind).start()

    @pl.when(u > 0)
    def _():
        put(3, jnp.where(lane == 0, first, held[...]))

    @pl.when(u < STEPS)
    def _():
        put(0, plus[:, :128])
        put(1, plus[:, 128:])
        put(2, jnp.where(lane == 0, second, jnp.take_along_axis(first, back, axis=1)))
        held[...] = jnp.take_along_axis(second, back, axis=1)

    @pl.when(u == STEPS)
    def _():
        out_wait(u - 1)
        out_wait(u)


def flow_kernel(spec_ref, leg_ref, held_ref, selected_ref, out_ref, last_ref, table_ref,
                spec, leg, order_ref, pick_ref, perm_ref, base, lat_ref, lhs, held, tiles, asend, arecv, coef,
                part1, core1, up1, in1, part2, core2, up2, in2, latf, bsend,
                load, leg_load, out_sem, table_sem, last_sem, a_s, a_r, b_s, b_r, *rad_sems):
    rad = lax.axis_index("rad")
    ma = lax.axis_index("ma")
    core = lax.rem(rad, 2)
    z = rad // 2
    partner = z * 2 + 1 - core
    zu = lax.rem(z + 1, 4)
    zd = lax.rem(z + 3, 4)
    zo = lax.rem(z + 2, 4)
    up = zu * 2 + core
    down = zd * 2 + core

    def each(first, last, body):
        def run(n, carry):
            body(n)
            return carry
        lax.fori_loop(first, last, run, 0)

    def load_copy(f, c):
        return pltpu.make_async_copy(spec_ref.at[2 * f + c], spec.at[c], load.at[c])

    def leg_copy(k):
        rows = pl.ds(lax.rem(k, BLOCKS) * CS, CS)
        return pltpu.make_async_copy(leg_ref.at[rows], leg.at[lax.rem(k, 2)], leg_load.at[lax.rem(k, 2)])

    load_copy(0, 0).start()
    load_copy(0, 1).start()
    leg_copy(0).start()

    lane = lax.broadcasted_iota(jnp.int32, (16, 128), 1)
    degree = rad * 128 + lax.broadcasted_iota(jnp.int32, (1, 128), 1)
    for r in range(8):
        line = jnp.broadcast_to(held_ref[r:r + 1, :].astype(jnp.float32), (128, 128))
        order_ref[128 * r:128 * (r + 1), :] = line.T.astype(jnp.int32)
    row = lax.broadcasted_iota(jnp.int32, (16, 128), 0)
    chosen = jnp.zeros((16, 128), jnp.int32)
    for i in range(SEL):
        chosen = jnp.where(row == i, selected_ref[i], chosen)
    for j in range(CS):
        for half in range(2):
            hit = (chosen == rad * 16 + 8 * half + lane // 16) & (lax.rem(lane, 16) == j)
            perm_ref[16 * j:16 * (j + 1), 128 * half:128 * (half + 1)] = jnp.where(hit, 1.0, 0.0).astype(jnp.bfloat16)

    def make_pick(b):
        def body(a):
            held = order_ref[pl.ds(a * 64 + b * CS, CS), :]
            for n in range(8):
                hit = jnp.where(held == lane + 128 * n, 1.0, 0.0).astype(jnp.bfloat16)
                pick_ref[b, pl.ds(pl.multiple_of(a * 16, 16), 16), 128 * n:128 * (n + 1)] = hit
        each(0, 16, body)

    def make_base():
        def body(n):
            rows = pl.ds(pl.multiple_of(n * 32, 32), 32)
            held = order_ref[rows, :]
            m = held.astype(jnp.float32)
            point = lax.broadcasted_iota(jnp.int32, (32, 128), 1).astype(jnp.float32)
            weight = jnp.where(held == 0, 1.0, 2.0)
            for at, scale, where in ((m * point, weight, 0), (m * 128.0, 1.0, 2)):
                at = at - NPHI * jnp.floor(at * (1.0 / NPHI))
                angle = at * (2.0 * jnp.pi / NPHI)
                base[where, rows, :] = scale * jnp.cos(angle)
                base[where + 1, rows, :] = scale * jnp.sin(angle)
        each(0, 32, body)

    barrier = pltpu.get_barrier_semaphore()
    for d in (partner, up, down):
        pl.semaphore_signal(barrier, inc=1, device_id={"rad": d}, device_id_type=MESH)
    for n in range(1, 16):
        pl.semaphore_signal(barrier, inc=1, device_id={"ma": lax.rem(ma + n, 16)}, device_id_type=MESH)

    def a_copy(k, n):
        to = lax.rem(ma + n, 16)
        return pltpu.make_async_remote_copy(
            src_ref=asend.at[lax.rem(k, 3), to], dst_ref=arecv.at[k, ma],
            send_sem=a_s.at[k, n], recv_sem=a_r.at[k, n],
            device_id={"ma": to}, device_id_type=MESH)

    def a_arrival(k, n):
        src = lax.rem(ma + 16 - n, 16)
        return pltpu.make_async_remote_copy(
            src_ref=asend.at[lax.rem(k, 3), src], dst_ref=arecv.at[k, src],
            send_sem=a_s.at[k, n], recv_sem=a_r.at[k, n],
            device_id={"ma": src}, device_id_type=MESH)

    def plane_copy(f, n):
        to = lax.rem(ma + n, 16)
        return pltpu.make_async_remote_copy(
            src_ref=bsend.at[f, to], dst_ref=lat_ref.at[f, ma],
            send_sem=b_s.at[f, n], recv_sem=b_r.at[f, n],
            device_id={"ma": to}, device_id_type=MESH)

    def plane_arrival(f, n):
        src = lax.rem(ma + 16 - n, 16)
        return pltpu.make_async_remote_copy(
            src_ref=bsend.at[f, src], dst_ref=lat_ref.at[f, src],
            send_sem=b_s.at[f, n], recv_sem=b_r.at[f, n],
            device_id={"ma": src}, device_id_type=MESH)

    class Reduce:
        def __init__(self, part, rcore, r1, r2, sems):
            self.part, self.rcore, self.r1, self.r2 = part, rcore, r1, r2
            self.core_s, self.core_r, self.z1_s, self.z1_r, self.z2_s, self.z2_r = sems

        def core_copy(self, k):
            return pltpu.make_async_remote_copy(
                src_ref=self.part.at[1 - core, lax.rem(k, 3)], dst_ref=self.rcore.at[k],
                send_sem=self.core_s.at[k], recv_sem=self.core_r.at[k],
                device_id={"rad": partner}, device_id_type=MESH)

        def z1_copy(self, k, side):
            return pltpu.make_async_remote_copy(
                src_ref=self.rcore.at[k, zo, side], dst_ref=self.r1.at[k, side],
                send_sem=self.z1_s.at[k, side], recv_sem=self.z1_r.at[k, side],
                device_id={"rad": up if side == 0 else down}, device_id_type=MESH)

        def z2_copy(self, k, side):
            return pltpu.make_async_remote_copy(
                src_ref=self.rcore.at[k, zu if side == 0 else zd], dst_ref=self.r2.at[k, side],
                send_sem=self.z2_s.at[k, side], recv_sem=self.z2_r.at[k, side],
                device_id={"rad": up if side == 0 else down}, device_id_type=MESH)

        def free(self, k):
            @pl.when(k >= 3)
            def _():
                self.core_copy(k - 3).wait_send()

        def add(self, k):
            self.core_copy(k).wait_recv()

            def body(n):
                q = n // 2
                h = lax.rem(n, 2)
                a = self.part[core, lax.rem(k, 3), q, h].astype(jnp.float32)
                b = self.rcore[k, q, h].astype(jnp.float32)
                self.rcore[k, q, h] = (a + b).astype(jnp.bfloat16)
            each(0, 8, body)
            self.z1_copy(k, 0).start()
            self.z1_copy(k, 1).start()

        def forward(self, k):
            for side in range(2):
                self.z1_copy(k, side).wait_recv()
                q = zu if side == 0 else zd
                a = self.rcore[k, q, side].astype(jnp.float32)
                b = self.r1[k, side].astype(jnp.float32)
                self.rcore[k, q, side] = (a + b).astype(jnp.bfloat16)
                self.z2_copy(k, side).start()

        def finish(self, k, store):
            self.z2_copy(k, 0).wait_recv()
            self.z2_copy(k, 1).wait_recv()
            for side in range(2):
                total = self.rcore[k, z, side].astype(jnp.float32)
                total = total + self.r2[k, 0, side].astype(jnp.float32)
                total = total + self.r2[k, 1, side].astype(jnp.float32)
                store(side, total)

        def drain(self):
            def body(k):
                for side in range(2):
                    self.z1_copy(k, side).wait_send()
                    self.z2_copy(k, side).wait_send()
            each(0, CHUNKS, body)
            each(CHUNKS - 3, CHUNKS, lambda k: self.core_copy(k).wait_send())

    relay = Reduce(part1, core1, up1, in1, rad_sems[:6])
    sums = Reduce(part2, core2, up2, in2, rad_sems[6:])

    def gather(k):
        f = k // BLOCKS
        b = lax.rem(k, BLOCKS)
        ring = lax.rem(k, 3)

        @pl.when(b == 0)
        def _():
            load_copy(f, 0).wait()
            load_copy(f, 1).wait()

        for c in range(2):
            for n in range(4):
                cols = slice(256 * n, 256 * (n + 1))
                rows = jnp.dot(pick_ref[b], spec[c, :, cols], preferred_element_type=jnp.float32)
                asend[ring, :, c, :, cols] = rows.reshape(16, CS, 256).astype(jnp.bfloat16)

        @pl.when((b == BLOCKS - 1) & (f < FIELDS - 1))
        def _():
            load_copy(f + 1, 0).start()
            load_copy(f + 1, 1).start()

    def compact(k):
        ring = lax.rem(k, 3)
        for c in range(2):
            for n in range(4):
                cols = slice(256 * n, 256 * (n + 1))
                rows = arecv[k, :, c, :, cols].reshape(256, 256)
                got = jnp.dot(perm_ref[...], rows, preferred_element_type=jnp.float32)
                got = got.reshape(CS, 16, 256).astype(jnp.bfloat16)
                part1[0, ring, n, c] = got[:, :, :128]
                part1[1, ring, n, c] = got[:, :, 128:]

    low = lax.broadcasted_iota(jnp.int32, (32, 128), 1) < 64
    top = lax.broadcasted_iota(jnp.int32, (8, 128), 0) < 4

    def legendre(k):
        first = lax.rem(k, BLOCKS) * CS
        ring = lax.rem(k, 3)
        leg_copy(k).wait()

        @pl.when(k < CHUNKS - 1)
        def _():
            leg_copy(k + 1).start()

        def store(side, total):
            keep = degree >= order_ref[pl.ds(ma * 64 + first, CS), :]
            coef[side] = jnp.where(keep[:, None, :], total, 0.0).astype(jnp.bfloat16)
        relay.finish(k, store)

        def slot(j):
            north = jnp.concatenate([coef[0, j], coef[1, j]], axis=0)
            odd = lax.rem(order_ref[pl.ds(ma * 64 + first + j, 1), :] + degree, 2)
            south = jnp.where(odd == 1, -north.astype(jnp.float32), north.astype(jnp.float32)).astype(jnp.bfloat16)
            both = jnp.concatenate([north, south], axis=0)
            res = jnp.dot(both, leg[lax.rem(k, 2), j], preferred_element_type=jnp.float32)
            for q in range(4):
                nt = res[:32, 128 * q:128 * (q + 1)]
                st = res[32:, 128 * q:128 * (q + 1)]
                even = jnp.where(low, nt, pltpu.roll(st, 64, 1)).astype(jnp.bfloat16)
                odd = jnp.where(low, pltpu.roll(nt, 64, 1), st).astype(jnp.bfloat16)
                for side in range(2):
                    part2[0, ring, q, side, j] = even[16 * side:16 * (side + 1)]
                    part2[1, ring, q, side, j] = odd[16 * side:16 * (side + 1)]
        each(0, CS, slot)

    def turn(half):
        def quad(n):
            turned = []
            for i in (4 * n, 4 * n + 2):
                block = jnp.concatenate(
                    [latf[c, pl.ds(i + odd, 32, stride=16), :] for odd in range(2) for c in range(2)], axis=0)
                turned.append(block.T)
            for b in range(8):
                first, second = [], []
                for x in turned:
                    nt, st = x[8 * b:8 * b + 8], x[64 + 8 * b:64 + 8 * b + 8]
                    first.append(jnp.where(top, nt, pltpu.roll(st, 4, 0)))
                    second.append(jnp.where(top, pltpu.roll(nt, 4, 0), st))
                bsend[half, 2 * b, n] = jnp.concatenate(first, axis=0).astype(jnp.bfloat16)
                bsend[half, 2 * b + 1, n] = jnp.concatenate(second, axis=0).astype(jnp.bfloat16)
        each(0, 4, quad)
        lat_ref[half, ma] = bsend[half, ma]

    def make_table(u):
        for half in range(2):
            for g in range(2):
                def rows(n, half=half, g=g):
                    r = pl.ds(pl.multiple_of(512 * g + 64 * n, 64), 64)
                    c = base[0, r, :]
                    s = base[1, r, :]
                    at = 256 * g + 128 * half
                    arecv[u, pl.ds(2 * n, 2), :, :, at:at + 128] = c.reshape(2, 2, CS, 128).astype(jnp.bfloat16)
                    arecv[u, pl.ds(2 * n, 2), :, :, 512 + at:640 + at] = (-s).reshape(2, 2, CS, 128).astype(jnp.bfloat16)
                    rc = base[2, r, :]
                    rs = base[3, r, :]
                    base[0, r, :] = c * rc - s * rs
                    base[1, r, :] = s * rc + c * rs
                each(0, 8, rows)

    def out_copy(f, u, kind):
        return tile_copy(tiles, out_sem, lambda cols: out_ref.at[:, f, :, :, cols], u, kind)

    def table_copy(u):
        return pltpu.make_async_copy(arecv.at[u], table_ref.at[u], table_sem.at[u])

    def gather_rows(f):
        for half in range(2):
            each(1, 16, lambda n: plane_arrival(2 * f + half, n).wait_recv())
        spread_rows(lambda half, a: lat_ref[2 * f + half, a], lhs)

    def longitudes(f, u):
        longitude_step(u, lambda cols: arecv[u, :, :, :, cols], lhs, held, tiles,
                       lambda v, kind: out_copy(f, v, kind))

    def between(k, first, last, body):
        @pl.when((k >= first) & (k < last))
        def _():
            body()

    def step(k, carry):
        def send():
            @pl.when(k >= 3)
            def _():
                each(1, 16, lambda n: a_copy(k - 3, n).wait_send())
            @pl.when((k > 0) & (k < BLOCKS))
            def _():
                make_pick(k)

            @pl.when(k > 0)
            def _():
                gather(k)
            each(1, 16, lambda n: a_copy(k, n).start())
            arecv[k, ma] = asend[lax.rem(k, 3), ma]
        between(k, 0, CHUNKS, send)

        @pl.when(k == 2)
        def _():
            make_base()
        between(k, 3, CHUNKS + 3, lambda: relay.forward(k - 3))
        between(k, 5, CHUNKS + 5, lambda: sums.forward(k - 5))
        first = jnp.where(k < 14, 2 * (k - 10), jnp.where(k == 15, 1, 4))
        count = jnp.where((k < 10) | (k == 14), 0, jnp.where(k < 14, 1, 2))

        @pl.when(k == 10)
        def _():
            gather_rows(0)
        each(first, first + count, lambda u: longitudes(jnp.where(k < 14, 0, 1), u))

        def arrive():
            c = k - 2
            each(1, 16, lambda n: a_arrival(c, n).wait_recv())
            relay.free(c)
            compact(c)
            relay.core_copy(c).start()
        between(k, 2, CHUNKS + 2, arrive)

        def transform():
            c = k - 4
            sums.free(c)
            legendre(c)
            sums.core_copy(c).start()
        between(k, 4, CHUNKS + 4, transform)
        between(k, 2, CHUNKS + 2, lambda: relay.add(k - 2))

        def settle():
            c = k - 5
            half = c // 2
            rows = pl.ds(pl.multiple_of(lax.rem(c, 2) * 256, 256), 256)

            def store(side, total):
                latf[side, rows, :] = total.reshape(256, 128)
            sums.finish(c, store)

            @pl.when(lax.rem(c, 2) == 1)
            def _():
                turn(half)
                each(1, 16, lambda n: plane_copy(half, n).start())
        between(k, 5, CHUNKS + 5, settle)
        between(k, 4, CHUNKS + 4, lambda: sums.add(k - 4))

        def fill():
            make_table(k - 3)
            table_copy(k - 3).start()
        between(k, 3, 3 + STEPS + 1, fill)

        @pl.when(k == 14)
        def _():
            gather_rows(1)
        second = jnp.where(k < 14, 2 * (k - 10) + 1, jnp.where(k == 14, 0, 3))
        more = jnp.where((k < 10) | (k == 13) | (k == 16), 0, 1)
        each(second, second + more, lambda u: longitudes(jnp.where(k < 14, 0, 1), u))
        return carry

    make_pick(0)
    gather(0)
    pl.semaphore_wait(barrier, 18)
    lax.fori_loop(0, CHUNKS + 5, step, 0)

    longitudes(1, STEPS)
    for half in (HALVES - 2, HALVES - 1):
        each(1, 16, lambda n: plane_arrival(half, n).wait_recv())
    last_copy = pltpu.make_async_copy(lat_ref.at[pl.ds(HALVES - 2, 2)], last_ref, last_sem)
    last_copy.start()
    last_copy.wait()
    each(0, STEPS + 1, lambda u: table_copy(u).wait())
    relay.drain()
    sums.drain()
    for k in range(CHUNKS - 3, CHUNKS):
        each(1, 16, lambda n: a_copy(k, n).wait_send())

    def last(n):
        for half in range(HALVES):
            plane_copy(half, n).wait_send()
    each(1, 16, last)


def flow(spec, leg, order, chosen):
    bf = jnp.bfloat16
    vm = pl.BlockSpec(memory_space=pltpu.VMEM)
    hbm = pl.BlockSpec(memory_space=pl.ANY)
    dma = pltpu.SemaphoreType.DMA
    reduce_scratch = [
        pltpu.VMEM((2, 3, 4, 2, CS, SEL, 128), bf),
        pltpu.VMEM((CHUNKS, 4, 2, CS, SEL, 128), bf),
        pltpu.VMEM((CHUNKS, 2, CS, SEL, 128), bf),
        pltpu.VMEM((CHUNKS, 2, 2, CS, SEL, 128), bf),
    ]
    return pl.pallas_call(
        flow_kernel,
        name="flow",
        out_shape=[jax.ShapeDtypeStruct((SEL, FIELDS - 1, 2, 4, NPHI), jnp.float32),
                   jax.ShapeDtypeStruct((2, 16, 4, 16, 128), bf),
                   jax.ShapeDtypeStruct((STEPS + 1, 16, 2, CS, M), bf)],
        in_specs=[hbm, hbm, vm, pl.BlockSpec(memory_space=pltpu.SMEM)],
        out_specs=[hbm, hbm, hbm],
        scratch_shapes=[
            pltpu.VMEM((2, M, M), bf),
            pltpu.VMEM((2, CS, 128, 512), bf),
            pltpu.VMEM((M, 128), jnp.int32),
            pltpu.VMEM((BLOCKS, 16 * CS, M), bf),
            pltpu.VMEM((16 * CS, 16 * CS), bf),
            pltpu.VMEM((4, M, 128), jnp.float32),
            pltpu.VMEM((HALVES, 16, 4, 16, 128), bf),
            pltpu.VMEM((2, 128, M), bf),
            pltpu.VMEM((128, 128), jnp.float32),
            pltpu.VMEM((8, SEL, 2, 4, 128), jnp.float32),
            pltpu.VMEM((3, 16, 2, CS, M), bf),
            pltpu.VMEM((CHUNKS, 16, 2, CS, M), bf),
            pltpu.VMEM((2, CS, SEL, 128), bf),
            *reduce_scratch, *reduce_scratch,
            pltpu.VMEM((2, 512, 128), jnp.float32),
            pltpu.VMEM((HALVES, 16, 4, 16, 128), bf),
            dma((2,)), dma((2,)), dma((8,)), dma((STEPS + 1,)), dma(()),
            dma((CHUNKS, 16)), dma((CHUNKS, 16)),
            dma((HALVES, 16)), dma((HALVES, 16)),
            *([dma((CHUNKS,))] * 2 + [dma((CHUNKS, 2))] * 4) * 2,
        ],
        compiler_params=pltpu.CompilerParams(
            collective_id=1, has_side_effects=True, vmem_limit_bytes=67043328),
    )(spec, leg, order, chosen)


def last_kernel(done_ref, lat_ref, table_ref, out_ref, moved, tables, lhs, held, tiles, in_sem, back_sem, table_sem, out_sem):
    def move_in(n):
        return pltpu.make_async_copy(done_ref.at[pl.ds(4 * n, 4)], moved.at[pl.ds(4 * n, 4)], in_sem.at[n])

    def move_out(n):
        return pltpu.make_async_copy(moved.at[pl.ds(4 * n, 4)], out_ref.at[pl.ds(4 * n, 4), :2], back_sem.at[n])

    def table_copy(u):
        return pltpu.make_async_copy(table_ref.at[u], tables.at[u], table_sem.at[u])

    table_copy(0).start()
    for u in range(1, STEPS + 1):
        if u <= 4:
            move_in(u - 1).start()
        table_copy(u).start()
    spread_rows(lambda half, a: lat_ref[half, a], lhs)

    def step(u, carry):
        table_copy(u).wait()

        @pl.when((u >= 1) & (u < 5))
        def _():
            move_in(u - 1).wait()
            move_out(u - 1).start()
        longitude_step(u, lambda cols: tables[u, :, :, :, cols], lhs, held, tiles,
                       lambda v, kind: tile_copy(tiles, out_sem, lambda c: out_ref.at[:, 2, :, :, c], v, kind))
        return carry
    lax.fori_loop(0, STEPS + 1, step, 0)
    for n in range(4):
        move_out(n).wait()


def last(done, lat, tables):
    bf = jnp.bfloat16
    hbm = pl.BlockSpec(memory_space=pl.ANY)
    dma = pltpu.SemaphoreType.DMA
    return pl.pallas_call(
        last_kernel,
        name="last",
        out_shape=jax.ShapeDtypeStruct((SEL, FIELDS, 2, 4, NPHI), jnp.float32),
        in_specs=[hbm, pl.BlockSpec(memory_space=pltpu.VMEM), hbm],
        out_specs=hbm,
        scratch_shapes=[
            pltpu.VMEM((SEL, FIELDS - 1, 2, 4, NPHI), jnp.float32),
            pltpu.VMEM((STEPS + 1, 16, 2, CS, M), bf),
            pltpu.VMEM((2, 128, M), bf),
            pltpu.VMEM((128, 128), jnp.float32),
            pltpu.VMEM((8, SEL, 2, 4, 128), jnp.float32),
            dma((4,)), dma((4,)), dma((STEPS + 1,)), dma((8,)),
        ],
        compiler_params=pltpu.CompilerParams(vmem_limit_bytes=60 * 1024 * 1024),
    )(done, lat, tables)


def local(spectra, legendre, selected, m_order):
    return last(*flow(spectra.reshape(2 * FIELDS, M, M), legendre, m_order.reshape(8, 128), selected))


def solution(mesh):
    rad_ma = ("rad", "ma")
    in_specs = (P(rad_ma, None, None, None, None), P("ma", "rad", None), P(), P())
    out_specs = P(None, None, None, rad_ma, None)
    return jax.shard_map(local, mesh=mesh, in_specs=in_specs, out_specs=out_specs, check_vma=False)
```

```python
import jax
import jax.numpy as jnp
from jax import lax
from jax.experimental import pallas as pl
from jax.experimental.pallas import tpu as pltpu
from jax.sharding import PartitionSpec as P

MESH = pl.DeviceIdType.MESH
M = 1024
NPHI = 3072
FIELDS = 3
SEL = 16
BLOCKS = 4
CS = 16
CHUNKS = FIELDS * BLOCKS
STEPS = NPHI // 2 // 256
HALVES = 2 * FIELDS


def tile_copy(tiles, sems, target, u, kind):
    tile = (2 * u, 2 * u + 1, 23 - 2 * u, 24 - 2 * u)[kind]
    slot = 4 * lax.rem(u, 2) + kind
    cols = pl.ds(pl.multiple_of(tile * 128, 128), 128)
    return pltpu.make_async_copy(tiles.at[slot], target(cols), sems.at[slot])


def spread_rows(lat, lhs):
    quarter = lax.broadcasted_iota(jnp.int32, (64, 128), 1) // 32
    for b in range(8):
        held = [lat(n % 2, 2 * b + n // 2).reshape(64, 128).astype(jnp.float32) for n in range(4)]
        for c in range(2):
            pair = []
            for odd in range(2):
                row = None
                for n in range(4):
                    shift = (32 * n - 64 * odd - 32 * c) % 128
                    piece = pltpu.roll(held[n], shift, 1) if shift else held[n]
                    row = piece if row is None else jnp.where(quarter == n, piece, row)
                pair.append(row)
            rows = [pair[n % 2][8 * (n // 2):8 * (n // 2) + 8] for n in range(16)]
            lhs[c, :, 128 * b:128 * (b + 1)] = jnp.concatenate(rows, axis=0).astype(jnp.bfloat16)


def longitude_step(u, table, lhs, held, tiles, out_copy):
    lane = lax.broadcasted_iota(jnp.int32, (128, 128), 1)
    back = lax.rem(128 - lane, 128)

    def out_wait(v):
        @pl.when(v < STEPS)
        def _():
            for kind in range(3):
                out_copy(v, kind).wait()

        @pl.when(v > 0)
        def _():
            out_copy(v, 3).wait()

    @pl.when(u >= 2)
    def _():
        out_wait(u - 2)
    parts = []
    for c in range(2):
        acc = jnp.zeros((128, 256), jnp.float32)
        for g in range(2):
            at = 512 * c + 256 * g
            rows = table(slice(at, at + 256)).reshape(512, 256)
            acc = acc + jnp.dot(lhs[c, :, 512 * g:512 * (g + 1)], rows, preferred_element_type=jnp.float32)
        parts.append(acc)
    plus = parts[0] + parts[1]
    less = parts[0] - parts[1]
    first, second = less[:, :128], less[:, 128:]
    slot = 4 * lax.rem(u, 2)

    def put(kind, x):
        tiles[slot + kind] = x.reshape(SEL, 2, 4, 128)
        out_copy(u, kind).start()

    @pl.when(u > 0)
    def _():
        put(3, jnp.where(lane == 0, first, held[...]))

    @pl.when(u < STEPS)
    def _():
        put(0, plus[:, :128])
        put(1, plus[:, 128:])
        put(2, jnp.where(lane == 0, second, jnp.take_along_axis(first, back, axis=1)))
        held[...] = jnp.take_along_axis(second, back, axis=1)

    @pl.when(u == STEPS)
    def _():
        out_wait(u - 1)
        out_wait(u)


def flow_kernel(spec_ref, leg_ref, held_ref, selected_ref, out_ref, last_ref, table_ref,
                spec, leg, order_ref, pick_ref, perm_ref, base, lat_ref, lhs, held, tiles, asend, arecv, coef,
                part1, core1, up1, in1, part2, core2, up2, in2, latf, bsend,
                load, leg_load, out_sem, table_sem, last_sem, a_s, a_r, b_s, b_r, *rad_sems):
    rad = lax.axis_index("rad")
    ma = lax.axis_index("ma")
    core = lax.rem(rad, 2)
    z = rad // 2
    partner = z * 2 + 1 - core
    zu = lax.rem(z + 1, 4)
    zd = lax.rem(z + 3, 4)
    zo = lax.rem(z + 2, 4)
    up = zu * 2 + core
    down = zd * 2 + core

    def each(first, last, body):
        def run(n, carry):
            body(n)
            return carry
        lax.fori_loop(first, last, run, 0)

    def load_copy(f, c):
        return pltpu.make_async_copy(spec_ref.at[2 * f + c], spec.at[c], load.at[c])

    def leg_copy(k):
        rows = pl.ds(lax.rem(k, BLOCKS) * CS, CS)
        return pltpu.make_async_copy(leg_ref.at[rows], leg.at[lax.rem(k, 2)], leg_load.at[lax.rem(k, 2)])

    load_copy(0, 0).start()
    load_copy(0, 1).start()
    leg_copy(0).start()

    lane = lax.broadcasted_iota(jnp.int32, (16, 128), 1)
    degree = rad * 128 + lax.broadcasted_iota(jnp.int32, (1, 128), 1)
    for r in range(8):
        line = jnp.broadcast_to(held_ref[r:r + 1, :].astype(jnp.float32), (128, 128))
        order_ref[128 * r:128 * (r + 1), :] = line.T.astype(jnp.int32)
    row = lax.broadcasted_iota(jnp.int32, (16, 128), 0)
    chosen = jnp.zeros((16, 128), jnp.int32)
    for i in range(SEL):
        chosen = jnp.where(row == i, selected_ref[i], chosen)
    for j in range(CS):
        for half in range(2):
            hit = (chosen == rad * 16 + 8 * half + lane // 16) & (lax.rem(lane, 16) == j)
            perm_ref[16 * j:16 * (j + 1), 128 * half:128 * (half + 1)] = jnp.where(hit, 1.0, 0.0).astype(jnp.bfloat16)

    def make_pick(b):
        def body(a):
            held = order_ref[pl.ds(a * 64 + b * CS, CS), :]
            for n in range(8):
                hit = jnp.where(held == lane + 128 * n, 1.0, 0.0).astype(jnp.bfloat16)
                pick_ref[b, pl.ds(pl.multiple_of(a * 16, 16), 16), 128 * n:128 * (n + 1)] = hit
        each(0, 16, body)

    def make_base():
        def body(n):
            rows = pl.ds(pl.multiple_of(n * 32, 32), 32)
            held = order_ref[rows, :]
            m = held.astype(jnp.float32)
            point = lax.broadcasted_iota(jnp.int32, (32, 128), 1).astype(jnp.float32)
            weight = jnp.where(held == 0, 1.0, 2.0)
            for at, scale, where in ((m * point, weight, 0), (m * 128.0, 1.0, 2)):
                at = at - NPHI * jnp.floor(at * (1.0 / NPHI))
                angle = at * (2.0 * jnp.pi / NPHI)
                base[where, rows, :] = scale * jnp.cos(angle)
                base[where + 1, rows, :] = scale * jnp.sin(angle)
        each(0, 32, body)

    barrier = pltpu.get_barrier_semaphore()
    for d in (partner, up, down):
        pl.semaphore_signal(barrier, inc=1, device_id={"rad": d}, device_id_type=MESH)
    for n in range(1, 16):
        pl.semaphore_signal(barrier, inc=1, device_id={"ma": lax.rem(ma + n, 16)}, device_id_type=MESH)

    def a_copy(k, n):
        to = lax.rem(ma + n, 16)
        return pltpu.make_async_remote_copy(
            src_ref=asend.at[lax.rem(k, 3), to], dst_ref=arecv.at[k, ma],
            send_sem=a_s.at[k, n], recv_sem=a_r.at[k, n],
            device_id={"ma": to}, device_id_type=MESH)

    def a_arrival(k, n):
        src = lax.rem(ma + 16 - n, 16)
        return pltpu.make_async_remote_copy(
            src_ref=asend.at[lax.rem(k, 3), src], dst_ref=arecv.at[k, src],
            send_sem=a_s.at[k, n], recv_sem=a_r.at[k, n],
            device_id={"ma": src}, device_id_type=MESH)

    def plane_copy(f, n):
        to = lax.rem(ma + n, 16)
        return pltpu.make_async_remote_copy(
            src_ref=bsend.at[f, to], dst_ref=lat_ref.at[f, ma],
            send_sem=b_s.at[f, n], recv_sem=b_r.at[f, n],
            device_id={"ma": to}, device_id_type=MESH)

    def plane_arrival(f, n):
        src = lax.rem(ma + 16 - n, 16)
        return pltpu.make_async_remote_copy(
            src_ref=bsend.at[f, src], dst_ref=lat_ref.at[f, src],
            send_sem=b_s.at[f, n], recv_sem=b_r.at[f, n],
            device_id={"ma": src}, device_id_type=MESH)

    class Reduce:
        def __init__(self, part, rcore, r1, r2, sems):
            self.part, self.rcore, self.r1, self.r2 = part, rcore, r1, r2
            self.core_s, self.core_r, self.z1_s, self.z1_r, self.z2_s, self.z2_r = sems

        def core_copy(self, k):
            return pltpu.make_async_remote_copy(
                src_ref=self.part.at[1 - core, lax.rem(k, 3)], dst_ref=self.rcore.at[k],
                send_sem=self.core_s.at[k], recv_sem=self.core_r.at[k],
                device_id={"rad": partner}, device_id_type=MESH)

        def z1_copy(self, k, side):
            return pltpu.make_async_remote_copy(
                src_ref=self.rcore.at[k, zo, side], dst_ref=self.r1.at[k, side],
                send_sem=self.z1_s.at[k, side], recv_sem=self.z1_r.at[k, side],
                device_id={"rad": up if side == 0 else down}, device_id_type=MESH)

        def z2_copy(self, k, side):
            return pltpu.make_async_remote_copy(
                src_ref=self.rcore.at[k, zu if side == 0 else zd], dst_ref=self.r2.at[k, side],
                send_sem=self.z2_s.at[k, side], recv_sem=self.z2_r.at[k, side],
                device_id={"rad": up if side == 0 else down}, device_id_type=MESH)

        def free(self, k):
            @pl.when(k >= 3)
            def _():
                self.core_copy(k - 3).wait_send()

        def add(self, k):
            self.core_copy(k).wait_recv()

            def body(n):
                q = n // 2
                h = lax.rem(n, 2)
                a = self.part[core, lax.rem(k, 3), q, h].astype(jnp.float32)
                b = self.rcore[k, q, h].astype(jnp.float32)
                self.rcore[k, q, h] = (a + b).astype(jnp.bfloat16)
            each(0, 8, body)
            self.z1_copy(k, 0).start()
            self.z1_copy(k, 1).start()

        def forward(self, k):
            for side in range(2):
                self.z1_copy(k, side).wait_recv()
                q = zu if side == 0 else zd
                a = self.rcore[k, q, side].astype(jnp.float32)
                b = self.r1[k, side].astype(jnp.float32)
                self.rcore[k, q, side] = (a + b).astype(jnp.bfloat16)
                self.z2_copy(k, side).start()

        def finish(self, k, store):
            self.z2_copy(k, 0).wait_recv()
            self.z2_copy(k, 1).wait_recv()
            for side in range(2):
                total = self.rcore[k, z, side].astype(jnp.float32)
                total = total + self.r2[k, 0, side].astype(jnp.float32)
                total = total + self.r2[k, 1, side].astype(jnp.float32)
                store(side, total)

        def drain(self):
            def body(k):
                for side in range(2):
                    self.z1_copy(k, side).wait_send()
                    self.z2_copy(k, side).wait_send()
            each(0, CHUNKS, body)
            each(CHUNKS - 3, CHUNKS, lambda k: self.core_copy(k).wait_send())

    relay = Reduce(part1, core1, up1, in1, rad_sems[:6])
    sums = Reduce(part2, core2, up2, in2, rad_sems[6:])

    def gather(k):
        f = k // BLOCKS
        b = lax.rem(k, BLOCKS)
        ring = lax.rem(k, 3)

        @pl.when(b == 0)
        def _():
            load_copy(f, 0).wait()
            load_copy(f, 1).wait()

        for c in range(2):
            for n in range(4):
                cols = slice(256 * n, 256 * (n + 1))
                rows = jnp.dot(pick_ref[b], spec[c, :, cols], preferred_element_type=jnp.float32)
                asend[ring, :, c, :, cols] = rows.reshape(16, CS, 256).astype(jnp.bfloat16)

        @pl.when((b == BLOCKS - 1) & (f < FIELDS - 1))
        def _():
            load_copy(f + 1, 0).start()
            load_copy(f + 1, 1).start()

    def compact(k):
        ring = lax.rem(k, 3)
        for c in range(2):
            for n in range(4):
                cols = slice(256 * n, 256 * (n + 1))
                rows = arecv[k, :, c, :, cols].reshape(256, 256)
                got = jnp.dot(perm_ref[...], rows, preferred_element_type=jnp.float32)
                got = got.reshape(CS, 16, 256).astype(jnp.bfloat16)
                part1[0, ring, n, c] = got[:, :, :128]
                part1[1, ring, n, c] = got[:, :, 128:]

    low = lax.broadcasted_iota(jnp.int32, (32, 128), 1) < 64
    top = lax.broadcasted_iota(jnp.int32, (8, 128), 0) < 4

    def legendre(k):
        first = lax.rem(k, BLOCKS) * CS
        ring = lax.rem(k, 3)
        leg_copy(k).wait()

        @pl.when(k < CHUNKS - 1)
        def _():
            leg_copy(k + 1).start()

        def store(side, total):
            keep = degree >= order_ref[pl.ds(ma * 64 + first, CS), :]
            coef[side] = jnp.where(keep[:, None, :], total, 0.0).astype(jnp.bfloat16)
        relay.finish(k, store)

        def slot(j):
            north = jnp.concatenate([coef[0, j], coef[1, j]], axis=0)
            odd = lax.rem(order_ref[pl.ds(ma * 64 + first + j, 1), :] + degree, 2)
            south = jnp.where(odd == 1, -north.astype(jnp.float32), north.astype(jnp.float32)).astype(jnp.bfloat16)
            both = jnp.concatenate([north, south], axis=0)
            res = jnp.dot(both, leg[lax.rem(k, 2), j], preferred_element_type=jnp.float32)
            for q in range(4):
                nt = res[:32, 128 * q:128 * (q + 1)]
                st = res[32:, 128 * q:128 * (q + 1)]
                even = jnp.where(low, nt, pltpu.roll(st, 64, 1)).astype(jnp.bfloat16)
                odd = jnp.where(low, pltpu.roll(nt, 64, 1), st).astype(jnp.bfloat16)
                for side in range(2):
                    part2[0, ring, q, side, j] = even[16 * side:16 * (side + 1)]
                    part2[1, ring, q, side, j] = odd[16 * side:16 * (side + 1)]
        each(0, CS, slot)

    def turn(half):
        def quad(n):
            turned = []
            for i in (4 * n, 4 * n + 2):
                block = jnp.concatenate(
                    [latf[c, pl.ds(i + odd, 32, stride=16), :] for odd in range(2) for c in range(2)], axis=0)
                turned.append(block.T)
            for b in range(8):
                first, second = [], []
                for x in turned:
                    nt, st = x[8 * b:8 * b + 8], x[64 + 8 * b:64 + 8 * b + 8]
                    first.append(jnp.where(top, nt, pltpu.roll(st, 4, 0)))
                    second.append(jnp.where(top, pltpu.roll(nt, 4, 0), st))
                bsend[half, 2 * b, n] = jnp.concatenate(first, axis=0).astype(jnp.bfloat16)
                bsend[half, 2 * b + 1, n] = jnp.concatenate(second, axis=0).astype(jnp.bfloat16)
        each(0, 4, quad)
        lat_ref[half, ma] = bsend[half, ma]

    def make_table(u):
        for half in range(2):
            for g in range(2):
                def rows(n, half=half, g=g):
                    r = pl.ds(pl.multiple_of(512 * g + 64 * n, 64), 64)
                    c = base[0, r, :]
                    s = base[1, r, :]
                    at = 256 * g + 128 * half
                    arecv[u, pl.ds(2 * n, 2), :, :, at:at + 128] = c.reshape(2, 2, CS, 128).astype(jnp.bfloat16)
                    arecv[u, pl.ds(2 * n, 2), :, :, 512 + at:640 + at] = (-s).reshape(2, 2, CS, 128).astype(jnp.bfloat16)
                    rc = base[2, r, :]
                    rs = base[3, r, :]
                    base[0, r, :] = c * rc - s * rs
                    base[1, r, :] = s * rc + c * rs
                each(0, 8, rows)

    def out_copy(f, u, kind):
        return tile_copy(tiles, out_sem, lambda cols: out_ref.at[:, f, :, :, cols], u, kind)

    def table_copy(u):
        return pltpu.make_async_copy(arecv.at[u], table_ref.at[u], table_sem.at[u])

    def gather_rows(f):
        for half in range(2):
            each(1, 16, lambda n: plane_arrival(2 * f + half, n).wait_recv())
        spread_rows(lambda half, a: lat_ref[2 * f + half, a], lhs)

    def longitudes(f, u):
        longitude_step(u, lambda cols: arecv[u, :, :, :, cols], lhs, held, tiles,
                       lambda v, kind: out_copy(f, v, kind))

    def between(k, first, last, body):
        @pl.when((k >= first) & (k < last))
        def _():
            body()

    def step(k, carry):
        def send():
            @pl.when(k >= 3)
            def _():
                each(1, 16, lambda n: a_copy(k - 3, n).wait_send())
            @pl.when((k > 0) & (k < BLOCKS))
            def _():
                make_pick(k)

            @pl.when(k > 0)
            def _():
                gather(k)
            each(1, 16, lambda n: a_copy(k, n).start())
            arecv[k, ma] = asend[lax.rem(k, 3), ma]
        between(k, 0, CHUNKS, send)

        @pl.when(k == 2)
        def _():
            make_base()
        between(k, 3, CHUNKS + 3, lambda: relay.forward(k - 3))
        between(k, 5, CHUNKS + 5, lambda: sums.forward(k - 5))
        first = jnp.where(k < 14, 2 * (k - 10), jnp.where(k == 15, 1, 4))
        count = jnp.where((k < 10) | (k > 13), 0, 1)

        @pl.when(k == 10)
        def _():
            gather_rows(0)
        each(first, first + count, lambda u: longitudes(jnp.where(k < 14, 0, 1), u))

        def arrive():
            c = k - 2
            each(1, 16, lambda n: a_arrival(c, n).wait_recv())
            relay.free(c)
            compact(c)
            relay.core_copy(c).start()
        between(k, 2, CHUNKS + 2, arrive)

        def transform():
            c = k - 4
            sums.free(c)
            legendre(c)
            sums.core_copy(c).start()
        between(k, 4, CHUNKS + 4, transform)
        between(k, 2, CHUNKS + 2, lambda: relay.add(k - 2))

        between(k, 4, CHUNKS + 4, lambda: sums.add(k - 4))
        def settle():
            c = k - 5
            half = c // 2
            rows = pl.ds(pl.multiple_of(lax.rem(c, 2) * 256, 256), 256)

            def store(side, total):
                latf[side, rows, :] = total.reshape(256, 128)
            sums.finish(c, store)

            @pl.when(lax.rem(c, 2) == 1)
            def _():
                turn(half)
                each(1, 16, lambda n: plane_copy(half, n).start())
        between(k, 5, CHUNKS + 5, settle)

        def fill():
            make_table(k - 3)
            table_copy(k - 3).start()
        between(k, 3, 3 + STEPS + 1, fill)

        @pl.when(k == 14)
        def _():
            gather_rows(1)
        second = jnp.where(k < 14, 2 * (k - 10) + 1, jnp.where(k == 14, 0, 3))
        more = jnp.where((k < 10) | (k >= 13), 0, 1)
        each(second, second + more, lambda u: longitudes(jnp.where(k < 14, 0, 1), u))
        return carry

    make_pick(0)
    gather(0)
    pl.semaphore_wait(barrier, 18)
    lax.fori_loop(0, CHUNKS + 5, step, 0)

    each(0, STEPS + 1, lambda u: longitudes(1, u))
    for half in (HALVES - 2, HALVES - 1):
        each(1, 16, lambda n: plane_arrival(half, n).wait_recv())
    last_copy = pltpu.make_async_copy(lat_ref.at[pl.ds(HALVES - 2, 2)], last_ref, last_sem)
    last_copy.start()
    last_copy.wait()
    each(0, STEPS + 1, lambda u: table_copy(u).wait())
    relay.drain()
    sums.drain()
    for k in range(CHUNKS - 3, CHUNKS):
        each(1, 16, lambda n: a_copy(k, n).wait_send())

    def last(n):
        for half in range(HALVES):
            plane_copy(half, n).wait_send()
    each(1, 16, last)


def flow(spec, leg, order, chosen):
    bf = jnp.bfloat16
    vm = pl.BlockSpec(memory_space=pltpu.VMEM)
    hbm = pl.BlockSpec(memory_space=pl.ANY)
    dma = pltpu.SemaphoreType.DMA
    reduce_scratch = [
        pltpu.VMEM((2, 3, 4, 2, CS, SEL, 128), bf),
        pltpu.VMEM((CHUNKS, 4, 2, CS, SEL, 128), bf),
        pltpu.VMEM((CHUNKS, 2, CS, SEL, 128), bf),
        pltpu.VMEM((CHUNKS, 2, 2, CS, SEL, 128), bf),
    ]
    return pl.pallas_call(
        flow_kernel,
        name="flow",
        out_shape=[jax.ShapeDtypeStruct((SEL, FIELDS - 1, 2, 4, NPHI), jnp.float32),
                   jax.ShapeDtypeStruct((2, 16, 4, 16, 128), bf),
                   jax.ShapeDtypeStruct((STEPS + 1, 16, 2, CS, M), bf)],
        in_specs=[hbm, hbm, vm, pl.BlockSpec(memory_space=pltpu.SMEM)],
        out_specs=[hbm, hbm, hbm],
        scratch_shapes=[
            pltpu.VMEM((2, M, M), bf),
            pltpu.VMEM((2, CS, 128, 512), bf),
            pltpu.VMEM((M, 128), jnp.int32),
            pltpu.VMEM((BLOCKS, 16 * CS, M), bf),
            pltpu.VMEM((16 * CS, 16 * CS), bf),
            pltpu.VMEM((4, M, 128), jnp.float32),
            pltpu.VMEM((HALVES, 16, 4, 16, 128), bf),
            pltpu.VMEM((2, 128, M), bf),
            pltpu.VMEM((128, 128), jnp.float32),
            pltpu.VMEM((8, SEL, 2, 4, 128), jnp.float32),
            pltpu.VMEM((3, 16, 2, CS, M), bf),
            pltpu.VMEM((CHUNKS, 16, 2, CS, M), bf),
            pltpu.VMEM((2, CS, SEL, 128), bf),
            *reduce_scratch, *reduce_scratch,
            pltpu.VMEM((2, 512, 128), jnp.float32),
            pltpu.VMEM((HALVES, 16, 4, 16, 128), bf),
            dma((2,)), dma((2,)), dma((8,)), dma((STEPS + 1,)), dma(()),
            dma((CHUNKS, 16)), dma((CHUNKS, 16)),
            dma((HALVES, 16)), dma((HALVES, 16)),
            *([dma((CHUNKS,))] * 2 + [dma((CHUNKS, 2))] * 4) * 2,
        ],
        compiler_params=pltpu.CompilerParams(
            collective_id=1, has_side_effects=True, vmem_limit_bytes=67043328),
    )(spec, leg, order, chosen)


def last_kernel(done_ref, lat_ref, table_ref, out_ref, moved, tables, lhs, held, tiles, in_sem, back_sem, table_sem, out_sem):
    def move_in(n):
        return pltpu.make_async_copy(done_ref.at[pl.ds(4 * n, 4)], moved.at[pl.ds(4 * n, 4)], in_sem.at[n])

    def move_out(n):
        return pltpu.make_async_copy(moved.at[pl.ds(4 * n, 4)], out_ref.at[pl.ds(4 * n, 4), :2], back_sem.at[n])

    def table_copy(u):
        return pltpu.make_async_copy(table_ref.at[u], tables.at[u], table_sem.at[u])

    table_copy(0).start()
    for u in range(1, STEPS + 1):
        if u <= 4:
            move_in(u - 1).start()
        table_copy(u).start()
    spread_rows(lambda half, a: lat_ref[half, a], lhs)

    def step(u, carry):
        table_copy(u).wait()

        @pl.when((u >= 1) & (u < 5))
        def _():
            move_in(u - 1).wait()
            move_out(u - 1).start()
        longitude_step(u, lambda cols: tables[u, :, :, :, cols], lhs, held, tiles,
                       lambda v, kind: tile_copy(tiles, out_sem, lambda c: out_ref.at[:, 2, :, :, c], v, kind))
        return carry
    lax.fori_loop(0, STEPS + 1, step, 0)
    for n in range(4):
        move_out(n).wait()


def last(done, lat, tables):
    bf = jnp.bfloat16
    hbm = pl.BlockSpec(memory_space=pl.ANY)
    dma = pltpu.SemaphoreType.DMA
    return pl.pallas_call(
        last_kernel,
        name="last",
        out_shape=jax.ShapeDtypeStruct((SEL, FIELDS, 2, 4, NPHI), jnp.float32),
        in_specs=[hbm, pl.BlockSpec(memory_space=pltpu.VMEM), hbm],
        out_specs=hbm,
        scratch_shapes=[
            pltpu.VMEM((SEL, FIELDS - 1, 2, 4, NPHI), jnp.float32),
            pltpu.VMEM((STEPS + 1, 16, 2, CS, M), bf),
            pltpu.VMEM((2, 128, M), bf),
            pltpu.VMEM((128, 128), jnp.float32),
            pltpu.VMEM((8, SEL, 2, 4, 128), jnp.float32),
            dma((4,)), dma((4,)), dma((STEPS + 1,)), dma((8,)),
        ],
        compiler_params=pltpu.CompilerParams(vmem_limit_bytes=60 * 1024 * 1024),
    )(done, lat, tables)


def local(spectra, legendre, selected, m_order):
    return last(*flow(spectra.reshape(2 * FIELDS, M, M), legendre, m_order.reshape(8, 128), selected))


def solution(mesh):
    rad_ma = ("rad", "ma")
    in_specs = (P(rad_ma, None, None, None, None), P("ma", "rad", None), P(), P())
    out_specs = P(None, None, None, rad_ma, None)
    return jax.shard_map(local, mesh=mesh, in_specs=in_specs, out_specs=out_specs, check_vma=False)
```

```python
import jax
import jax.numpy as jnp
from jax import lax
from jax.experimental import pallas as pl
from jax.experimental.pallas import tpu as pltpu
from jax.sharding import PartitionSpec as P

MESH = pl.DeviceIdType.MESH
M = 1024
NPHI = 3072
FIELDS = 3
SEL = 16
BLOCKS = 4
CS = 16
CHUNKS = FIELDS * BLOCKS
STEPS = NPHI // 2 // 256
HALVES = 2 * FIELDS


def tile_copy(tiles, sems, target, u, kind):
    tile = (2 * u, 2 * u + 1, 23 - 2 * u, 24 - 2 * u)[kind]
    slot = 4 * lax.rem(u, 2) + kind
    cols = pl.ds(pl.multiple_of(tile * 128, 128), 128)
    return pltpu.make_async_copy(tiles.at[slot], target(cols), sems.at[slot])


def spread_rows(lat, lhs):
    quarter = lax.broadcasted_iota(jnp.int32, (64, 128), 1) // 32
    for b in range(8):
        held = [lat(n % 2, 2 * b + n // 2).reshape(64, 128).astype(jnp.float32) for n in range(4)]
        for c in range(2):
            pair = []
            for odd in range(2):
                row = None
                for n in range(4):
                    shift = (32 * n - 64 * odd - 32 * c) % 128
                    piece = pltpu.roll(held[n], shift, 1) if shift else held[n]
                    row = piece if row is None else jnp.where(quarter == n, piece, row)
                pair.append(row)
            rows = [pair[n % 2][8 * (n // 2):8 * (n // 2) + 8] for n in range(16)]
            lhs[c, :, 128 * b:128 * (b + 1)] = jnp.concatenate(rows, axis=0).astype(jnp.bfloat16)


def longitude_step(u, table, lhs, held, tiles, out_copy):
    lane = lax.broadcasted_iota(jnp.int32, (128, 128), 1)
    back = lax.rem(128 - lane, 128)

    def out_wait(v):
        @pl.when(v < STEPS)
        def _():
            for kind in range(3):
                out_copy(v, kind).wait()

        @pl.when(v > 0)
        def _():
            out_copy(v, 3).wait()

    @pl.when(u >= 2)
    def _():
        out_wait(u - 2)
    parts = []
    for c in range(2):
        acc = jnp.zeros((128, 256), jnp.float32)
        for g in range(2):
            at = 512 * c + 256 * g
            rows = table(slice(at, at + 256)).reshape(512, 256)
            acc = acc + jnp.dot(lhs[c, :, 512 * g:512 * (g + 1)], rows, preferred_element_type=jnp.float32)
        parts.append(acc)
    plus = parts[0] + parts[1]
    less = parts[0] - parts[1]
    first, second = less[:, :128], less[:, 128:]
    slot = 4 * lax.rem(u, 2)

    def put(kind, x):
        tiles[slot + kind] = x.reshape(SEL, 2, 4, 128)
        out_copy(u, kind).start()

    @pl.when(u > 0)
    def _():
        put(3, jnp.where(lane == 0, first, held[...]))

    @pl.when(u < STEPS)
    def _():
        put(0, plus[:, :128])
        put(1, plus[:, 128:])
        put(2, jnp.where(lane == 0, second, jnp.take_along_axis(first, back, axis=1)))
        held[...] = jnp.take_along_axis(second, back, axis=1)

    @pl.when(u == STEPS)
    def _():
        out_wait(u - 1)
        out_wait(u)


def flow_kernel(spec_ref, leg_ref, held_ref, selected_ref, out_ref, last_ref, table_ref,
                spec, leg, order_ref, pick_ref, perm_ref, base, lat_ref, lhs, held, tiles, asend, arecv, coef,
                part1, core1, up1, in1, part2, core2, up2, in2, latf, bsend,
                load, leg_load, out_sem, table_sem, last_sem, a_s, a_r, b_s, b_r, *rad_sems):
    rad = lax.axis_index("rad")
    ma = lax.axis_index("ma")
    core = lax.rem(rad, 2)
    z = rad // 2
    partner = z * 2 + 1 - core
    zu = lax.rem(z + 1, 4)
    zd = lax.rem(z + 3, 4)
    zo = lax.rem(z + 2, 4)
    up = zu * 2 + core
    down = zd * 2 + core

    def each(first, last, body):
        def run(n, carry):
            body(n)
            return carry
        lax.fori_loop(first, last, run, 0)

    def load_copy(f, c):
        return pltpu.make_async_copy(spec_ref.at[2 * f + c], spec.at[c], load.at[c])

    def leg_copy(k):
        rows = pl.ds(lax.rem(k, BLOCKS) * CS, CS)
        return pltpu.make_async_copy(leg_ref.at[rows], leg.at[lax.rem(k, 2)], leg_load.at[lax.rem(k, 2)])

    load_copy(0, 0).start()
    load_copy(0, 1).start()
    leg_copy(0).start()

    lane = lax.broadcasted_iota(jnp.int32, (16, 128), 1)
    degree = rad * 128 + lax.broadcasted_iota(jnp.int32, (1, 128), 1)
    for r in range(8):
        line = jnp.broadcast_to(held_ref[r:r + 1, :].astype(jnp.float32), (128, 128))
        order_ref[128 * r:128 * (r + 1), :] = line.T.astype(jnp.int32)
    def make_perm():
        row = lax.broadcasted_iota(jnp.int32, (16, 128), 0)
        chosen = jnp.zeros((16, 128), jnp.int32)
        for i in range(SEL):
            chosen = jnp.where(row == i, selected_ref[i], chosen)
        for j in range(CS):
            for half in range(2):
                hit = (chosen == rad * 16 + 8 * half + lane // 16) & (lax.rem(lane, 16) == j)
                perm_ref[16 * j:16 * (j + 1), 128 * half:128 * (half + 1)] = jnp.where(hit, 1.0, 0.0).astype(jnp.bfloat16)

    def make_pick(b):
        def body(a):
            held = order_ref[pl.ds(a * 64 + b * CS, CS), :]
            for n in range(8):
                hit = jnp.where(held == lane + 128 * n, 1.0, 0.0).astype(jnp.bfloat16)
                pick_ref[b, pl.ds(pl.multiple_of(a * 16, 16), 16), 128 * n:128 * (n + 1)] = hit
        each(0, 16, body)

    def make_base():
        def body(n):
            rows = pl.ds(pl.multiple_of(n * 32, 32), 32)
            held = order_ref[rows, :]
            m = held.astype(jnp.float32)
            point = lax.broadcasted_iota(jnp.int32, (32, 128), 1).astype(jnp.float32)
            weight = jnp.where(held == 0, 1.0, 2.0)
            for at, scale, where in ((m * point, weight, 0), (m * 128.0, 1.0, 2)):
                at = at - NPHI * jnp.floor(at * (1.0 / NPHI))
                angle = at * (2.0 * jnp.pi / NPHI)
                base[where, rows, :] = scale * jnp.cos(angle)
                base[where + 1, rows, :] = scale * jnp.sin(angle)
        each(0, 32, body)

    barrier = pltpu.get_barrier_semaphore()
    for d in (partner, up, down):
        pl.semaphore_signal(barrier, inc=1, device_id={"rad": d}, device_id_type=MESH)
    for n in range(1, 16):
        pl.semaphore_signal(barrier, inc=1, device_id={"ma": lax.rem(ma + n, 16)}, device_id_type=MESH)

    def a_copy(k, n):
        to = lax.rem(ma + n, 16)
        return pltpu.make_async_remote_copy(
            src_ref=asend.at[lax.rem(k, 3), to], dst_ref=arecv.at[k, ma],
            send_sem=a_s.at[k, n], recv_sem=a_r.at[k, n],
            device_id={"ma": to}, device_id_type=MESH)

    def a_arrival(k, n):
        src = lax.rem(ma + 16 - n, 16)
        return pltpu.make_async_remote_copy(
            src_ref=asend.at[lax.rem(k, 3), src], dst_ref=arecv.at[k, src],
            send_sem=a_s.at[k, n], recv_sem=a_r.at[k, n],
            device_id={"ma": src}, device_id_type=MESH)

    def plane_copy(f, n):
        to = lax.rem(ma + n, 16)
        return pltpu.make_async_remote_copy(
            src_ref=bsend.at[f, to], dst_ref=lat_ref.at[f, ma],
            send_sem=b_s.at[f, n], recv_sem=b_r.at[f, n],
            device_id={"ma": to}, device_id_type=MESH)

    def plane_arrival(f, n):
        src = lax.rem(ma + 16 - n, 16)
        return pltpu.make_async_remote_copy(
            src_ref=bsend.at[f, src], dst_ref=lat_ref.at[f, src],
            send_sem=b_s.at[f, n], recv_sem=b_r.at[f, n],
            device_id={"ma": src}, device_id_type=MESH)

    class Reduce:
        def __init__(self, part, rcore, r1, r2, sems):
            self.part, self.rcore, self.r1, self.r2 = part, rcore, r1, r2
            self.core_s, self.core_r, self.z1_s, self.z1_r, self.z2_s, self.z2_r = sems

        def core_copy(self, k):
            return pltpu.make_async_remote_copy(
                src_ref=self.part.at[1 - core, lax.rem(k, 3)], dst_ref=self.rcore.at[k],
                send_sem=self.core_s.at[k], recv_sem=self.core_r.at[k],
                device_id={"rad": partner}, device_id_type=MESH)

        def z1_copy(self, k, side):
            return pltpu.make_async_remote_copy(
                src_ref=self.rcore.at[k, zo, side], dst_ref=self.r1.at[k, side],
                send_sem=self.z1_s.at[k, side], recv_sem=self.z1_r.at[k, side],
                device_id={"rad": up if side == 0 else down}, device_id_type=MESH)

        def z2_copy(self, k, side):
            return pltpu.make_async_remote_copy(
                src_ref=self.rcore.at[k, zu if side == 0 else zd], dst_ref=self.r2.at[k, side],
                send_sem=self.z2_s.at[k, side], recv_sem=self.z2_r.at[k, side],
                device_id={"rad": up if side == 0 else down}, device_id_type=MESH)

        def free(self, k):
            @pl.when(k >= 3)
            def _():
                self.core_copy(k - 3).wait_send()

        def add(self, k):
            self.core_copy(k).wait_recv()

            def body(n):
                q = n // 2
                h = lax.rem(n, 2)
                a = self.part[core, lax.rem(k, 3), q, h].astype(jnp.float32)
                b = self.rcore[k, q, h].astype(jnp.float32)
                self.rcore[k, q, h] = (a + b).astype(jnp.bfloat16)
            each(0, 8, body)
            self.z1_copy(k, 0).start()
            self.z1_copy(k, 1).start()

        def forward(self, k):
            for side in range(2):
                self.z1_copy(k, side).wait_recv()
                q = zu if side == 0 else zd
                a = self.rcore[k, q, side].astype(jnp.float32)
                b = self.r1[k, side].astype(jnp.float32)
                self.rcore[k, q, side] = (a + b).astype(jnp.bfloat16)
                self.z2_copy(k, side).start()

        def finish(self, k, store):
            self.z2_copy(k, 0).wait_recv()
            self.z2_copy(k, 1).wait_recv()
            for side in range(2):
                total = self.rcore[k, z, side].astype(jnp.float32)
                total = total + self.r2[k, 0, side].astype(jnp.float32)
                total = total + self.r2[k, 1, side].astype(jnp.float32)
                store(side, total)

        def drain(self):
            def body(k):
                for side in range(2):
                    self.z1_copy(k, side).wait_send()
                    self.z2_copy(k, side).wait_send()
            each(0, CHUNKS, body)
            each(CHUNKS - 3, CHUNKS, lambda k: self.core_copy(k).wait_send())

    relay = Reduce(part1, core1, up1, in1, rad_sems[:6])
    sums = Reduce(part2, core2, up2, in2, rad_sems[6:])

    def gather(k):
        f = k // BLOCKS
        b = lax.rem(k, BLOCKS)
        ring = lax.rem(k, 3)

        @pl.when(b == 0)
        def _():
            load_copy(f, 0).wait()
            load_copy(f, 1).wait()

        for c in range(2):
            for n in range(4):
                cols = slice(256 * n, 256 * (n + 1))
                rows = jnp.dot(pick_ref[b], spec[c, :, cols], preferred_element_type=jnp.float32)
                asend[ring, :, c, :, cols] = rows.reshape(16, CS, 256).astype(jnp.bfloat16)

        @pl.when((b == BLOCKS - 1) & (f < FIELDS - 1))
        def _():
            load_copy(f + 1, 0).start()
            load_copy(f + 1, 1).start()

    def compact(k):
        ring = lax.rem(k, 3)
        for c in range(2):
            for n in range(4):
                cols = slice(256 * n, 256 * (n + 1))
                rows = arecv[k, :, c, :, cols].reshape(256, 256)
                got = jnp.dot(perm_ref[...], rows, preferred_element_type=jnp.float32)
                got = got.reshape(CS, 16, 256).astype(jnp.bfloat16)
                part1[0, ring, n, c] = got[:, :, :128]
                part1[1, ring, n, c] = got[:, :, 128:]

    low = lax.broadcasted_iota(jnp.int32, (32, 128), 1) < 64
    top = lax.broadcasted_iota(jnp.int32, (8, 128), 0) < 4

    def legendre(k):
        first = lax.rem(k, BLOCKS) * CS
        ring = lax.rem(k, 3)
        leg_copy(k).wait()

        @pl.when(k < CHUNKS - 1)
        def _():
            leg_copy(k + 1).start()

        def store(side, total):
            keep = degree >= order_ref[pl.ds(ma * 64 + first, CS), :]
            coef[side] = jnp.where(keep[:, None, :], total, 0.0).astype(jnp.bfloat16)
        relay.finish(k, store)

        def slot(j):
            north = jnp.concatenate([coef[0, j], coef[1, j]], axis=0)
            odd = lax.rem(order_ref[pl.ds(ma * 64 + first + j, 1), :] + degree, 2)
            south = jnp.where(odd == 1, -north.astype(jnp.float32), north.astype(jnp.float32)).astype(jnp.bfloat16)
            both = jnp.concatenate([north, south], axis=0)
            res = jnp.dot(both, leg[lax.rem(k, 2), j], preferred_element_type=jnp.float32)
            for q in range(4):
                nt = res[:32, 128 * q:128 * (q + 1)]
                st = res[32:, 128 * q:128 * (q + 1)]
                even = jnp.where(low, nt, pltpu.roll(st, 64, 1)).astype(jnp.bfloat16)
                odd = jnp.where(low, pltpu.roll(nt, 64, 1), st).astype(jnp.bfloat16)
                for side in range(2):
                    part2[0, ring, q, side, j] = even[16 * side:16 * (side + 1)]
                    part2[1, ring, q, side, j] = odd[16 * side:16 * (side + 1)]
        each(0, CS, slot)

    def turn(half):
        def quad(n):
            turned = []
            for i in (4 * n, 4 * n + 2):
                block = jnp.concatenate(
                    [latf[c, pl.ds(i + odd, 32, stride=16), :] for odd in range(2) for c in range(2)], axis=0)
                turned.append(block.T)
            for b in range(8):
                first, second = [], []
                for x in turned:
                    nt, st = x[8 * b:8 * b + 8], x[64 + 8 * b:64 + 8 * b + 8]
                    first.append(jnp.where(top, nt, pltpu.roll(st, 4, 0)))
                    second.append(jnp.where(top, pltpu.roll(nt, 4, 0), st))
                bsend[half, 2 * b, n] = jnp.concatenate(first, axis=0).astype(jnp.bfloat16)
                bsend[half, 2 * b + 1, n] = jnp.concatenate(second, axis=0).astype(jnp.bfloat16)
        each(0, 4, quad)
        lat_ref[half, ma] = bsend[half, ma]

    def make_table(u):
        for half in range(2):
            for g in range(2):
                def rows(n, half=half, g=g):
                    r = pl.ds(pl.multiple_of(512 * g + 64 * n, 64), 64)
                    c = base[0, r, :]
                    s = base[1, r, :]
                    at = 256 * g + 128 * half
                    arecv[u, pl.ds(2 * n, 2), :, :, at:at + 128] = c.reshape(2, 2, CS, 128).astype(jnp.bfloat16)
                    arecv[u, pl.ds(2 * n, 2), :, :, 512 + at:640 + at] = (-s).reshape(2, 2, CS, 128).astype(jnp.bfloat16)
                    rc = base[2, r, :]
                    rs = base[3, r, :]
                    base[0, r, :] = c * rc - s * rs
                    base[1, r, :] = s * rc + c * rs
                each(0, 8, rows)

    def out_copy(f, u, kind):
        return tile_copy(tiles, out_sem, lambda cols: out_ref.at[:, f, :, :, cols], u, kind)

    def table_copy(u):
        return pltpu.make_async_copy(arecv.at[u], table_ref.at[u], table_sem.at[u])

    def gather_rows(f):
        for half in range(2):
            each(1, 16, lambda n: plane_arrival(2 * f + half, n).wait_recv())
        spread_rows(lambda half, a: lat_ref[2 * f + half, a], lhs)

    def longitudes(f, u):
        longitude_step(u, lambda cols: arecv[u, :, :, :, cols], lhs, held, tiles,
                       lambda v, kind: out_copy(f, v, kind))

    def between(k, first, last, body):
        @pl.when((k >= first) & (k < last))
        def _():
            body()

    def step(k, carry):
        def send():
            @pl.when(k >= 3)
            def _():
                each(1, 16, lambda n: a_copy(k - 3, n).wait_send())
            @pl.when((k > 0) & (k < BLOCKS))
            def _():
                make_pick(k)

            @pl.when(k > 0)
            def _():
                gather(k)
            each(1, 16, lambda n: a_copy(k, n).start())
            arecv[k, ma] = asend[lax.rem(k, 3), ma]
        between(k, 0, CHUNKS, send)

        @pl.when(k == 1)
        def _():
            make_perm()

        @pl.when(k == 2)
        def _():
            make_base()
        between(k, 3, CHUNKS + 3, lambda: relay.forward(k - 3))
        between(k, 5, CHUNKS + 5, lambda: sums.forward(k - 5))
        first = jnp.where(k < 14, 2 * (k - 10), jnp.where(k == 15, 1, 4))
        count = jnp.where((k < 10) | (k > 13), 0, 1)

        @pl.when(k == 10)
        def _():
            gather_rows(0)
        each(first, first + count, lambda u: longitudes(jnp.where(k < 14, 0, 1), u))

        def arrive():
            c = k - 2
            each(1, 16, lambda n: a_arrival(c, n).wait_recv())
            relay.free(c)
            compact(c)
            relay.core_copy(c).start()
        between(k, 2, CHUNKS + 2, arrive)

        def transform():
            c = k - 4
            sums.free(c)
            legendre(c)
            sums.core_copy(c).start()
        between(k, 4, CHUNKS + 4, transform)
        between(k, 2, CHUNKS + 2, lambda: relay.add(k - 2))

        between(k, 4, CHUNKS + 4, lambda: sums.add(k - 4))
        def settle():
            c = k - 5
            half = c // 2
            rows = pl.ds(pl.multiple_of(lax.rem(c, 2) * 256, 256), 256)

            def store(side, total):
                latf[side, rows, :] = total.reshape(256, 128)
            sums.finish(c, store)

            @pl.when(lax.rem(c, 2) == 1)
            def _():
                turn(half)
                each(1, 16, lambda n: plane_copy(half, n).start())
        between(k, 5, CHUNKS + 5, settle)

        def fill():
            make_table(k - 3)
            table_copy(k - 3).start()
        between(k, 3, 3 + STEPS + 1, fill)

        @pl.when(k == 14)
        def _():
            gather_rows(1)
        second = jnp.where(k < 14, 2 * (k - 10) + 1, jnp.where(k == 14, 0, 3))
        more = jnp.where((k < 10) | (k >= 13), 0, 1)
        each(second, second + more, lambda u: longitudes(jnp.where(k < 14, 0, 1), u))
        return carry

    make_pick(0)
    gather(0)
    pl.semaphore_wait(barrier, 18)
    lax.fori_loop(0, CHUNKS + 5, step, 0)

    each(0, STEPS + 1, lambda u: longitudes(1, u))
    for half in (HALVES - 2, HALVES - 1):
        each(1, 16, lambda n: plane_arrival(half, n).wait_recv())
    last_copy = pltpu.make_async_copy(lat_ref.at[pl.ds(HALVES - 2, 2)], last_ref, last_sem)
    last_copy.start()
    last_copy.wait()
    each(0, STEPS + 1, lambda u: table_copy(u).wait())
    relay.drain()
    sums.drain()
    for k in range(CHUNKS - 3, CHUNKS):
        each(1, 16, lambda n: a_copy(k, n).wait_send())

    def last(n):
        for half in range(HALVES):
            plane_copy(half, n).wait_send()
    each(1, 16, last)


def flow(spec, leg, order, chosen):
    bf = jnp.bfloat16
    vm = pl.BlockSpec(memory_space=pltpu.VMEM)
    hbm = pl.BlockSpec(memory_space=pl.ANY)
    dma = pltpu.SemaphoreType.DMA
    reduce_scratch = [
        pltpu.VMEM((2, 3, 4, 2, CS, SEL, 128), bf),
        pltpu.VMEM((CHUNKS, 4, 2, CS, SEL, 128), bf),
        pltpu.VMEM((CHUNKS, 2, CS, SEL, 128), bf),
        pltpu.VMEM((CHUNKS, 2, 2, CS, SEL, 128), bf),
    ]
    return pl.pallas_call(
        flow_kernel,
        name="flow",
        out_shape=[jax.ShapeDtypeStruct((SEL, FIELDS - 1, 2, 4, NPHI), jnp.float32),
                   jax.ShapeDtypeStruct((2, 16, 4, 16, 128), bf),
                   jax.ShapeDtypeStruct((STEPS + 1, 16, 2, CS, M), bf)],
        in_specs=[hbm, hbm, vm, pl.BlockSpec(memory_space=pltpu.SMEM)],
        out_specs=[hbm, hbm, hbm],
        scratch_shapes=[
            pltpu.VMEM((2, M, M), bf),
            pltpu.VMEM((2, CS, 128, 512), bf),
            pltpu.VMEM((M, 128), jnp.int32),
            pltpu.VMEM((BLOCKS, 16 * CS, M), bf),
            pltpu.VMEM((16 * CS, 16 * CS), bf),
            pltpu.VMEM((4, M, 128), jnp.float32),
            pltpu.VMEM((HALVES, 16, 4, 16, 128), bf),
            pltpu.VMEM((2, 128, M), bf),
            pltpu.VMEM((128, 128), jnp.float32),
            pltpu.VMEM((8, SEL, 2, 4, 128), jnp.float32),
            pltpu.VMEM((3, 16, 2, CS, M), bf),
            pltpu.VMEM((CHUNKS, 16, 2, CS, M), bf),
            pltpu.VMEM((2, CS, SEL, 128), bf),
            *reduce_scratch, *reduce_scratch,
            pltpu.VMEM((2, 512, 128), jnp.float32),
            pltpu.VMEM((HALVES, 16, 4, 16, 128), bf),
            dma((2,)), dma((2,)), dma((8,)), dma((STEPS + 1,)), dma(()),
            dma((CHUNKS, 16)), dma((CHUNKS, 16)),
            dma((HALVES, 16)), dma((HALVES, 16)),
            *([dma((CHUNKS,))] * 2 + [dma((CHUNKS, 2))] * 4) * 2,
        ],
        compiler_params=pltpu.CompilerParams(
            collective_id=1, has_side_effects=True, vmem_limit_bytes=67043328),
    )(spec, leg, order, chosen)


def last_kernel(done_ref, lat_ref, table_ref, out_ref, moved, tables, lhs, held, tiles, in_sem, back_sem, table_sem, out_sem):
    def move_in(n):
        return pltpu.make_async_copy(done_ref.at[pl.ds(4 * n, 4)], moved.at[pl.ds(4 * n, 4)], in_sem.at[n])

    def move_out(n):
        return pltpu.make_async_copy(moved.at[pl.ds(4 * n, 4)], out_ref.at[pl.ds(4 * n, 4), :2], back_sem.at[n])

    def table_copy(u):
        return pltpu.make_async_copy(table_ref.at[u], tables.at[u], table_sem.at[u])

    table_copy(0).start()
    for u in range(1, STEPS + 1):
        if u <= 4:
            move_in(u - 1).start()
        table_copy(u).start()
    spread_rows(lambda half, a: lat_ref[half, a], lhs)

    def step(u, carry):
        table_copy(u).wait()

        @pl.when((u >= 1) & (u < 5))
        def _():
            move_in(u - 1).wait()
            move_out(u - 1).start()
        longitude_step(u, lambda cols: tables[u, :, :, :, cols], lhs, held, tiles,
                       lambda v, kind: tile_copy(tiles, out_sem, lambda c: out_ref.at[:, 2, :, :, c], v, kind))
        return carry
    lax.fori_loop(0, STEPS + 1, step, 0)
    for n in range(4):
        move_out(n).wait()


def last(done, lat, tables):
    bf = jnp.bfloat16
    hbm = pl.BlockSpec(memory_space=pl.ANY)
    dma = pltpu.SemaphoreType.DMA
    return pl.pallas_call(
        last_kernel,
        name="last",
        out_shape=jax.ShapeDtypeStruct((SEL, FIELDS, 2, 4, NPHI), jnp.float32),
        in_specs=[hbm, pl.BlockSpec(memory_space=pltpu.VMEM), hbm],
        out_specs=hbm,
        scratch_shapes=[
            pltpu.VMEM((SEL, FIELDS - 1, 2, 4, NPHI), jnp.float32),
            pltpu.VMEM((STEPS + 1, 16, 2, CS, M), bf),
            pltpu.VMEM((2, 128, M), bf),
            pltpu.VMEM((128, 128), jnp.float32),
            pltpu.VMEM((8, SEL, 2, 4, 128), jnp.float32),
            dma((4,)), dma((4,)), dma((STEPS + 1,)), dma((8,)),
        ],
        compiler_params=pltpu.CompilerParams(vmem_limit_bytes=60 * 1024 * 1024),
    )(done, lat, tables)


def local(spectra, legendre, selected, m_order):
    return last(*flow(spectra.reshape(2 * FIELDS, M, M), legendre, m_order.reshape(8, 128), selected))


def solution(mesh):
    rad_ma = ("rad", "ma")
    in_specs = (P(rad_ma, None, None, None, None), P("ma", "rad", None), P(), P())
    out_specs = P(None, None, None, rad_ma, None)
    return jax.shard_map(local, mesh=mesh, in_specs=in_specs, out_specs=out_specs, check_vma=False)
```
